256 devices in a mesh: dp: 32 (over y, x, core), seq: 8 (over z).
Axes of the slice: x: 4, y: 4, z: 8, core: 2. Of those that a mesh axis runs over, the one named last changes fastest.
Arguments:
- tokens: bfloat16 [32, 1024, 1024], P('dp', 'seq'), may hold values from -6 to 6
- cotangent: bfloat16 [32, 1024, 1024], P('dp', 'seq'), may hold values from -6 to 6
- stamps: int32 [32, 1024], P('dp'), may hold values from 0 to 1113088, as said below
- lengths: int32 [32], P('dp'), may hold values from 128 to 1024, as said below
- w_qkvu: bfloat16 [1024, 4096], P('dp'), may hold values from -0.1875 to 0.1875
- w_out: bfloat16 [1024, 1024], P('dp'), may hold values from -0.1875 to 0.1875
- gain_in: float32 [1024], replicated, may hold values from 0.25 to 1.75
- gain_out: float32 [1024], replicated, may hold values from 0.25 to 1.75
- bias_table: float32 [8, 16], replicated, may hold values from -4 to 4
Outputs:
- mixed: bfloat16 [32, 1024, 1024], P('dp', 'seq')
- input_grad: bfloat16 [32, 1024, 1024], P('dp', 'seq')
- out_weight_grad: float32 [1024, 1024], P('dp')
The draws below stay inside these ranges and needn't reach their ends.
Inputs may be any that keep to these rules, and one draw needn't show every extreme that they name: `lengths`: each stream has 128 valid actions or more; some stream is full. `stamps`: timestamps never fall along a stream, and consecutive ones differ by less than 64.
All inputs are finite; a program needn't handle non-finite values.
Results may differ from the reference program's by a relative error of at most 0.019.
Values may be sent and summed in bfloat16 or wider, within the bound.
No kernel may reach another device: no remote copies, remote signals or barrier semaphores. Data moves between devices by JAX's collectives and lax.ppermute only.
A program may use at most 128 MiB of HBM per device.

```python
import jax
import jax.numpy as jnp
from jax import lax

D = 1024
H = 8
DH = 128
NB = 16
TOK_DEV = 128
SEQLEN = 1024
STREAMS = 32
N_SEQ = 8


def draw_lengths(key, part):
    spread = jax.random.randint(key, (STREAMS,), SEQLEN // 8, SEQLEN + 1)
    chosen = jax.random.randint(jax.random.fold_in(key, 7), (), 0, STREAMS)
    return jnp.where(jnp.arange(STREAMS) == chosen, SEQLEN, spread).astype(jnp.int32)


def draw_stamps(key, part):
    anchor = jax.random.randint(key, (STREAMS, 1), 0, 2 ** 20)
    increments = jax.random.randint(jax.random.fold_in(key, 3), (STREAMS, SEQLEN), 0, 64)
    return (anchor + jnp.cumsum(increments, axis=1) - increments[:, :1]).astype(jnp.int32)


def shard_levels(rng, dims, pieces, low, high):
    def one(position, shards_of):
        steps = jax.random.uniform(jax.random.fold_in(jax.random.fold_in(rng, 6), position), (shards_of,), jnp.float32, low / len(pieces), high / len(pieces))
        return jnp.repeat(jnp.exp(steps), dims[position] // shards_of).reshape((-1,) + (1,) * (len(dims) - position - 1))

    loudness = one(*pieces[0])
    for cut in pieces[1:]:
        loudness = loudness * one(*cut)
    return loudness


def normal_values(own_key, shape, deviation, limit, pieces=(), held_as=jnp.bfloat16):
    level = shard_levels(own_key, shape, pieces, -0.22, 0.18) if pieces else 1.0
    entries = jax.random.normal(own_key, shape, jnp.float32) * deviation * level
    return jnp.minimum(jnp.maximum(entries, -limit), limit).astype(held_as)


def setup_inputs(seed: int = 0) -> dict:
    streams_of = jax.random.split(jax.random.key(seed), 10)
    tokens = normal_values(streams_of[0], (STREAMS, SEQLEN, D), 1.0, 6.0, ((0, 32), (1, 8)))
    cotangent = normal_values(streams_of[1], (STREAMS, SEQLEN, D), 1.0, 6.0, ((0, 32), (1, 8)))
    stamps = draw_stamps(jax.random.fold_in(streams_of[9], 71), 0)
    lengths = draw_lengths(jax.random.fold_in(streams_of[9], 71), 0)
    w_qkvu = normal_values(streams_of[4], (D, 4 * D), D ** -0.5, 0.1875, ((0, 32),))
    w_out = normal_values(streams_of[5], (D, D), D ** -0.5, 0.1875, ((0, 32),))
    gain_in = jnp.clip(1.0 + 0.15 * jax.random.normal(streams_of[6], (D,), jnp.float32), 0.25, 1.75)
    gain_out = jnp.clip(1.0 + 0.15 * jax.random.normal(streams_of[7], (D,), jnp.float32), 0.25, 1.75)
    bias_table = normal_values(streams_of[8], (H, NB), 1.0, 4.0, (), jnp.float32)
    return {"tokens": tokens, "cotangent": cotangent, "stamps": stamps, "lengths": lengths, "w_qkvu": w_qkvu, "w_out": w_out, "gain_in": gain_in, "gain_out": gain_out, "bias_table": bias_table}


EPS = 1e-05

def layer_norm(values, gain):
    average = lax.optimization_barrier(jnp.mean(values, axis=-1, keepdims=True))
    centred = values - average
    variance = lax.optimization_barrier(jnp.mean(centred * centred, axis=-1, keepdims=True))
    return centred * lax.rsqrt(variance + EPS) * gain

def silu_slope(values):
    sigmoid_v = jax.nn.sigmoid(values)
    return sigmoid_v * (1.0 + values * (1.0 - sigmoid_v))

def rounded(values):
    return lax.optimization_barrier(values.astype(jnp.bfloat16)).astype(jnp.float32)

def time_bias(bias_table, stamps_q, stamps_k):
    elapsed = stamps_q[:, None] - stamps_k[None, :]
    bucket = jnp.zeros(elapsed.shape, jnp.int32)
    for degree in range(1, bias_table.shape[1]):
        bucket = bucket + (elapsed >= 2 ** degree - 1).astype(jnp.int32)
    biases = jnp.zeros((bias_table.shape[0],) + elapsed.shape, jnp.float32)
    for degree in range(bias_table.shape[1]):
        biases = biases + jnp.where(bucket[None] == degree, bias_table[:, degree][:, None, None], 0.0)
    return biases

def one_stream(x_rows, cot_rows, stamp_row, length, w_qkvu, w_out, gain_in, gain_out, bias_table):
    scale = DH ** (-0.5)
    wide_rows = x_rows.astype(jnp.float32)
    normed = layer_norm(wide_rows, gain_in).astype(jnp.bfloat16)
    projected = jnp.dot(normed, w_qkvu, preferred_element_type=jnp.float32)
    activated = jax.nn.silu(projected)
    gate_u = activated[:, :D]
    v_heads = rounded(activated[:, D:2 * D]).reshape(SEQLEN, H, DH)
    q_heads = rounded(activated[:, 2 * D:3 * D]).reshape(SEQLEN, H, DH)
    k_heads = rounded(activated[:, 3 * D:]).reshape(SEQLEN, H, DH)
    positions = jnp.arange(SEQLEN, dtype=jnp.int32)
    live = positions < length
    allowed = (positions[None, :] <= positions[:, None]) & live[None, :] & live[:, None]
    scores = jnp.einsum('qhd,khd->hqk', q_heads, k_heads) * scale + time_bias(bias_table, stamp_row, stamp_row)
    weight = rounded(jnp.where(allowed[None], jax.nn.silu(scores), 0.0))
    attended = jnp.einsum('hqk,khd->qhd', weight, v_heads).reshape(SEQLEN, D)
    normed_att, norm_back = jax.vjp(lambda values: layer_norm(values, gain_out), attended)
    mixed_rows = (normed_att * gate_u).astype(jnp.bfloat16)
    mixed = (wide_rows + jnp.dot(mixed_rows, w_out, preferred_element_type=jnp.float32)).astype(jnp.bfloat16)
    w_grad = jnp.dot(mixed_rows.T, cot_rows, preferred_element_type=jnp.float32)
    d_mix = jnp.dot(cot_rows, w_out.T, preferred_element_type=jnp.float32)
    d_gate = d_mix * normed_att
    d_heads = rounded(norm_back(d_mix * gate_u)[0]).reshape(SEQLEN, H, DH)
    d_weight = jnp.einsum('qhd,khd->hqk', d_heads, v_heads)
    d_scores = rounded(jnp.where(allowed[None], d_weight * silu_slope(scores), 0.0))
    q_grad = jnp.einsum('hqk,khd->qhd', d_scores, k_heads) * scale
    scores_sh = d_scores.reshape(H, N_SEQ, TOK_DEV, SEQLEN)
    weight_sh = weight.reshape(H, N_SEQ, TOK_DEV, SEQLEN)
    q_sh = q_heads.reshape(N_SEQ, TOK_DEV, H, DH)
    d_sh = d_heads.reshape(N_SEQ, TOK_DEV, H, DH)
    k_parts = rounded(jnp.einsum('hsqk,sqhd->skhd', scores_sh, q_sh) * scale)
    v_parts = rounded(jnp.einsum('hsqk,sqhd->skhd', weight_sh, d_sh))
    k_grad = lax.optimization_barrier(jnp.sum(k_parts, axis=0)).reshape(SEQLEN, D)
    v_grad = lax.optimization_barrier(jnp.sum(v_parts, axis=0)).reshape(SEQLEN, D)
    d_act = jnp.concatenate([d_gate, v_grad, q_grad.reshape(SEQLEN, D), k_grad], axis=1)
    d_proj = (d_act * silu_slope(projected)).astype(jnp.bfloat16)
    d_normed = jnp.dot(d_proj, w_qkvu.T, preferred_element_type=jnp.float32)
    unused_rows, in_back = jax.vjp(lambda values: layer_norm(values, gain_in), wide_rows)
    input_grad = (cot_rows.astype(jnp.float32) + in_back(d_normed)[0]).astype(jnp.bfloat16)
    return (mixed, input_grad, w_grad)

def reference(tokens, cotangent, stamps, lengths, w_qkvu, w_out, gain_in, gain_out, bias_table):

    def visit(total, inputs):
        x_rows, cot_rows, stamp_row, length = inputs
        mixed, input_grad, w_grad = one_stream(x_rows, cot_rows, stamp_row, length, w_qkvu, w_out, gain_in, gain_out, bias_table)
        return (total + w_grad, (mixed, input_grad))
    w_total, outputs = lax.scan(visit, jnp.zeros((D, D), jnp.float32), (tokens, cotangent, stamps, lengths))
    return (outputs[0], outputs[1], w_total)
```

```python
import functools

import jax
import jax.numpy as jnp
from jax import lax
from jax.experimental import pallas as pl
from jax.experimental.pallas import tpu as pltpu
from jax.sharding import Mesh
from jax.sharding import PartitionSpec as P

H = 8
DH = 128
D = 1024
T = 128
S = 1024
NB = 16
TI = 256
CH = 32
DP = ("dp_0", "dp_1", "dp_2")
EPS = 1e-05
MSG = 144
F32 = jnp.float32
BF16 = jnp.bfloat16

VMEM = pl.BlockSpec(memory_space=pltpu.VMEM)
SMEM = pl.BlockSpec(memory_space=pltpu.SMEM)


def sigmoid(v):
    return 0.5 * jnp.tanh(0.5 * v) + 0.5


def nt(a, b):
    return lax.dot_general(a, b, (((1,), (1,)), ((), ())), preferred_element_type=F32)


def tn(a, b):
    return lax.dot_general(a, b, (((0,), (0,)), ((), ())), preferred_element_type=F32)


def mm(a, b):
    return jnp.dot(a, b, preferred_element_type=F32)


def norm_kernel(x_ref, gain_ref, a_ref, b_ref):
    x = x_ref[...].astype(F32)
    c = x - jnp.mean(x, axis=-1, keepdims=True)
    var = jnp.mean(c * c, axis=-1, keepdims=True)
    n = (c * lax.rsqrt(var + EPS) * gain_ref[...]).astype(BF16)
    a_ref[...] = n[:64]
    b_ref[...] = n[64:]


ARRIVALS = (
    [(0, 0), (0, 1)]
    + [(-k, 0) for k in (1, 2, 3, 4)]
    + [(-k, 1) for k in (1, 2, 3)]
    + [(k, 0) for k in (1, 2, 3)]
    + [(k, 1) for k in (1, 2, 3, 4)]
)


def forward_kernel(*refs):
    meta, bias_ref = refs[0], refs[1]
    blocks = refs[2:18]
    ws_ref, row_ref, col_ref = refs[18:21]
    msg_ref, proj_ref, w_ref, g_ref = refs[21:25]
    x_all, q_sc, k_sc, vt_sc, s_sc = refs[25:]
    me, length = meta[0], meta[1]
    for (far, half), blk in zip(ARRIVALS, blocks):
        at = lax.rem(me + far + H, H) * T + half * 64
        x_all[pl.ds(pl.multiple_of(at, 64), 64), :] = blk[...]
    proj = mm(x_all[...], ws_ref[...])
    proj_ref[...] = proj
    for c in range(8):
        rows = slice(c * T, (c + 1) * T)
        p = proj_ref[rows, :]
        a = p * sigmoid(p)
        vt_sc[:, rows] = a[:, :DH].T.astype(BF16)
        q_sc[rows, :] = a[:, DH : 2 * DH].astype(BF16)
        k_sc[rows, :] = a[:, 2 * DH :].astype(BF16)
    scale = DH ** (-0.5)
    levels = [bias_ref[me, b] for b in range(NB)]

    def tile(i0, j0, diagonal):
        s_sc[...] = nt(k_sc[pl.ds(j0, TI), :], q_sc[i0 : i0 + TI, :])
        for c in range(TI // CH):
            rows = pl.ds(j0 + c * CH, CH)
            e = row_ref[:, i0 : i0 + TI] - col_ref[rows, :]
            bias = jnp.full((CH, TI), levels[0], F32)
            for b in range(1, NB):
                bias = jnp.where(e >= 2**b - 1, levels[b], bias)
            s = s_sc[c * CH : (c + 1) * CH, :] * scale + bias
            sg = sigmoid(s)
            w = s * sg
            g = sg + w * (1.0 - sg)
            if diagonal:
                jj = lax.broadcasted_iota(jnp.int32, (CH, TI), 0) + c * CH
                ii = lax.broadcasted_iota(jnp.int32, (CH, TI), 1)
                keep = jj <= ii
                w = jnp.where(keep, w, 0.0)
                g = jnp.where(keep, g, 0.0)
            w_ref[rows, i0 : i0 + TI] = w.astype(BF16)
            g_ref[rows, i0 : i0 + TI] = g.astype(BF16)

    for bi in range(S // TI):
        i0 = bi * TI
        if bi:

            def below(bj, carry, i0=i0):
                tile(i0, pl.multiple_of(bj * TI, TI), False)
                return carry

            lax.fori_loop(0, bi, below, 0)
        tile(i0, i0, True)
        att = mm(vt_sc[:, : i0 + TI], w_ref[: i0 + TI, i0 : i0 + TI])
        pos = lax.broadcasted_iota(jnp.int32, (DH, TI), 1) + i0
        att = jnp.where(pos < length, att, 0.0)
        mean = jnp.mean(att, axis=0, keepdims=True)
        high = mean.astype(BF16)
        left = mean - high.astype(F32)
        mid = left.astype(BF16)
        low = (left - mid.astype(F32)).astype(BF16)
        kept = high.astype(F32) + mid.astype(F32) + low.astype(F32)
        centred = (att - kept).astype(BF16)
        which = lax.broadcasted_iota(jnp.int32, (16, TI), 0)
        tail = jnp.where(
            which == 0,
            high.astype(F32),
            jnp.where(which == 1, mid.astype(F32), jnp.where(which == 2, low.astype(F32), 0.0)),
        ).astype(BF16)
        for t in range(TI // T):
            dest = bi * (TI // T) + t
            msg_ref[dest, :DH, :] = centred[:, t * T : (t + 1) * T]
            msg_ref[dest, DH:, :] = tail[:, t * T : (t + 1) * T]


def tail_kernel(
    meta,
    msg_ref,
    na_ref,
    nb_ref,
    x_ref,
    cot_ref,
    wg_ref,
    wo_ref,
    gain_ref,
    mixed_ref,
    datt_ref,
    dpg_ref,
    wpart_ref,
    att_sc,
):
    me, length, core = meta[0], meta[1], meta[2]
    for h in range(H):
        blk = msg_ref[h].astype(F32)
        att_t = blk[:DH] + (blk[DH : DH + 1] + blk[DH + 1 : DH + 2] + blk[DH + 2 : DH + 3])
        att_sc[:, h * DH : (h + 1) * DH] = att_t.T
    pg = jnp.concatenate([mm(na_ref[...], wg_ref[...]), mm(nb_ref[...], wg_ref[...])], axis=0)
    cot = cot_ref[...]
    d_mix = nt(cot, wo_ref[...])
    att = att_sc[...]
    gain = gain_ref[...]
    c = att - jnp.mean(att, axis=-1, keepdims=True)
    var = jnp.mean(c * c, axis=-1, keepdims=True)
    r = lax.rsqrt(var + EPS)
    xhat = c * r
    normed_att = xhat * gain
    sg = sigmoid(pg)
    gate = pg * sg
    mixed_rows = (normed_att * gate).astype(BF16)
    mixed_ref[...] = (x_ref[...].astype(F32) + mm(mixed_rows, wo_ref[...])).astype(BF16)
    dpg_ref[...] = (d_mix * normed_att * (sg + gate * (1.0 - sg))).astype(BF16)
    u = d_mix * gate * gain
    d_att = r * (
        u
        - jnp.mean(u, axis=-1, keepdims=True)
        - xhat * jnp.mean(u * xhat, axis=-1, keepdims=True)
    )
    pos = lax.broadcasted_iota(jnp.int32, (T, D), 0) + me * T
    d_att = jnp.where(pos < length, d_att, 0.0).astype(BF16)
    for h in range(H):
        cols = slice(h * DH, (h + 1) * DH)
        datt_ref[h] = d_att[:, cols]
        part = tn(mixed_rows[:, cols], cot).astype(BF16)
        for t in range(4):
            side = lax.rem(core + t, 2)
            at = (2 * h + t // 2) * 32
            wpart_ref[side, at : at + 32, :] = part[t * 32 : (t + 1) * 32]


def backward_kernel(d_ref, proj_ref, w_ref, g_ref, out_ref, q_sc, k_sc, kt_sc, v_sc, ds_sc, dqt_sc):
    for c in range(8):
        rows = slice(c * T, (c + 1) * T)
        p = proj_ref[rows, :]
        a = p * sigmoid(p)
        v_sc[rows, :] = a[:, :DH].astype(BF16)
        q_sc[rows, :] = a[:, DH : 2 * DH].astype(BF16)
        k_sc[rows, :] = a[:, 2 * DH :].astype(BF16)
        kt_sc[:, rows] = a[:, 2 * DH :].T.astype(BF16)
    scale = DH ** (-0.5)
    d = d_ref[...].reshape(S, DH)
    for bj in range(S // TI):
        j0 = bj * TI
        rows = slice(j0, j0 + TI)
        dw = nt(v_sc[rows, :], d[j0:, :])
        ds_sc[rows, j0:] = (dw * g_ref[rows, j0:].astype(F32)).astype(BF16)
        dk = mm(ds_sc[rows, j0:], q_sc[j0:, :]) * scale
        dv = mm(w_ref[rows, j0:], d[j0:, :])
        for t in range(TI // T):
            at = slice(j0 + t * T, j0 + (t + 1) * T)
            dest = bj * (TI // T) + t
            for n, grad in ((0, dv), (2, dk)):
                p = proj_ref[at, n * DH : (n + 1) * DH]
                sg = sigmoid(p)
                slope = sg * (1.0 + p * (1.0 - sg))
                out_ref[dest, :, n * DH : (n + 1) * DH] = (
                    grad[t * T : (t + 1) * T] * slope
                ).astype(BF16)
    for bi in range(S // TI):
        i0 = bi * TI
        dqt_sc[:, i0 : i0 + TI] = (
            mm(kt_sc[:, : i0 + TI], ds_sc[: i0 + TI, i0 : i0 + TI]) * scale
        )
    for t in range(8):
        at = slice(t * T, (t + 1) * T)
        p = proj_ref[at, DH : 2 * DH]
        sg = sigmoid(p)
        slope = sg * (1.0 + p * (1.0 - sg))
        out_ref[t, :, DH : 2 * DH] = (dqt_sc[:, at].T * slope).astype(BF16)


def final_kernel(msg_ref, dpg_ref, w_ref, x_ref, cot_ref, gain_ref, out_ref, lhs, acc):
    b = pl.program_id(0)

    @pl.when(b == 0)
    def _():
        lhs[0] = dpg_ref[...]
        for n in range(3):
            for h in range(H):
                lhs[n + 1, :, h * DH : (h + 1) * DH] = msg_ref[h, :, n * DH : (n + 1) * DH]
        acc[...] = jnp.zeros_like(acc)

    acc[...] += nt(lhs[b], w_ref[...])

    @pl.when(b == 3)
    def _():
        x = x_ref[...].astype(F32)
        c = x - jnp.mean(x, axis=-1, keepdims=True)
        var = jnp.mean(c * c, axis=-1, keepdims=True)
        r = lax.rsqrt(var + EPS)
        xhat = c * r
        u = acc[...] * gain_ref[...]
        dx = r * (
            u
            - jnp.mean(u, axis=-1, keepdims=True)
            - xhat * jnp.mean(u * xhat, axis=-1, keepdims=True)
        )
        out_ref[...] = (cot_ref[...].astype(F32) + dx).astype(BF16)


def sum_kernel(meta, *refs):
    shares, out_ref, held = refs[:H], refs[H], refs[H + 1]
    for k in range(H):
        held[lax.rem(meta[0] - k + H, H)] = shares[k][...].astype(F32)
    total = held[0]
    for k in range(1, H):
        total = total + held[k]
    out_ref[...] = total


def params(**more):
    return pltpu.CompilerParams(vmem_limit_bytes=48 * 1024 * 1024, **more)


def cost(us):
    flops = int(us * 4.0e6)
    return pl.CostEstimate(flops=flops, bytes_accessed=1 << 20, transcendentals=0)


def shifted(value, by):
    return lax.ppermute(value, "seq", [(i, (i + by) % H) for i in range(H)])


def per_device(tokens, cotangent, stamps, lengths, w_qkvu, w_out, gain_in, gain_out, bias_table):
    x = tokens[0]
    cot = cotangent[0]
    me = lax.axis_index("seq")
    core = lax.axis_index("dp_2")
    meta = jnp.stack([me, lengths[0], core]).astype(jnp.int32)
    gain_in = gain_in.reshape(1, D)
    gain_out = gain_out.reshape(1, D)
    stamp_row = stamps
    stamp_col = stamps.reshape(S, 1)

    w_full = lax.all_gather(jnp.concatenate([w_qkvu, w_out], axis=1), DP, axis=0, tiled=True)

    na, nb = pl.pallas_call(
        norm_kernel,
        out_shape=[jax.ShapeDtypeStruct((64, D), BF16)] * 2,
        in_specs=[VMEM, VMEM],
        out_specs=[VMEM, VMEM],
        compiler_params=params(),
        cost_estimate=cost(1),
        name="norm",
    )(x, gain_in)

    head_w = jnp.concatenate(
        [
            lax.dynamic_slice_in_dim(w_qkvu, part * D + me * DH, DH, axis=1)
            for part in (1, 2, 3)
        ],
        axis=1,
    )
    ws = lax.all_to_all(
        jnp.broadcast_to(head_w[None], (32, *head_w.shape)), DP, 0, 0, tiled=True
    ).reshape(D, 3 * DH)

    arrived = {(0, 0): na, (0, 1): nb}
    for k in range(1, 5):
        arrived[(-k, 0)] = shifted(arrived[(1 - k, 0)], 1)
        arrived[(k, 1)] = shifted(arrived[(k - 1, 1)], -1)
        if k < 4:
            arrived[(-k, 1)] = shifted(arrived[(1 - k, 1)], 1)
            arrived[(k, 0)] = shifted(arrived[(k - 1, 0)], -1)

    msg, proj, weight, slope = pl.pallas_call(
        forward_kernel,
        out_shape=[
            jax.ShapeDtypeStruct((H, MSG, T), BF16),
            jax.ShapeDtypeStruct((S, 3 * DH), F32),
            jax.ShapeDtypeStruct((S, S), BF16),
            jax.ShapeDtypeStruct((S, S), BF16),
        ],
        in_specs=[SMEM, SMEM] + [VMEM] * 19,
        out_specs=[VMEM] * 4,
        scratch_shapes=[
            pltpu.VMEM((S, D), BF16),
            pltpu.VMEM((S, DH), BF16),
            pltpu.VMEM((S, DH), BF16),
            pltpu.VMEM((DH, S), BF16),
            pltpu.VMEM((TI, TI), F32),
        ],
        compiler_params=params(),
        cost_estimate=cost(10),
        name="attend",
    )(meta, bias_table, *[arrived[a] for a in ARRIVALS], ws, stamp_row, stamp_col)

    att_msg = lax.all_to_all(msg, "seq", 0, 0, tiled=True)

    mixed, d_att, d_pg, w_part = pl.pallas_call(
        tail_kernel,
        grid=(1,),
        out_shape=[
            jax.ShapeDtypeStruct((T, D), BF16),
            jax.ShapeDtypeStruct((H, T, DH), BF16),
            jax.ShapeDtypeStruct((T, D), BF16),
            jax.ShapeDtypeStruct((2, D // 2, D), BF16),
        ],
        in_specs=[
            SMEM,
            VMEM,
            VMEM,
            VMEM,
            VMEM,
            VMEM,
            pl.BlockSpec((D, D), lambda i: (0, 0)),
            pl.BlockSpec((D, D), lambda i: (0, 4)),
            VMEM,
        ],
        out_specs=[VMEM] * 4,
        scratch_shapes=[pltpu.VMEM((T, D), F32)],
        compiler_params=params(),
        cost_estimate=cost(8),
        name="tail",
    )(meta, att_msg, na, nb, x, cot, w_full, w_full, gain_out)

    d_all = lax.all_to_all(d_att, "seq", 0, 0, tiled=True)

    other = lax.ppermute(w_part[1], "dp_2", [(0, 1), (1, 0)])
    pair = (w_part[0].astype(F32) + other.astype(F32)).astype(BF16)
    planes = lax.all_to_all(pair.reshape(16, 32, D), ("dp_0", "dp_1"), 0, 0, tiled=True)
    own = jnp.sum(planes.astype(F32), axis=0).astype(BF16)
    shares = [own] + [shifted(own, k) for k in range(1, H)]
    w_grad = pl.pallas_call(
        sum_kernel,
        out_shape=jax.ShapeDtypeStruct((32, D), F32),
        in_specs=[SMEM] + [VMEM] * H,
        out_specs=VMEM,
        scratch_shapes=[pltpu.VMEM((H, 32, D), F32)],
        compiler_params=params(),
        cost_estimate=cost(1),
        name="share_sum",
    )(meta, *shares)

    d_proj = pl.pallas_call(
        backward_kernel,
        out_shape=jax.ShapeDtypeStruct((H, T, 3 * DH), BF16),
        in_specs=[VMEM] * 4,
        out_specs=VMEM,
        scratch_shapes=[
            pltpu.VMEM((S, DH), BF16),
            pltpu.VMEM((S, DH), BF16),
            pltpu.VMEM((DH, S), BF16),
            pltpu.VMEM((S, DH), BF16),
            pltpu.VMEM((S, S), BF16),
            pltpu.VMEM((DH, S), F32),
        ],
        compiler_params=params(),
        cost_estimate=cost(8),
        name="attend_back",
    )(d_all, proj, weight, slope)

    d_rows = lax.all_to_all(d_proj, "seq", 0, 0, tiled=True)

    input_grad = pl.pallas_call(
        final_kernel,
        grid=(4,),
        out_shape=jax.ShapeDtypeStruct((T, D), BF16),
        in_specs=[
            VMEM,
            VMEM,
            pl.BlockSpec((D, D), lambda b: (0, b)),
            VMEM,
            VMEM,
            VMEM,
        ],
        out_specs=VMEM,
        scratch_shapes=[pltpu.VMEM((4, T, D), BF16), pltpu.VMEM((T, D), F32)],
        compiler_params=params(dimension_semantics=("arbitrary",)),
        cost_estimate=cost(8),
        name="final",
    )(d_rows, d_pg, w_full, x, cot, gain_in)

    return (mixed[None], input_grad[None], w_grad)


def solution(mesh):
    finer = Mesh(mesh.devices.reshape(4, 4, 2, mesh.shape["seq"]), (*DP, "seq"))
    placed = (
        P(DP, "seq", None),
        P(DP, "seq", None),
        P(DP, None),
        P(DP),
        P(DP, None),
        P(DP, None),
        P(),
        P(),
        P(),
    )
    return jax.shard_map(
        per_device,
        mesh=finer,
        in_specs=placed,
        out_specs=(P(DP, "seq", None), P(DP, "seq", None), P(DP, None)),
        check_vma=False,
    )
```

```python
import jax
import jax.numpy as jnp
from jax import lax
from jax.experimental import pallas as pl
from jax.experimental.pallas import tpu as pltpu
from jax.sharding import Mesh
from jax.sharding import PartitionSpec as P


H = 8
DH = 128
D = 1024
T = 128
S = 1024
NB = 16
TI = 256
CH = 32
DP = ("dp_0", "dp_1", "dp_2")
EPS = 1e-05
MSG = 144
F32 = jnp.float32
BF16 = jnp.bfloat16

VMEM = pl.BlockSpec(memory_space=pltpu.VMEM)
SMEM = pl.BlockSpec(memory_space=pltpu.SMEM)
HBM = pl.BlockSpec(memory_space=pltpu.HBM)


def sigmoid(v):
    return 0.5 * jnp.tanh(0.5 * v) + 0.5


def nt(a, b):
    return lax.dot_general(a, b, (((1,), (1,)), ((), ())), preferred_element_type=F32)


def tn(a, b):
    return lax.dot_general(a, b, (((0,), (0,)), ((), ())), preferred_element_type=F32)


def mm(a, b):
    return jnp.dot(a, b, preferred_element_type=F32)


def norm_kernel(x_ref, gain_ref, a_ref, b_ref):
    x = x_ref[...].astype(F32)
    c = x - jnp.mean(x, axis=-1, keepdims=True)
    var = jnp.mean(c * c, axis=-1, keepdims=True)
    n = (c * lax.rsqrt(var + EPS) * gain_ref[...]).astype(BF16)
    a_ref[...] = n[:64]
    b_ref[...] = n[64:]


ARRIVALS = (
    [(0, 0), (0, 1)]
    + [(-k, 0) for k in (1, 2, 3, 4)]
    + [(-k, 1) for k in (1, 2, 3)]
    + [(k, 0) for k in (1, 2, 3)]
    + [(k, 1) for k in (1, 2, 3, 4)]
)


def forward_kernel(*refs):
    meta, bias_ref = refs[0], refs[1]
    blocks = refs[2:18]
    ws_hbm, row_ref = refs[18:20]
    msg_out, proj_out, w_out, g_out = refs[20:24]
    (
        x_all, ws_ref, col_sc, q_sc, k_sc, vt_sc, s_sc, msg_ref, proj_ref, w_ref, g_ref,
        in_sem, ws_sem, out_sem, proj_sem,
    ) = refs[24:]
    me, length = meta[0], meta[1]
    fetches = [pltpu.make_async_copy(ws_hbm, ws_ref, ws_sem)]
    for n, ((far, half), blk) in enumerate(zip(ARRIVALS, blocks)):
        at = lax.rem(me + far + H, H) * T + half * 64
        fetches.append(
            pltpu.make_async_copy(
                blk, x_all.at[pl.ds(pl.multiple_of(at, 64), 64), :], in_sem.at[n]
            )
        )
    for fetch in fetches:
        fetch.start()
    for c in range(8):
        cols = slice(c * T, (c + 1) * T)
        col_sc[cols, :] = jnp.broadcast_to(row_ref[:, cols], (T, T)).T
    for fetch in fetches:
        fetch.wait()
    proj_ref[...] = mm(x_all[...], ws_ref[...])
    store_proj = pltpu.make_async_copy(proj_ref, proj_out, proj_sem)
    store_proj.start()
    for c in range(8):
        rows = slice(c * T, (c + 1) * T)
        p = proj_ref[rows, :]
        a = p * sigmoid(p)
        vt_sc[:, rows] = a[:, :DH].T.astype(BF16)
        q_sc[rows, :] = a[:, DH : 2 * DH].astype(BF16)
        k_sc[rows, :] = a[:, 2 * DH :].astype(BF16)
    scale = DH ** (-0.5)
    levels = [bias_ref[me, b] for b in range(NB)]

    def tile(i0, j0, diagonal):
        s_sc[...] = nt(k_sc[pl.ds(j0, TI), :], q_sc[i0 : i0 + TI, :])

        def chunk(c, carry):
            at = pl.multiple_of(c * CH, CH)
            rows = pl.ds(pl.multiple_of(j0 + at, CH), CH)
            col = col_sc[rows, :]
            e = row_ref[:, i0 : i0 + TI] - jnp.concatenate([col, col], axis=1)
            bias = jnp.full((CH, TI), levels[0], F32)
            for b in range(1, NB):
                bias = jnp.where(e >= float(2**b - 1), levels[b], bias)
            s = s_sc[pl.ds(at, CH), :] * scale + bias
            sg = sigmoid(s)
            w = s * sg
            g = sg + w * (1.0 - sg)
            if diagonal:
                jj = lax.broadcasted_iota(jnp.int32, (CH, TI), 0) + at
                ii = lax.broadcasted_iota(jnp.int32, (CH, TI), 1)
                keep = jj <= ii
                w = jnp.where(keep, w, 0.0)
                g = jnp.where(keep, g, 0.0)
            w_ref[rows, i0 : i0 + TI] = w.astype(BF16)
            g_ref[rows, i0 : i0 + TI] = g.astype(BF16)
            return carry

        lax.fori_loop(0, TI // CH, chunk, 0, unroll=2)

    stores = []
    for bi in range(S // TI):
        i0 = bi * TI
        if bi:

            def below(bj, carry, i0=i0):
                tile(i0, pl.multiple_of(bj * TI, TI), False)
                return carry

            lax.fori_loop(0, bi, below, 0)
        tile(i0, i0, True)
        att = mm(vt_sc[:, : i0 + TI], w_ref[: i0 + TI, i0 : i0 + TI])
        pos = lax.broadcasted_iota(jnp.int32, (DH, TI), 1) + i0
        att = jnp.where(pos < length, att, 0.0)
        mean = jnp.mean(att, axis=0, keepdims=True)
        high = mean.astype(BF16)
        left = mean - high.astype(F32)
        mid = left.astype(BF16)
        low = (left - mid.astype(F32)).astype(BF16)
        kept = high.astype(F32) + mid.astype(F32) + low.astype(F32)
        centred = (att - kept).astype(BF16)
        which = lax.broadcasted_iota(jnp.int32, (16, TI), 0)
        tail = jnp.where(
            which == 0,
            high.astype(F32),
            jnp.where(which == 1, mid.astype(F32), jnp.where(which == 2, low.astype(F32), 0.0)),
        ).astype(BF16)
        for t in range(TI // T):
            dest = bi * (TI // T) + t
            msg_ref[dest, :DH, :] = centred[:, t * T : (t + 1) * T]
            msg_ref[dest, DH:, :] = tail[:, t * T : (t + 1) * T]
        done = pl.ds(0, i0 + TI), pl.ds(i0, TI)
        some = pl.ds(bi * (TI // T), TI // T)
        for n, (src, dst, view) in enumerate(
            ((w_ref, w_out, done), (g_ref, g_out, done), (msg_ref, msg_out, (some,)))
        ):
            stores.append(
                pltpu.make_async_copy(src.at[view], dst.at[view], out_sem.at[3 * bi + n])
            )
            stores[-1].start()
    for store in stores:
        store.wait()
    store_proj.wait()


def tail_kernel(
    meta,
    msg_hbm,
    na_ref,
    nb_ref,
    cot_ref,
    early_hbm,
    gain_ref,
    datt_out,
    rows_ref,
    dpg_ref,
    att_sc,
    wg_ref,
    wo_ref,
    msg_ref,
    datt_ref,
    sems,
):
    me, length = meta[0], meta[1]
    fetch_msg = pltpu.make_async_copy(msg_hbm, msg_ref, sems.at[0])
    fetch_wo = pltpu.make_async_copy(early_hbm.at[:, pl.ds(D, D)], wo_ref, sems.at[1])
    fetch_wg = pltpu.make_async_copy(early_hbm.at[:, pl.ds(0, D)], wg_ref, sems.at[2])
    fetch_msg.start()
    fetch_wo.start()
    fetch_wg.start()
    fetch_msg.wait()
    for h in range(H):
        blk = msg_ref[h].astype(F32)
        att_t = blk[:DH] + (blk[DH : DH + 1] + blk[DH + 1 : DH + 2] + blk[DH + 2 : DH + 3])
        att_sc[:, h * DH : (h + 1) * DH] = att_t.T
    fetch_wo.wait()
    d_mix = nt(cot_ref[...], wo_ref[...])
    fetch_wg.wait()
    pg = jnp.concatenate([mm(na_ref[...], wg_ref[...]), mm(nb_ref[...], wg_ref[...])], axis=0)
    att = att_sc[...]
    gain = gain_ref[...]
    c = att - jnp.mean(att, axis=-1, keepdims=True)
    var = jnp.mean(c * c, axis=-1, keepdims=True)
    r = lax.rsqrt(var + EPS)
    xhat = c * r
    normed_att = xhat * gain
    sg = sigmoid(pg)
    gate = pg * sg
    rows_ref[...] = (normed_att * gate).astype(BF16)
    dpg_ref[...] = (d_mix * normed_att * (sg + gate * (1.0 - sg))).astype(BF16)
    u = d_mix * gate * gain
    d_att = r * (
        u
        - jnp.mean(u, axis=-1, keepdims=True)
        - xhat * jnp.mean(u * xhat, axis=-1, keepdims=True)
    )
    pos = lax.broadcasted_iota(jnp.int32, (T, D), 0) + me * T
    d_att = jnp.where(pos < length, d_att, 0.0).astype(BF16)
    for h in range(H):
        datt_ref[h] = d_att[:, h * DH : (h + 1) * DH]
    store = pltpu.make_async_copy(datt_ref, datt_out, sems.at[3])
    store.start()
    store.wait()


def output_kernel(
    meta, rows_ref, dpg_ref, x_ref, cot_ref, early_hbm, mixed_ref, back_ref, own_out, send_out,
    wg_ref, wo_ref, part_sc, sems,
):
    core = meta[2]
    fetch_wo = pltpu.make_async_copy(early_hbm.at[:, pl.ds(D, D)], wo_ref, sems.at[0])
    fetch_wg = pltpu.make_async_copy(early_hbm.at[:, pl.ds(0, D)], wg_ref, sems.at[1])
    fetch_wo.start()
    fetch_wg.start()
    cot = cot_ref[...]
    mixed_rows = rows_ref[...]

    def head(h, carry):
        part = tn(rows_ref[:, pl.ds(pl.multiple_of(h * DH, DH), DH)], cot).astype(BF16)
        for t in range(4):
            side = lax.rem(core + t, 2)
            at = pl.multiple_of((2 * h + t // 2) * 32, 32)
            part_sc[side, pl.ds(at, 32), :] = part[t * 32 : (t + 1) * 32]
        return carry

    lax.fori_loop(0, H, head, 0)
    stores = [
        pltpu.make_async_copy(part_sc.at[0], own_out, sems.at[2]),
        pltpu.make_async_copy(part_sc.at[1], send_out, sems.at[3]),
    ]
    for store in stores:
        store.start()
    fetch_wo.wait()
    mixed_ref[...] = (x_ref[...].astype(F32) + mm(mixed_rows, wo_ref[...])).astype(BF16)
    fetch_wg.wait()
    back_ref[...] = nt(dpg_ref[...], wg_ref[...])
    for store in stores:
        store.wait()


def backward_kernel(*refs):
    meta, d_hbm, proj_hbm, w_hbm, g_hbm = refs[:5]
    outs = refs[5:13]
    (
        d_ref, proj_ref, w_ref, g_ref, q_sc, k_sc, kt_sc, v_sc, ds_sc, dqt_sc, out_ref,
        sems, out_sem,
    ) = refs[13:]
    me = meta[0]
    fetch_proj = pltpu.make_async_copy(proj_hbm, proj_ref, sems.at[0])
    fetch_d = pltpu.make_async_copy(d_hbm, d_ref, sems.at[1])
    fetch_proj.start()
    fetch_d.start()
    fetches = []
    for bj in range(S // TI):
        view = pl.ds(bj * TI, TI), pl.ds(bj * TI, S - bj * TI)
        pair = (
            pltpu.make_async_copy(g_hbm.at[view], g_ref.at[view], sems.at[2 + 2 * bj]),
            pltpu.make_async_copy(w_hbm.at[view], w_ref.at[view], sems.at[3 + 2 * bj]),
        )
        pair[0].start()
        pair[1].start()
        fetches.append(pair)
    fetch_proj.wait()
    for c in range(8):
        rows = slice(c * T, (c + 1) * T)
        p = proj_ref[rows, :]
        a = p * sigmoid(p)
        v_sc[rows, :] = a[:, :DH].astype(BF16)
        q_sc[rows, :] = a[:, DH : 2 * DH].astype(BF16)
        k_sc[rows, :] = a[:, 2 * DH :].astype(BF16)
        kt_sc[:, rows] = a[:, 2 * DH :].T.astype(BF16)
    scale = DH ** (-0.5)
    fetch_d.wait()
    d = d_ref[...].reshape(S, DH)
    for bj in range(S // TI):
        j0 = bj * TI
        rows = slice(j0, j0 + TI)
        dw = nt(v_sc[rows, :], d[j0:, :])
        fetches[bj][0].wait()
        ds_sc[rows, j0:] = (dw * g_ref[rows, j0:].astype(F32)).astype(BF16)
        dk = mm(ds_sc[rows, j0:], q_sc[j0:, :]) * scale
        fetches[bj][1].wait()
        dv = mm(w_ref[rows, j0:], d[j0:, :])
        for t in range(TI // T):
            at = slice(j0 + t * T, j0 + (t + 1) * T)
            dest = bj * (TI // T) + t
            for n, grad in ((0, dv), (2, dk)):
                p = proj_ref[at, n * DH : (n + 1) * DH]
                sg = sigmoid(p)
                slope = sg * (1.0 + p * (1.0 - sg))
                out_ref[dest, :, n * DH : (n + 1) * DH] = (
                    grad[t * T : (t + 1) * T] * slope
                ).astype(BF16)
    for bi in range(S // TI):
        i0 = bi * TI
        dqt_sc[:, i0 : i0 + TI] = (
            mm(kt_sc[:, : i0 + TI], ds_sc[: i0 + TI, i0 : i0 + TI]) * scale
        )
    for t in range(8):
        at = slice(t * T, (t + 1) * T)
        p = proj_ref[at, DH : 2 * DH]
        sg = sigmoid(p)
        slope = sg * (1.0 + p * (1.0 - sg))
        out_ref[t, :, DH : 2 * DH] = (dqt_sc[:, at].T * slope).astype(BF16)
    stores = [
        pltpu.make_async_copy(out_ref.at[lax.rem(me + k, H)], outs[k], out_sem.at[k])
        for k in range(H)
    ]
    for store in stores:
        store.start()
    for store in stores:
        store.wait()


def final_kernel(*refs):
    meta = refs[0]
    blocks = refs[1:9]
    back_ref, late_hbm, x_ref, cot_ref, gain_ref, out_ref = refs[9:15]
    msg_ref, lhs, late_ref, acc, sems, w_sems = refs[15:]
    me = meta[0]
    fetches = [
        pltpu.make_async_copy(blocks[k], msg_ref.at[lax.rem(me - k + H, H)], sems.at[k])
        for k in range(H)
    ]
    weights = []
    for n in range(3):
        view = slice(None), pl.ds(n * D, D)
        weights.append(
            pltpu.make_async_copy(late_hbm.at[view], late_ref.at[n], w_sems.at[n])
        )
    for fetch in fetches:
        fetch.start()
    for fetch in weights:
        fetch.start()
    for fetch in fetches:
        fetch.wait()
    for n in range(3):
        for h in range(H):
            lhs[n, :, h * DH : (h + 1) * DH] = msg_ref[h, :, n * DH : (n + 1) * DH]
    acc[...] = back_ref[...]
    for n in range(3):
        weights[n].wait()

        def columns(c, carry, n=n):
            at = pl.ds(pl.multiple_of(c * 256, 256), 256)
            acc[:, at] += nt(lhs[n], late_ref[n, at, :])
            return carry

        lax.fori_loop(0, D // 256, columns, 0)
    d_normed = acc[...]
    x = x_ref[...].astype(F32)
    c = x - jnp.mean(x, axis=-1, keepdims=True)
    var = jnp.mean(c * c, axis=-1, keepdims=True)
    r = lax.rsqrt(var + EPS)
    xhat = c * r
    u = d_normed * gain_ref[...]
    dx = r * (
        u
        - jnp.mean(u, axis=-1, keepdims=True)
        - xhat * jnp.mean(u * xhat, axis=-1, keepdims=True)
    )
    out_ref[...] = (cot_ref[...].astype(F32) + dx).astype(BF16)


def params(**more):
    return pltpu.CompilerParams(vmem_limit_bytes=60 * 1024 * 1024, **more)


def cost(us):
    flops = int(us * 3.0e8)
    return pl.CostEstimate(flops=flops, bytes_accessed=1 << 20, transcendentals=0)


def paired(value, axis, mask):
    count = lax.axis_size(axis)
    return lax.ppermute(value, axis, [(i, i ^ mask) for i in range(count)])


def shifted(value, by):
    return lax.ppermute(value, "seq", [(i, (i + by) % H) for i in range(H)])


def layer(tokens, cotangent, stamps, lengths, w_qkvu, w_out, gain_in, gain_out, bias_table):
    x = tokens[0]
    cot = cotangent[0]
    me = lax.axis_index("seq")
    core = lax.axis_index("dp_2")
    meta = jnp.stack([me, lengths[0], core]).astype(jnp.int32)
    gain_in = gain_in.reshape(1, D)
    gain_out = gain_out.reshape(1, D)
    stamp_row = stamps.astype(F32)

    w_early = lax.all_gather(
        jnp.concatenate([w_qkvu[:, :D], w_out], axis=1), DP, axis=0, tiled=True
    )
    w_late = lax.all_gather(w_qkvu[:, D:], DP, axis=0, tiled=True)

    na, nb = pl.pallas_call(
        norm_kernel,
        out_shape=[jax.ShapeDtypeStruct((64, D), BF16)] * 2,
        in_specs=[VMEM, VMEM],
        out_specs=[VMEM, VMEM],
        compiler_params=params(),
        cost_estimate=cost(1),
        name="norm",
    )(x, gain_in)

    head_w = jnp.concatenate(
        [
            lax.dynamic_slice_in_dim(w_qkvu, part * D + me * DH, DH, axis=1)
            for part in (1, 2, 3)
        ],
        axis=1,
    )
    copies = jnp.broadcast_to(head_w[None], (32, *head_w.shape))
    ws = lax.all_to_all(copies, DP, 0, 0, tiled=True)
    ws = ws.reshape(D, 3 * DH)

    arrived = {(0, 0): na, (0, 1): nb}
    for k in range(1, 5):
        arrived[(-k, 0)] = shifted(arrived[(1 - k, 0)], 1)
        arrived[(k, 1)] = shifted(arrived[(k - 1, 1)], -1)
        if k < 4:
            arrived[(-k, 1)] = shifted(arrived[(1 - k, 1)], 1)
            arrived[(k, 0)] = shifted(arrived[(k - 1, 0)], -1)

    dma = pltpu.SemaphoreType.DMA
    msg, proj, weight, slope = pl.pallas_call(
        forward_kernel,
        out_shape=[
            jax.ShapeDtypeStruct((H, MSG, T), BF16),
            jax.ShapeDtypeStruct((S, 3 * DH), F32),
            jax.ShapeDtypeStruct((S, S), BF16),
            jax.ShapeDtypeStruct((S, S), BF16),
        ],
        in_specs=[SMEM, SMEM] + [HBM] * 17 + [VMEM],
        out_specs=[HBM] * 4,
        scratch_shapes=[
            pltpu.VMEM((S, D), BF16),
            pltpu.VMEM((D, 3 * DH), BF16),
            pltpu.VMEM((S, T), F32),
            pltpu.VMEM((S, DH), BF16),
            pltpu.VMEM((S, DH), BF16),
            pltpu.VMEM((DH, S), BF16),
            pltpu.VMEM((TI, TI), F32),
            pltpu.VMEM((H, MSG, T), BF16),
            pltpu.VMEM((S, 3 * DH), F32),
            pltpu.VMEM((S, S), BF16),
            pltpu.VMEM((S, S), BF16),
            dma((16,)),
            dma,
            dma((12,)),
            dma,
        ],
        compiler_params=params(),
        cost_estimate=cost(10),
        name="attend",
    )(meta, bias_table, *[arrived[a] for a in ARRIVALS], ws, stamp_row)

    att_msg = lax.all_to_all(msg, "seq", 0, 0, tiled=True)

    d_att, mixed_rows, d_pg = pl.pallas_call(
        tail_kernel,
        out_shape=[
            jax.ShapeDtypeStruct((H, T, DH), BF16),
            jax.ShapeDtypeStruct((T, D), BF16),
            jax.ShapeDtypeStruct((T, D), BF16),
        ],
        in_specs=[SMEM, HBM, VMEM, VMEM, VMEM, HBM, VMEM],
        out_specs=[HBM, VMEM, VMEM],
        scratch_shapes=[
            pltpu.VMEM((T, D), F32),
            pltpu.VMEM((D, D), BF16),
            pltpu.VMEM((D, D), BF16),
            pltpu.VMEM((H, MSG, T), BF16),
            pltpu.VMEM((H, T, DH), BF16),
            dma((4,)),
        ],
        compiler_params=params(),
        cost_estimate=cost(5),
        name="tail",
    )(meta, att_msg, na, nb, cot, w_early, gain_out)

    d_all = lax.all_to_all(d_att, "seq", 0, 0, tiled=True)

    outputs = pl.pallas_call(
        output_kernel,
        out_shape=[
            jax.ShapeDtypeStruct((T, D), BF16),
            jax.ShapeDtypeStruct((T, D), F32),
            jax.ShapeDtypeStruct((D // 2, D), BF16),
            jax.ShapeDtypeStruct((D // 2, D), BF16),
        ],
        in_specs=[SMEM, VMEM, VMEM, VMEM, VMEM, HBM],
        out_specs=[VMEM, VMEM, HBM, HBM],
        scratch_shapes=[
            pltpu.VMEM((D, D), BF16),
            pltpu.VMEM((D, D), BF16),
            pltpu.VMEM((2, D // 2, D), BF16),
            dma((4,)),
        ],
        compiler_params=params(),
        cost_estimate=cost(4),
        name="outputs",
    )
    mixed, gate_back, w_own_part, w_send = outputs(meta, mixed_rows, d_pg, x, cot, w_early)

    other = paired(w_send, "dp_2", 1)
    pair = (w_own_part.astype(F32) + other.astype(F32)).astype(BF16)
    pair, d_all = lax.optimization_barrier((pair, d_all))
    planes = lax.all_to_all(pair.reshape(16, 32, D), ("dp_0", "dp_1"), 0, 0, tiled=True)

    attend_back = pl.pallas_call(
        backward_kernel,
        out_shape=[jax.ShapeDtypeStruct((T, 3 * DH), BF16)] * H,
        in_specs=[SMEM] + [HBM] * 4,
        out_specs=[HBM] * H,
        scratch_shapes=[
            pltpu.VMEM((H, T, DH), BF16),
            pltpu.VMEM((S, 3 * DH), F32),
            pltpu.VMEM((S, S), BF16),
            pltpu.VMEM((S, S), BF16),
            pltpu.VMEM((S, DH), BF16),
            pltpu.VMEM((S, DH), BF16),
            pltpu.VMEM((DH, S), BF16),
            pltpu.VMEM((S, DH), BF16),
            pltpu.VMEM((S, S), BF16),
            pltpu.VMEM((DH, S), F32),
            pltpu.VMEM((H, T, 3 * DH), BF16),
            dma((10,)),
            dma((H,)),
        ],
        compiler_params=params(),
        cost_estimate=cost(6),
        name="attend_back",
    )
    d_proj = attend_back(meta, d_all, proj, weight, slope)

    total = jnp.sum(planes.astype(F32), axis=0)
    for mask in (1, 3, 7):
        own = total.astype(BF16)
        far = paired(own, "seq", mask)
        total = own.astype(F32) + far.astype(F32)
    w_grad = total

    d_rows = {0: d_proj[0]}
    for k in (4, 5, 3, 6, 2, 7, 1):
        d_rows[k] = shifted(d_proj[k], k)

    final = pl.pallas_call(
        final_kernel,
        out_shape=jax.ShapeDtypeStruct((T, D), BF16),
        in_specs=[SMEM] + [HBM] * H + [VMEM, HBM, VMEM, VMEM, VMEM],
        out_specs=VMEM,
        scratch_shapes=[
            pltpu.VMEM((H, T, 3 * DH), BF16),
            pltpu.VMEM((3, T, D), BF16),
            pltpu.VMEM((3, D, D), BF16),
            pltpu.VMEM((T, D), F32),
            dma((H,)),
            dma((3,)),
        ],
        compiler_params=params(),
        cost_estimate=cost(5),
        name="final",
    )
    input_grad = final(
        meta, *[d_rows[k] for k in range(H)], gate_back, w_late, x, cot, gain_in
    )

    return (mixed[None], input_grad[None], w_grad)


def solution(mesh):
    finer = Mesh(mesh.devices.reshape(4, 4, 2, mesh.shape["seq"]), (*DP, "seq"))
    placed = (
        P(DP, "seq", None),
        P(DP, "seq", None),
        P(DP, None),
        P(DP),
        P(DP, None),
        P(DP, None),
        P(),
        P(),
        P(),
    )
    return jax.shard_map(
        layer,
        mesh=finer,
        in_specs=placed,
        out_specs=(P(DP, "seq", None), P(DP, "seq", None), P(DP, None)),
        check_vma=False,
    )
```

```python
import jax
import jax.numpy as jnp
from jax import lax
from jax.experimental import pallas as pl
from jax.experimental.pallas import tpu as pltpu
from jax.sharding import Mesh
from jax.sharding import PartitionSpec as P


H = 8
DH = 128
D = 1024
T = 128
S = 1024
NB = 16
TI = 256
CH = 32
DP = ("dp_0", "dp_1", "dp_2")
EPS = 1e-05
MSG = 144
LIMIT = 48000
F32 = jnp.float32
BF16 = jnp.bfloat16

VMEM = pl.BlockSpec(memory_space=pltpu.VMEM)
SMEM = pl.BlockSpec(memory_space=pltpu.SMEM)


def sigmoid(v):
    return 0.5 * jnp.tanh(0.5 * v) + 0.5


def nt(a, b):
    return lax.dot_general(a, b, (((1,), (1,)), ((), ())), preferred_element_type=F32)


def tn(a, b):
    return lax.dot_general(a, b, (((0,), (0,)), ((), ())), preferred_element_type=F32)


def mm(a, b):
    return jnp.dot(a, b, preferred_element_type=F32)


def norm_kernel(x_ref, gain_ref, a_ref, b_ref):
    x = x_ref[...].astype(F32)
    c = x - jnp.mean(x, axis=-1, keepdims=True)
    var = jnp.mean(c * c, axis=-1, keepdims=True)
    n = (c * lax.rsqrt(var + EPS) * gain_ref[...]).astype(BF16)
    a_ref[...] = n[:64]
    b_ref[...] = n[64:]


ARRIVALS = (
    [(0, 0), (0, 1)]
    + [(-k, 0) for k in (1, 2, 3, 4)]
    + [(-k, 1) for k in (1, 2, 3)]
    + [(k, 0) for k in (1, 2, 3)]
    + [(k, 1) for k in (1, 2, 3, 4)]
)


def forward_kernel(*refs):
    meta, bias_ref = refs[0], refs[1]
    blocks = refs[2:18]
    ws_ref, row_ref = refs[18:20]
    msg_ref, proj_ref, w_ref, g_ref = refs[20:24]
    x_all, col_sc, q_sc, k_sc, vt_sc, s_sc = refs[24:]
    me, length = meta[0], meta[1]
    for (far, half), blk in zip(ARRIVALS, blocks):
        at = lax.rem(me + far + H, H) * T + half * 64
        x_all[pl.ds(pl.multiple_of(at, 64), 64), :] = blk[...]
    proj_ref[...] = mm(x_all[...], ws_ref[...])
    for c in range(8):
        cols = slice(c * T, (c + 1) * T)
        col_sc[cols, :] = jnp.broadcast_to(row_ref[:, cols], (T, T)).T
    for c in range(8):
        rows = slice(c * T, (c + 1) * T)
        p = proj_ref[rows, :]
        a = p * sigmoid(p)
        vt_sc[:, rows] = a[:, :DH].T.astype(BF16)
        q_sc[rows, :] = a[:, DH : 2 * DH].astype(BF16)
        k_sc[rows, :] = a[:, 2 * DH :].astype(BF16)
    scale = DH ** (-0.5)
    levels = [bias_ref[me, b] for b in range(NB)]

    def tile(i0, j0, diagonal):
        s_sc[...] = nt(k_sc[pl.ds(j0, TI), :], q_sc[i0 : i0 + TI, :])
        for c in range(TI // CH):
            rows = pl.ds(j0 + c * CH, CH)
            col = col_sc[rows, :]
            e = row_ref[:, i0 : i0 + TI] - jnp.concatenate([col, col], axis=1)
            bias = jnp.full((CH, TI), levels[0], F32)
            for b in range(1, NB):
                bias = jnp.where(e >= float(2**b - 1), levels[b], bias)
            s = s_sc[c * CH : (c + 1) * CH, :] * scale + bias
            sg = sigmoid(s)
            w = s * sg
            g = sg + w * (1.0 - sg)
            if diagonal:
                jj = lax.broadcasted_iota(jnp.int32, (CH, TI), 0) + c * CH
                ii = lax.broadcasted_iota(jnp.int32, (CH, TI), 1)
                keep = jj <= ii
                w = jnp.where(keep, w, 0.0)
                g = jnp.where(keep, g, 0.0)
            w_ref[rows, i0 : i0 + TI] = w.astype(BF16)
            g_ref[rows, i0 : i0 + TI] = g.astype(BF16)

    for bi in range(S // TI):
        i0 = bi * TI
        if bi:

            def below(bj, carry, i0=i0):
                tile(i0, pl.multiple_of(bj * TI, TI), False)
                return carry

            lax.fori_loop(0, bi, below, 0)
        tile(i0, i0, True)
        att = mm(vt_sc[:, : i0 + TI], w_ref[: i0 + TI, i0 : i0 + TI])
        pos = lax.broadcasted_iota(jnp.int32, (DH, TI), 1) + i0
        att = jnp.where(pos < length, att, 0.0)
        mean = jnp.mean(att, axis=0, keepdims=True)
        high = mean.astype(BF16)
        left = mean - high.astype(F32)
        mid = left.astype(BF16)
        low = (left - mid.astype(F32)).astype(BF16)
        kept = high.astype(F32) + mid.astype(F32) + low.astype(F32)
        centred = (att - kept).astype(BF16)
        which = lax.broadcasted_iota(jnp.int32, (16, TI), 0)
        tail = jnp.where(
            which == 0,
            high.astype(F32),
            jnp.where(which == 1, mid.astype(F32), jnp.where(which == 2, low.astype(F32), 0.0)),
        ).astype(BF16)
        for t in range(TI // T):
            dest = bi * (TI // T) + t
            msg_ref[dest, :DH, :] = centred[:, t * T : (t + 1) * T]
            msg_ref[dest, DH:, :] = tail[:, t * T : (t + 1) * T]


def tail_kernel(
    meta,
    msg_ref,
    na_ref,
    nb_ref,
    x_ref,
    cot_ref,
    wg_ref,
    wo_ref,
    gain_ref,
    mixed_ref,
    datt_ref,
    dpg_ref,
    own_ref,
    send_ref,
    att_sc,
):
    me, length, core = meta[0], meta[1], meta[2]
    for h in range(H):
        blk = msg_ref[h].astype(F32)
        att_t = blk[:DH] + (blk[DH : DH + 1] + blk[DH + 1 : DH + 2] + blk[DH + 2 : DH + 3])
        att_sc[:, h * DH : (h + 1) * DH] = att_t.T
    pg = jnp.concatenate([mm(na_ref[...], wg_ref[...]), mm(nb_ref[...], wg_ref[...])], axis=0)
    cot = cot_ref[...]
    d_mix = nt(cot, wo_ref[...])
    att = att_sc[...]
    gain = gain_ref[...]
    c = att - jnp.mean(att, axis=-1, keepdims=True)
    var = jnp.mean(c * c, axis=-1, keepdims=True)
    r = lax.rsqrt(var + EPS)
    xhat = c * r
    normed_att = xhat * gain
    sg = sigmoid(pg)
    gate = pg * sg
    mixed_rows = (normed_att * gate).astype(BF16)
    mixed_ref[...] = (x_ref[...].astype(F32) + mm(mixed_rows, wo_ref[...])).astype(BF16)
    dpg_ref[...] = (d_mix * normed_att * (sg + gate * (1.0 - sg))).astype(BF16)
    u = d_mix * gate * gain
    d_att = r * (
        u
        - jnp.mean(u, axis=-1, keepdims=True)
        - xhat * jnp.mean(u * xhat, axis=-1, keepdims=True)
    )
    pos = lax.broadcasted_iota(jnp.int32, (T, D), 0) + me * T
    d_att = jnp.where(pos < length, d_att, 0.0).astype(BF16)
    for h in range(H):
        cols = slice(h * DH, (h + 1) * DH)
        datt_ref[h] = d_att[:, cols]
        part = tn(mixed_rows[:, cols], cot).astype(BF16)
        for t in range(2):
            at = slice((2 * h + t) * 32, (2 * h + t + 1) * 32)
            even, odd = part[t * 64 : t * 64 + 32], part[t * 64 + 32 : t * 64 + 64]
            own_ref[at, :] = jnp.where(core == 0, even, odd)
            send_ref[at, :] = jnp.where(core == 0, odd, even)


def gate_kernel(dpg_ref, wg_ref, out_ref):
    out_ref[...] = nt(dpg_ref[...], wg_ref[...])


def backward_kernel(*refs):
    meta, d_ref, proj_ref, w_ref, g_ref = refs[:5]
    outs = refs[5:13]
    q_sc, k_sc, kt_sc, v_sc, ds_sc, dqt_sc, out_ref = refs[13:]
    for c in range(8):
        rows = slice(c * T, (c + 1) * T)
        p = proj_ref[rows, :]
        a = p * sigmoid(p)
        v_sc[rows, :] = a[:, :DH].astype(BF16)
        q_sc[rows, :] = a[:, DH : 2 * DH].astype(BF16)
        k_sc[rows, :] = a[:, 2 * DH :].astype(BF16)
        kt_sc[:, rows] = a[:, 2 * DH :].T.astype(BF16)
    scale = DH ** (-0.5)
    d = d_ref[...].reshape(S, DH)
    for bj in range(S // TI):
        j0 = bj * TI
        rows = slice(j0, j0 + TI)
        dw = nt(v_sc[rows, :], d[j0:, :])
        ds_sc[rows, j0:] = (dw * g_ref[rows, j0:].astype(F32)).astype(BF16)
        dk = mm(ds_sc[rows, j0:], q_sc[j0:, :]) * scale
        dv = mm(w_ref[rows, j0:], d[j0:, :])
        for t in range(TI // T):
            at = slice(j0 + t * T, j0 + (t + 1) * T)
            dest = bj * (TI // T) + t
            for n, grad in ((0, dv), (2, dk)):
                p = proj_ref[at, n * DH : (n + 1) * DH]
                sg = sigmoid(p)
                slope = sg * (1.0 + p * (1.0 - sg))
                out_ref[dest, :, n * DH : (n + 1) * DH] = (
                    grad[t * T : (t + 1) * T] * slope
                ).astype(BF16)
    for bi in range(S // TI):
        i0 = bi * TI
        dqt_sc[:, i0 : i0 + TI] = (
            mm(kt_sc[:, : i0 + TI], ds_sc[: i0 + TI, i0 : i0 + TI]) * scale
        )
    for t in range(8):
        at = slice(t * T, (t + 1) * T)
        p = proj_ref[at, DH : 2 * DH]
        sg = sigmoid(p)
        slope = sg * (1.0 + p * (1.0 - sg))
        out_ref[t, :, DH : 2 * DH] = (dqt_sc[:, at].T * slope).astype(BF16)
    for k in range(H):
        outs[k][...] = out_ref[lax.rem(meta[0] + k, H)]


def final_kernel(*refs):
    meta = refs[0]
    blocks = refs[1:9]
    back_ref, w_ref, x_ref, cot_ref, gain_ref, out_ref, msg_ref, lhs, acc = refs[9:]
    b = pl.program_id(0)

    @pl.when(b == 0)
    def _():
        for k in range(H):
            msg_ref[lax.rem(meta[0] - k + H, H)] = blocks[k][...]
        for n in range(3):
            for h in range(H):
                lhs[n, :, h * DH : (h + 1) * DH] = msg_ref[h, :, n * DH : (n + 1) * DH]
        acc[...] = back_ref[...]

    acc[...] += nt(lhs[b], w_ref[...])

    @pl.when(b == 2)
    def _():
        x = x_ref[...].astype(F32)
        c = x - jnp.mean(x, axis=-1, keepdims=True)
        var = jnp.mean(c * c, axis=-1, keepdims=True)
        r = lax.rsqrt(var + EPS)
        xhat = c * r
        u = acc[...] * gain_ref[...]
        dx = r * (
            u
            - jnp.mean(u, axis=-1, keepdims=True)
            - xhat * jnp.mean(u * xhat, axis=-1, keepdims=True)
        )
        out_ref[...] = (cot_ref[...].astype(F32) + dx).astype(BF16)


def params(**more):
    return pltpu.CompilerParams(vmem_limit_bytes=LIMIT * 1024, **more)


def cost(us):
    flops = int(us * 3.0e8)
    return pl.CostEstimate(flops=flops, bytes_accessed=1 << 20, transcendentals=0)


def paired(value, axis, mask):
    count = lax.axis_size(axis)
    return lax.ppermute(value, axis, [(i, i ^ mask) for i in range(count)])


def shifted(value, by):
    return lax.ppermute(value, "seq", [(i, (i + by) % H) for i in range(H)])


def layer(tokens, cotangent, stamps, lengths, w_qkvu, w_out, gain_in, gain_out, bias_table):
    x = tokens[0]
    cot = cotangent[0]
    me = lax.axis_index("seq")
    core = lax.axis_index("dp_2")
    meta = jnp.stack([me, lengths[0], core]).astype(jnp.int32)
    gain_in = gain_in.reshape(1, D)
    gain_out = gain_out.reshape(1, D)
    stamp_row = stamps.astype(F32)

    na, nb = pl.pallas_call(
        norm_kernel,
        out_shape=[jax.ShapeDtypeStruct((64, D), BF16)] * 2,
        in_specs=[VMEM, VMEM],
        out_specs=[VMEM, VMEM],
        compiler_params=params(),
        cost_estimate=cost(1),
        name="norm",
    )(x, gain_in)

    w_full = lax.all_gather(jnp.concatenate([w_qkvu, w_out], axis=1), DP, axis=0, tiled=True)

    head_w = jnp.concatenate(
        [
            lax.dynamic_slice_in_dim(w_qkvu, part * D + me * DH, DH, axis=1)
            for part in (1, 2, 3)
        ],
        axis=1,
    )
    copies = jnp.broadcast_to(head_w[None], (32, *head_w.shape))
    ws = lax.all_to_all(copies, DP, 0, 0, tiled=True)
    ws = ws.reshape(D, 3 * DH)

    arrived = {(0, 0): na, (0, 1): nb}
    for k in range(1, 5):
        arrived[(-k, 0)] = shifted(arrived[(1 - k, 0)], 1)
        arrived[(k, 1)] = shifted(arrived[(k - 1, 1)], -1)
        if k < 4:
            arrived[(-k, 1)] = shifted(arrived[(1 - k, 1)], 1)
            arrived[(k, 0)] = shifted(arrived[(k - 1, 0)], -1)

    msg, proj, weight, slope = pl.pallas_call(
        forward_kernel,
        out_shape=[
            jax.ShapeDtypeStruct((H, MSG, T), BF16),
            jax.ShapeDtypeStruct((S, 3 * DH), F32),
            jax.ShapeDtypeStruct((S, S), BF16),
            jax.ShapeDtypeStruct((S, S), BF16),
        ],
        in_specs=[SMEM, SMEM] + [VMEM] * 18,
        out_specs=[VMEM] * 4,
        scratch_shapes=[
            pltpu.VMEM((S, D), BF16),
            pltpu.VMEM((S, T), F32),
            pltpu.VMEM((S, DH), BF16),
            pltpu.VMEM((S, DH), BF16),
            pltpu.VMEM((DH, S), BF16),
            pltpu.VMEM((TI, TI), F32),
        ],
        compiler_params=params(),
        cost_estimate=cost(10),
        name="attend",
    )(meta, bias_table, *[arrived[a] for a in ARRIVALS], ws, stamp_row)

    att_msg = lax.all_to_all(msg, "seq", 0, 0, tiled=True)

    mixed, d_att, d_pg, w_own, w_send = pl.pallas_call(
        tail_kernel,
        grid=(1,),
        out_shape=[
            jax.ShapeDtypeStruct((T, D), BF16),
            jax.ShapeDtypeStruct((H, T, DH), BF16),
            jax.ShapeDtypeStruct((T, D), BF16),
            jax.ShapeDtypeStruct((D // 2, D), BF16),
            jax.ShapeDtypeStruct((D // 2, D), BF16),
        ],
        in_specs=[SMEM]
        + [VMEM] * 5
        + [
            pl.BlockSpec((D, D), lambda i: (0, 0)),
            pl.BlockSpec((D, D), lambda i: (0, 4)),
            VMEM,
        ],
        out_specs=[VMEM] * 5,
        scratch_shapes=[pltpu.VMEM((T, D), F32)],
        compiler_params=params(),
        cost_estimate=cost(5),
        name="tail",
    )(meta, att_msg, na, nb, x, cot, w_full, w_full, gain_out)

    d_all = lax.all_to_all(d_att, "seq", 0, 0, tiled=True)

    gate_call = pl.pallas_call(
        gate_kernel,
        grid=(1,),
        out_shape=jax.ShapeDtypeStruct((T, D), F32),
        in_specs=[VMEM, pl.BlockSpec((D, D), lambda i: (0, 0))],
        out_specs=VMEM,
        compiler_params=params(),
        cost_estimate=cost(2),
        name="gate",
    )
    gate_back = gate_call(d_pg, w_full)

    other = paired(w_send, "dp_2", 1)
    pair = (w_own.astype(F32) + other.astype(F32)).astype(BF16)
    pair, d_all = lax.optimization_barrier((pair, d_all))
    planes = lax.all_to_all(pair.reshape(16, 32, D), ("dp_0", "dp_1"), 0, 0, tiled=True)

    attend_back = pl.pallas_call(
        backward_kernel,
        out_shape=[jax.ShapeDtypeStruct((T, 3 * DH), BF16)] * H,
        in_specs=[SMEM] + [VMEM] * 4,
        out_specs=[VMEM] * H,
        scratch_shapes=[
            pltpu.VMEM((S, DH), BF16),
            pltpu.VMEM((S, DH), BF16),
            pltpu.VMEM((DH, S), BF16),
            pltpu.VMEM((S, DH), BF16),
            pltpu.VMEM((S, S), BF16),
            pltpu.VMEM((DH, S), F32),
            pltpu.VMEM((H, T, 3 * DH), BF16),
        ],
        compiler_params=params(),
        cost_estimate=cost(6),
        name="attend_back",
    )
    d_proj = attend_back(meta, d_all, proj, weight, slope)

    total = jnp.sum(planes.astype(F32), axis=0)
    for mask in (1, 3, 7):
        own = total.astype(BF16)
        far = paired(own, "seq", mask)
        total = own.astype(F32) + far.astype(F32)
    w_grad = total

    d_rows = {0: d_proj[0]}
    for k in (4, 5, 3, 6, 2, 7, 1):
        d_rows[k] = shifted(d_proj[k], k)

    final = pl.pallas_call(
        final_kernel,
        grid=(3,),
        out_shape=jax.ShapeDtypeStruct((T, D), BF16),
        in_specs=[SMEM]
        + [VMEM] * (H + 1)
        + [pl.BlockSpec((D, D), lambda b: (0, b + 1)), VMEM, VMEM, VMEM],
        out_specs=VMEM,
        scratch_shapes=[
            pltpu.VMEM((H, T, 3 * DH), BF16),
            pltpu.VMEM((3, T, D), BF16),
            pltpu.VMEM((T, D), F32),
        ],
        compiler_params=params(dimension_semantics=("arbitrary",)),
        cost_estimate=cost(5),
        name="final",
    )
    input_grad = final(
        meta, *[d_rows[k] for k in range(H)], gate_back, w_full, x, cot, gain_in
    )

    return (mixed[None], input_grad[None], w_grad)


def solution(mesh):
    finer = Mesh(mesh.devices.reshape(4, 4, 2, mesh.shape["seq"]), (*DP, "seq"))
    placed = (
        P(DP, "seq", None),
        P(DP, "seq", None),
        P(DP, None),
        P(DP),
        P(DP, None),
        P(DP, None),
        P(),
        P(),
        P(),
    )
    return jax.shard_map(
        layer,
        mesh=finer,
        in_specs=placed,
        out_specs=(P(DP, "seq", None), P(DP, "seq", None), P(DP, None)),
        check_vma=False,
    )
```

```python
import jax
import jax.numpy as jnp
from jax import lax
from jax.experimental import pallas as pl
from jax.experimental.pallas import tpu as pltpu
from jax.sharding import Mesh
from jax.sharding import PartitionSpec as P


H = 8
DH = 128
D = 1024
T = 128
S = 1024
NB = 16
TI = 256
CH = 32
DP = ("dp_0", "dp_1", "dp_2")
EPS = 1e-05
MSG = 144
LIMIT = 52000
F32 = jnp.float32
BF16 = jnp.bfloat16

ORDER = (4, 5, 3, 6, 2, 7, 1)

VMEM = pl.BlockSpec(memory_space=pltpu.VMEM)
SMEM = pl.BlockSpec(memory_space=pltpu.SMEM)


def sigmoid(v):
    return 0.5 * jnp.tanh(0.5 * v) + 0.5


def nt(a, b):
    return lax.dot_general(a, b, (((1,), (1,)), ((), ())), preferred_element_type=F32)


def tn(a, b):
    return lax.dot_general(a, b, (((0,), (0,)), ((), ())), preferred_element_type=F32)


def mm(a, b):
    return jnp.dot(a, b, preferred_element_type=F32)


def norm_kernel(x_ref, gain_ref, a_ref, b_ref):
    x = x_ref[...].astype(F32)
    c = x - jnp.mean(x, axis=-1, keepdims=True)
    var = jnp.mean(c * c, axis=-1, keepdims=True)
    n = (c * lax.rsqrt(var + EPS) * gain_ref[...]).astype(BF16)
    a_ref[...] = n[:64]
    b_ref[...] = n[64:]


ARRIVALS = (
    [(0, 0), (0, 1)]
    + [(-k, 0) for k in (1, 2, 3, 4)]
    + [(-k, 1) for k in (1, 2, 3)]
    + [(k, 0) for k in (1, 2, 3)]
    + [(k, 1) for k in (1, 2, 3, 4)]
)


def forward_kernel(*refs):
    meta, bias_ref = refs[0], refs[1]
    blocks = refs[2:18]
    ws_ref, row_ref = refs[18:20]
    msg_ref, proj_ref, w_ref, g_ref = refs[20:24]
    x_all, col_sc, q_sc, k_sc, vt_sc, s_sc = refs[24:]
    me, length = meta[0], meta[1]
    for (far, half), blk in zip(ARRIVALS, blocks):
        at = lax.rem(me + far + H, H) * T + half * 64
        x_all[pl.ds(pl.multiple_of(at, 64), 64), :] = blk[...]

    def project(c, carry):
        rows = pl.ds(pl.multiple_of(c * TI, TI), TI)
        proj_ref[rows, :] = mm(x_all[rows, :], ws_ref[...])
        return carry

    lax.fori_loop(0, S // TI, project, 0)
    for c in range(8):
        cols = slice(c * T, (c + 1) * T)
        col_sc[cols, :] = jnp.broadcast_to(row_ref[:, cols], (T, T)).T
    for c in range(8):
        rows = slice(c * T, (c + 1) * T)
        p = proj_ref[rows, :]
        a = p * sigmoid(p)
        vt_sc[:, rows] = a[:, :DH].T.astype(BF16)
        q_sc[rows, :] = a[:, DH : 2 * DH].astype(BF16)
        k_sc[rows, :] = a[:, 2 * DH :].astype(BF16)
    scale = DH ** (-0.5)
    levels = [bias_ref[me, b] for b in range(NB)]

    def tile(i0, j0, diagonal):
        s_sc[...] = nt(k_sc[pl.ds(j0, TI), :], q_sc[i0 : i0 + TI, :])

        def chunk(c, carry):
            at = pl.multiple_of(c * CH, CH)
            rows = pl.ds(pl.multiple_of(j0 + at, CH), CH)
            col = col_sc[rows, :]
            e = row_ref[:, i0 : i0 + TI] - jnp.concatenate([col, col], axis=1)
            bias = jnp.full((CH, TI), levels[0], F32)
            for b in range(1, NB):
                bias = jnp.where(e >= float(2**b - 1), levels[b], bias)
            s = s_sc[pl.ds(at, CH), :] * scale + bias
            sg = sigmoid(s)
            w = s * sg
            g = sg + w * (1.0 - sg)
            if diagonal:
                jj = lax.broadcasted_iota(jnp.int32, (CH, TI), 0) + at
                ii = lax.broadcasted_iota(jnp.int32, (CH, TI), 1)
                keep = jj <= ii
                w = jnp.where(keep, w, 0.0)
                g = jnp.where(keep, g, 0.0)
            w_ref[rows, i0 : i0 + TI] = w.astype(BF16)
            g_ref[rows, i0 : i0 + TI] = g.astype(BF16)
            return carry

        lax.fori_loop(0, TI // CH, chunk, 0, unroll=2)

    for bi in range(S // TI):
        i0 = bi * TI
        if bi:

            def below(bj, carry, i0=i0):
                tile(i0, pl.multiple_of(bj * TI, TI), False)
                return carry

            lax.fori_loop(0, bi, below, 0)
        tile(i0, i0, True)
        att = mm(vt_sc[:, : i0 + TI], w_ref[: i0 + TI, i0 : i0 + TI])
        pos = lax.broadcasted_iota(jnp.int32, (DH, TI), 1) + i0
        att = jnp.where(pos < length, att, 0.0)
        mean = jnp.mean(att, axis=0, keepdims=True)
        high = mean.astype(BF16)
        left = mean - high.astype(F32)
        mid = left.astype(BF16)
        low = (left - mid.astype(F32)).astype(BF16)
        kept = high.astype(F32) + mid.astype(F32) + low.astype(F32)
        centred = (att - kept).astype(BF16)
        which = lax.broadcasted_iota(jnp.int32, (16, TI), 0)
        tail = jnp.where(
            which == 0,
            high.astype(F32),
            jnp.where(which == 1, mid.astype(F32), jnp.where(which == 2, low.astype(F32), 0.0)),
        ).astype(BF16)
        for t in range(TI // T):
            dest = bi * (TI // T) + t
            msg_ref[dest, :DH, :] = centred[:, t * T : (t + 1) * T]
            msg_ref[dest, DH:, :] = tail[:, t * T : (t + 1) * T]


def tail_kernel(
    meta,
    msg_ref,
    na_ref,
    nb_ref,
    x_ref,
    cot_ref,
    wg_ref,
    wo_ref,
    gain_ref,
    mixed_ref,
    dpg_ref,
    own_ref,
    send_ref,
    *more,
):
    datt_out, (att_sc, datt_ref, rows_sc, pg_sc, dmix_sc) = more[:H], more[H:]
    me, length, core = meta[0], meta[1], meta[2]
    for h in range(H):
        blk = msg_ref[h].astype(F32)
        att_t = blk[:DH] + (blk[DH : DH + 1] + blk[DH + 1 : DH + 2] + blk[DH + 2 : DH + 3])
        att_sc[:, h * DH : (h + 1) * DH] = att_t.T
    rows_sc[:64, :] = na_ref[...]
    rows_sc[64:, :] = nb_ref[...]
    cot = cot_ref[...]

    def columns(n, carry):
        at = pl.ds(pl.multiple_of(n * 256, 256), 256)
        pg_sc[:, at] = mm(rows_sc[...], wg_ref[:, at])
        dmix_sc[:, at] = nt(cot, wo_ref[at, :])
        return carry

    lax.fori_loop(0, D // 256, columns, 0)
    pg = pg_sc[...]
    d_mix = dmix_sc[...]
    att = att_sc[...]
    gain = gain_ref[...]
    c = att - jnp.mean(att, axis=-1, keepdims=True)
    var = jnp.mean(c * c, axis=-1, keepdims=True)
    r = lax.rsqrt(var + EPS)
    xhat = c * r
    normed_att = xhat * gain
    sg = sigmoid(pg)
    gate = pg * sg
    mixed_rows = (normed_att * gate).astype(BF16)
    rows_sc[...] = mixed_rows
    dpg_ref[...] = (d_mix * normed_att * (sg + gate * (1.0 - sg))).astype(BF16)
    u = d_mix * gate * gain
    d_att = r * (
        u
        - jnp.mean(u, axis=-1, keepdims=True)
        - xhat * jnp.mean(u * xhat, axis=-1, keepdims=True)
    )
    pos = lax.broadcasted_iota(jnp.int32, (T, D), 0) + me * T
    d_att = jnp.where(pos < length, d_att, 0.0).astype(BF16)
    for h in range(H):
        datt_ref[h] = d_att[:, h * DH : (h + 1) * DH]

    def head(h, carry):
        part = tn(rows_sc[:, pl.ds(pl.multiple_of(h * DH, DH), DH)], cot).astype(BF16)
        for t in range(2):
            at = pl.ds(pl.multiple_of((2 * h + t) * 32, 32), 32)
            even, odd = part[t * 64 : t * 64 + 32], part[t * 64 + 32 : t * 64 + 64]
            own_ref[at, :] = jnp.where(core == 0, even, odd)
            send_ref[at, :] = jnp.where(core == 0, odd, even)
        return carry

    lax.fori_loop(0, H, head, 0)

    def mix(n, carry):
        at = pl.ds(pl.multiple_of(n * 256, 256), 256)
        mixed_ref[:, at] = (
            x_ref[:, at].astype(F32) + mm(rows_sc[...], wo_ref[:, at])
        ).astype(BF16)
        return carry

    lax.fori_loop(0, D // 256, mix, 0)
    for k in range(H):
        datt_out[k][...] = datt_ref[lax.rem(me + k, H)]


def gate_kernel(dpg_ref, wg_ref, out_ref):
    def columns(n, carry):
        at = pl.ds(pl.multiple_of(n * 256, 256), 256)
        out_ref[:, at] = nt(dpg_ref[...], wg_ref[at, :])
        return carry

    lax.fori_loop(0, D // 256, columns, 0)


def backward_kernel(*refs):
    meta, blocks = refs[0], refs[1:9]
    proj_ref, w_ref, g_ref = refs[9:12]
    outs = refs[12:20]
    q_sc, k_sc, kt_sc, v_sc, ds_sc, dqt_sc, out_ref, d_ref = refs[20:]
    for k in range(H):
        d_ref[lax.rem(meta[0] - k + H, H)] = blocks[k][...]
    for c in range(8):
        rows = slice(c * T, (c + 1) * T)
        p = proj_ref[rows, :]
        a = p * sigmoid(p)
        v_sc[rows, :] = a[:, :DH].astype(BF16)
        q_sc[rows, :] = a[:, DH : 2 * DH].astype(BF16)
        k_sc[rows, :] = a[:, 2 * DH :].astype(BF16)
        kt_sc[:, rows] = a[:, 2 * DH :].T.astype(BF16)
    scale = DH ** (-0.5)
    d = d_ref[...].reshape(S, DH)
    for bj in range(S // TI):
        j0 = bj * TI
        rows = slice(j0, j0 + TI)
        dw = nt(v_sc[rows, :], d[j0:, :])
        ds_sc[rows, j0:] = (dw * g_ref[rows, j0:].astype(F32)).astype(BF16)
        dk = mm(ds_sc[rows, j0:], q_sc[j0:, :]) * scale
        dv = mm(w_ref[rows, j0:], d[j0:, :])
        for t in range(TI // T):
            at = slice(j0 + t * T, j0 + (t + 1) * T)
            dest = bj * (TI // T) + t
            for n, grad in ((0, dv), (2, dk)):
                p = proj_ref[at, n * DH : (n + 1) * DH]
                sg = sigmoid(p)
                slope = sg * (1.0 + p * (1.0 - sg))
                out_ref[dest, :, n * DH : (n + 1) * DH] = (
                    grad[t * T : (t + 1) * T] * slope
                ).astype(BF16)
    for bi in range(S // TI):
        i0 = bi * TI
        dqt_sc[:, i0 : i0 + TI] = (
            mm(kt_sc[:, : i0 + TI], ds_sc[: i0 + TI, i0 : i0 + TI]) * scale
        )
    for t in range(8):
        at = slice(t * T, (t + 1) * T)
        p = proj_ref[at, DH : 2 * DH]
        sg = sigmoid(p)
        slope = sg * (1.0 + p * (1.0 - sg))
        out_ref[t, :, DH : 2 * DH] = (dqt_sc[:, at].T * slope).astype(BF16)
    for k in range(H):
        outs[k][...] = out_ref[lax.rem(meta[0] + k, H)]


def final_kernel(*refs):
    meta = refs[0]
    blocks = refs[1:9]
    back_ref, w_ref, x_ref, cot_ref, gain_ref, out_ref, msg_ref, lhs, acc = refs[9:]
    b = pl.program_id(0)

    @pl.when(b == 0)
    def _():
        for k in range(H):
            msg_ref[lax.rem(meta[0] - k + H, H)] = blocks[k][...]
        for n in range(3):
            for h in range(H):
                lhs[n, :, h * DH : (h + 1) * DH] = msg_ref[h, :, n * DH : (n + 1) * DH]
        acc[...] = back_ref[...]

    def columns(n, carry):
        at = pl.ds(pl.multiple_of(n * 256, 256), 256)
        acc[:, at] += nt(lhs[b], w_ref[at, :])
        return carry

    lax.fori_loop(0, D // 256, columns, 0)

    @pl.when(b == 2)
    def _():
        x = x_ref[...].astype(F32)
        c = x - jnp.mean(x, axis=-1, keepdims=True)
        var = jnp.mean(c * c, axis=-1, keepdims=True)
        r = lax.rsqrt(var + EPS)
        xhat = c * r
        u = acc[...] * gain_ref[...]
        dx = r * (
            u
            - jnp.mean(u, axis=-1, keepdims=True)
            - xhat * jnp.mean(u * xhat, axis=-1, keepdims=True)
        )
        out_ref[...] = (cot_ref[...].astype(F32) + dx).astype(BF16)


def params(kib=LIMIT, **more):
    return pltpu.CompilerParams(vmem_limit_bytes=kib * 1024, **more)


def cost(us):
    flops = int(us * 3.0e8)
    return pl.CostEstimate(flops=flops, bytes_accessed=1 << 20, transcendentals=0)


def paired(value, axis, mask):
    count = lax.axis_size(axis)
    return lax.ppermute(value, axis, [(i, i ^ mask) for i in range(count)])


def shifted(value, by):
    return lax.ppermute(value, "seq", [(i, (i + by) % H) for i in range(H)])


def layer(tokens, cotangent, stamps, lengths, w_qkvu, w_out, gain_in, gain_out, bias_table):
    x = tokens[0]
    cot = cotangent[0]
    me = lax.axis_index("seq")
    core = lax.axis_index("dp_2")
    meta = jnp.stack([me, lengths[0], core]).astype(jnp.int32)
    gain_in = gain_in.reshape(1, D)
    gain_out = gain_out.reshape(1, D)
    stamp_row = stamps.astype(F32)

    na, nb = pl.pallas_call(
        norm_kernel,
        out_shape=[jax.ShapeDtypeStruct((64, D), BF16)] * 2,
        in_specs=[VMEM, VMEM],
        out_specs=[VMEM, VMEM],
        compiler_params=params(),
        cost_estimate=cost(1),
        name="norm",
    )(x, gain_in)

    w_early = lax.all_gather(
        jnp.concatenate([w_qkvu[:, :D], w_out], axis=1), DP, axis=0, tiled=True
    )
    w_late = lax.all_gather(w_qkvu[:, D:], DP, axis=0, tiled=True)

    head_w = jnp.concatenate(
        [
            lax.dynamic_slice_in_dim(w_qkvu, part * D + me * DH, DH, axis=1)
            for part in (1, 2, 3)
        ],
        axis=1,
    )
    copies = jnp.broadcast_to(head_w[None], (32, *head_w.shape))
    ws = lax.all_to_all(copies, DP, 0, 0, tiled=True)
    ws = ws.reshape(D, 3 * DH)

    arrived = {(0, 0): na, (0, 1): nb}
    for k in range(1, 5):
        arrived[(-k, 0)] = shifted(arrived[(1 - k, 0)], 1)
        arrived[(k, 1)] = shifted(arrived[(k - 1, 1)], -1)
        if k < 4:
            arrived[(-k, 1)] = shifted(arrived[(1 - k, 1)], 1)
            arrived[(k, 0)] = shifted(arrived[(k - 1, 0)], -1)

    msg, proj, weight, slope = pl.pallas_call(
        forward_kernel,
        out_shape=[
            jax.ShapeDtypeStruct((H, MSG, T), BF16),
            jax.ShapeDtypeStruct((S, 3 * DH), F32),
            jax.ShapeDtypeStruct((S, S), BF16),
            jax.ShapeDtypeStruct((S, S), BF16),
        ],
        in_specs=[SMEM, SMEM] + [VMEM] * 18,
        out_specs=[VMEM] * 4,
        scratch_shapes=[
            pltpu.VMEM((S, D), BF16),
            pltpu.VMEM((S, T), F32),
            pltpu.VMEM((S, DH), BF16),
            pltpu.VMEM((S, DH), BF16),
            pltpu.VMEM((DH, S), BF16),
            pltpu.VMEM((TI, TI), F32),
        ],
        compiler_params=params(),
        cost_estimate=cost(10),
        name="attend",
    )(meta, bias_table, *[arrived[a] for a in ARRIVALS], ws, stamp_row)

    att_msg = lax.all_to_all(msg, "seq", 0, 0, tiled=True)

    mixed, d_pg, w_own, w_send, *d_att = pl.pallas_call(
        tail_kernel,
        grid=(1,),
        out_shape=[
            jax.ShapeDtypeStruct((T, D), BF16),
            jax.ShapeDtypeStruct((T, D), BF16),
            jax.ShapeDtypeStruct((D // 2, D), BF16),
            jax.ShapeDtypeStruct((D // 2, D), BF16),
        ]
        + [jax.ShapeDtypeStruct((T, DH), BF16)] * H,
        in_specs=[SMEM]
        + [VMEM] * 5
        + [
            pl.BlockSpec((D, D), lambda i: (0, 0)),
            pl.BlockSpec((D, D), lambda i: (0, 1)),
            VMEM,
        ],
        out_specs=[VMEM] * (4 + H),
        scratch_shapes=[
            pltpu.VMEM((T, D), F32),
            pltpu.VMEM((H, T, DH), BF16),
            pltpu.VMEM((T, D), BF16),
            pltpu.VMEM((T, D), F32),
            pltpu.VMEM((T, D), F32),
        ],
        compiler_params=params(),
        cost_estimate=cost(5),
        name="tail",
    )(meta, att_msg, na, nb, x, cot, w_early, w_early, gain_out)

    d_all = {0: d_att[0]}
    for k in ORDER:
        d_all[k] = shifted(d_att[k], k)

    gate_call = pl.pallas_call(
        gate_kernel,
        grid=(1,),
        out_shape=jax.ShapeDtypeStruct((T, D), F32),
        in_specs=[VMEM, pl.BlockSpec((D, D), lambda i: (0, 0))],
        out_specs=VMEM,
        compiler_params=params(),
        cost_estimate=cost(2),
        name="gate",
    )
    gate_back = gate_call(d_pg, w_early)

    other = paired(w_send, "dp_2", 1)
    pair = (w_own.astype(F32) + other.astype(F32)).astype(BF16)

    attend_back = pl.pallas_call(
        backward_kernel,
        out_shape=[jax.ShapeDtypeStruct((T, 3 * DH), BF16)] * H,
        in_specs=[SMEM] + [VMEM] * (3 + H),
        out_specs=[VMEM] * H,
        scratch_shapes=[
            pltpu.VMEM((S, DH), BF16),
            pltpu.VMEM((S, DH), BF16),
            pltpu.VMEM((DH, S), BF16),
            pltpu.VMEM((S, DH), BF16),
            pltpu.VMEM((S, S), BF16),
            pltpu.VMEM((DH, S), F32),
            pltpu.VMEM((H, T, 3 * DH), BF16),
            pltpu.VMEM((H, T, DH), BF16),
        ],
        compiler_params=params(24000),
        cost_estimate=cost(6),
        name="attend_back",
    )
    d_proj = attend_back(meta, *[d_all[k] for k in range(H)], proj, weight, slope)

    pair, first = lax.optimization_barrier((pair, d_proj[0]))
    d_proj = [first, *d_proj[1:]]
    planes = lax.all_to_all(pair.reshape(16, 32, D), ("dp_0", "dp_1"), 0, 0, tiled=True)

    total = jnp.sum(planes.astype(F32), axis=0)
    for mask in (1, 3, 7):
        own = total.astype(BF16)
        far = paired(own, "seq", mask)
        total = own.astype(F32) + far.astype(F32)
    w_grad = total

    d_rows = {0: d_proj[0]}
    for k in ORDER:
        d_rows[k] = shifted(d_proj[k], k)

    final = pl.pallas_call(
        final_kernel,
        grid=(3,),
        out_shape=jax.ShapeDtypeStruct((T, D), BF16),
        in_specs=[SMEM]
        + [VMEM] * (H + 1)
        + [pl.BlockSpec((D, D), lambda b: (0, b)), VMEM, VMEM, VMEM],
        out_specs=VMEM,
        scratch_shapes=[
            pltpu.VMEM((H, T, 3 * DH), BF16),
            pltpu.VMEM((3, T, D), BF16),
            pltpu.VMEM((T, D), F32),
        ],
        compiler_params=params(dimension_semantics=("arbitrary",)),
        cost_estimate=cost(5),
        name="final",
    )
    input_grad = final(
        meta, *[d_rows[k] for k in range(H)], gate_back, w_late, x, cot, gain_in
    )

    return (mixed[None], input_grad[None], w_grad)


def solution(mesh):
    finer = Mesh(mesh.devices.reshape(4, 4, 2, mesh.shape["seq"]), (*DP, "seq"))
    placed = (
        P(DP, "seq", None),
        P(DP, "seq", None),
        P(DP, None),
        P(DP),
        P(DP, None),
        P(DP, None),
        P(),
        P(),
        P(),
    )
    return jax.shard_map(
        layer,
        mesh=finer,
        in_specs=placed,
        out_specs=(P(DP, "seq", None), P(DP, "seq", None), P(DP, None)),
        check_vma=False,
    )
```

```python
import jax
import jax.numpy as jnp
from jax import lax
from jax.experimental import pallas as pl
from jax.experimental.pallas import tpu as pltpu
from jax.sharding import Mesh
from jax.sharding import PartitionSpec as P


H = 8
DH = 128
D = 1024
T = 128
S = 1024
NB = 16
TI = 256
CH = 32
DP = ("dp_0", "dp_1", "dp_2")
EPS = 1e-05
MSG = 144
LIMIT = 52000
UNROLL = 8
F32 = jnp.float32
BF16 = jnp.bfloat16

ORDER = (4, 5, 3, 6, 2, 7, 1)

VMEM = pl.BlockSpec(memory_space=pltpu.VMEM)
SMEM = pl.BlockSpec(memory_space=pltpu.SMEM)


def sigmoid(v):
    return 0.5 * jnp.tanh(0.5 * v) + 0.5


def nt(a, b):
    return lax.dot_general(a, b, (((1,), (1,)), ((), ())), preferred_element_type=F32)


def tn(a, b):
    return lax.dot_general(a, b, (((0,), (0,)), ((), ())), preferred_element_type=F32)


def mm(a, b):
    return jnp.dot(a, b, preferred_element_type=F32)


def prep_kernel(
    x_ref, gain_ref, w_ref, wout_ref, a_ref, b_ref, early_ref, late_ref, copies_ref
):
    me = lax.axis_index("seq")
    x = x_ref[...].astype(F32)
    c = x - jnp.mean(x, axis=-1, keepdims=True)
    var = jnp.mean(c * c, axis=-1, keepdims=True)
    n = (c * lax.rsqrt(var + EPS) * gain_ref[...]).astype(BF16)
    a_ref[...] = n[:64]
    b_ref[...] = n[64:]
    early_ref[:, :D] = w_ref[:, :D]
    early_ref[:, D:] = wout_ref[...]
    late_ref[...] = w_ref[:, D:]
    for part in range(3):
        at = pl.multiple_of((part + 1) * D + me * DH, DH)
        own = w_ref[:, pl.ds(at, DH)]
        for n in range(32):
            copies_ref[n, :, part * DH : (part + 1) * DH] = own


ARRIVALS = (
    [(0, 0), (0, 1)]
    + [(-k, 0) for k in (1, 2, 3, 4)]
    + [(-k, 1) for k in (1, 2, 3)]
    + [(k, 0) for k in (1, 2, 3)]
    + [(k, 1) for k in (1, 2, 3, 4)]
)


def forward_kernel(*refs):
    length_ref, bias_ref = refs[0], refs[1]
    blocks = refs[2:18]
    ws_ref, row_ref = refs[18:20]
    msg_ref, proj_ref, w_ref, g_ref = refs[20:24]
    x_all, col_sc, q_sc, k_sc, vt_sc, s_sc = refs[24:]
    me, length = lax.axis_index("seq"), length_ref[0]
    for (far, half), blk in zip(ARRIVALS, blocks):
        at = lax.rem(me + far + H, H) * T + half * 64
        x_all[pl.ds(pl.multiple_of(at, 64), 64), :] = blk[...]

    proj_ref[...] = mm(x_all[...], ws_ref[...])
    for c in range(8):
        cols = slice(c * T, (c + 1) * T)
        col_sc[cols, :] = jnp.broadcast_to(row_ref[:, cols].astype(F32), (T, T)).T
    for c in range(8):
        rows = slice(c * T, (c + 1) * T)
        p = proj_ref[rows, :]
        a = p * sigmoid(p)
        vt_sc[:, rows] = a[:, :DH].T.astype(BF16)
        q_sc[rows, :] = a[:, DH : 2 * DH].astype(BF16)
        k_sc[rows, :] = a[:, 2 * DH :].astype(BF16)
    scale = DH ** (-0.5)
    levels = [bias_ref[me, b] for b in range(NB)]

    def tile(i0, j0, diagonal):
        s_sc[...] = nt(k_sc[pl.ds(j0, TI), :], q_sc[i0 : i0 + TI, :])

        def chunk(c, carry):
            at = pl.multiple_of(c * CH, CH)
            rows = pl.ds(pl.multiple_of(j0 + at, CH), CH)
            col = col_sc[rows, :]
            e = row_ref[:, i0 : i0 + TI].astype(F32) - jnp.concatenate([col, col], axis=1)
            bias = jnp.full((CH, TI), levels[0], F32)
            for b in range(1, NB):
                bias = jnp.where(e >= float(2**b - 1), levels[b], bias)
            s = s_sc[pl.ds(at, CH), :] * scale + bias
            sg = sigmoid(s)
            w = s * sg
            g = sg + w * (1.0 - sg)
            if diagonal:
                jj = lax.broadcasted_iota(jnp.int32, (CH, TI), 0) + at
                ii = lax.broadcasted_iota(jnp.int32, (CH, TI), 1)
                keep = jj <= ii
                w = jnp.where(keep, w, 0.0)
                g = jnp.where(keep, g, 0.0)
            w_ref[rows, i0 : i0 + TI] = w.astype(BF16)
            g_ref[rows, i0 : i0 + TI] = g.astype(BF16)
            return carry

        lax.fori_loop(0, TI // CH, chunk, 0, unroll=UNROLL)

    for bi in range(S // TI):
        i0 = bi * TI
        if bi:

            def below(bj, carry, i0=i0):
                tile(i0, pl.multiple_of(bj * TI, TI), False)
                return carry

            lax.fori_loop(0, bi, below, 0)
        tile(i0, i0, True)
        att = mm(vt_sc[:, : i0 + TI], w_ref[: i0 + TI, i0 : i0 + TI])
        pos = lax.broadcasted_iota(jnp.int32, (DH, TI), 1) + i0
        att = jnp.where(pos < length, att, 0.0)
        mean = jnp.mean(att, axis=0, keepdims=True)
        high = mean.astype(BF16)
        left = mean - high.astype(F32)
        mid = left.astype(BF16)
        low = (left - mid.astype(F32)).astype(BF16)
        kept = high.astype(F32) + mid.astype(F32) + low.astype(F32)
        centred = (att - kept).astype(BF16)
        which = lax.broadcasted_iota(jnp.int32, (16, TI), 0)
        tail = jnp.where(
            which == 0,
            high.astype(F32),
            jnp.where(which == 1, mid.astype(F32), jnp.where(which == 2, low.astype(F32), 0.0)),
        ).astype(BF16)
        for t in range(TI // T):
            dest = bi * (TI // T) + t
            msg_ref[dest, :DH, :] = centred[:, t * T : (t + 1) * T]
            msg_ref[dest, DH:, :] = tail[:, t * T : (t + 1) * T]


def tail_kernel(
    length_ref,
    msg_ref,
    na_ref,
    nb_ref,
    x_ref,
    cot_ref,
    wg_ref,
    wo_ref,
    gain_ref,
    mixed_ref,
    dpg_ref,
    own_ref,
    send_ref,
    *more,
):
    datt_out, (att_sc, datt_ref, rows_sc, pg_sc, dmix_sc) = more[:H], more[H:]
    me, core, length = lax.axis_index("seq"), lax.axis_index("dp_2"), length_ref[0]
    for h in range(H):
        blk = msg_ref[h].astype(F32)
        att_t = blk[:DH] + (blk[DH : DH + 1] + blk[DH + 1 : DH + 2] + blk[DH + 2 : DH + 3])
        att_sc[:, h * DH : (h + 1) * DH] = att_t.T
    rows_sc[:64, :] = na_ref[...]
    rows_sc[64:, :] = nb_ref[...]
    cot = cot_ref[...]

    def columns(n, carry):
        at = pl.ds(pl.multiple_of(n * 512, 512), 512)
        pg_sc[:, at] = mm(rows_sc[...], wg_ref[:, at])
        dmix_sc[:, at] = nt(cot, wo_ref[at, :])
        return carry

    lax.fori_loop(0, D // 512, columns, 0)
    pg = pg_sc[...]
    d_mix = dmix_sc[...]
    att = att_sc[...]
    gain = gain_ref[...]
    c = att - jnp.mean(att, axis=-1, keepdims=True)
    var = jnp.mean(c * c, axis=-1, keepdims=True)
    r = lax.rsqrt(var + EPS)
    xhat = c * r
    normed_att = xhat * gain
    sg = sigmoid(pg)
    gate = pg * sg
    mixed_rows = (normed_att * gate).astype(BF16)
    rows_sc[...] = mixed_rows
    dpg_ref[...] = (d_mix * normed_att * (sg + gate * (1.0 - sg))).astype(BF16)
    u = d_mix * gate * gain
    d_att = r * (
        u
        - jnp.mean(u, axis=-1, keepdims=True)
        - xhat * jnp.mean(u * xhat, axis=-1, keepdims=True)
    )
    pos = lax.broadcasted_iota(jnp.int32, (T, D), 0) + me * T
    d_att = jnp.where(pos < length, d_att, 0.0).astype(BF16)
    for h in range(H):
        datt_ref[h] = d_att[:, h * DH : (h + 1) * DH]

    for h in range(H):
        part = tn(rows_sc[:, h * DH : (h + 1) * DH], cot).astype(BF16)
        for t in range(2):
            at = slice((2 * h + t) * 32, (2 * h + t + 1) * 32)
            even, odd = part[t * 64 : t * 64 + 32], part[t * 64 + 32 : t * 64 + 64]
            own_ref[at, :] = jnp.where(core == 0, even, odd)
            send_ref[at, :] = jnp.where(core == 0, odd, even)
    mixed_ref[...] = (x_ref[...].astype(F32) + mm(rows_sc[...], wo_ref[...])).astype(BF16)
    for k in range(H):
        datt_out[k][...] = datt_ref[lax.rem(me + k, H)]


def gate_kernel(dpg_ref, wg_ref, out_ref):
    def columns(n, carry):
        at = pl.ds(pl.multiple_of(n * 256, 256), 256)
        out_ref[:, at] = nt(dpg_ref[...], wg_ref[at, :])
        return carry

    lax.fori_loop(0, D // 256, columns, 0)


def backward_kernel(*refs):
    blocks = refs[:8]
    proj_ref, w_ref, g_ref = refs[8:11]
    outs = refs[11:19]
    me = lax.axis_index("seq")
    q_sc, k_sc, kt_sc, v_sc, ds_sc, dqt_sc, out_ref, d_ref = refs[19:]
    for k in range(H):
        d_ref[lax.rem(me - k + H, H)] = blocks[k][...]
    for c in range(8):
        rows = slice(c * T, (c + 1) * T)
        p = proj_ref[rows, :]
        a = p * sigmoid(p)
        v_sc[rows, :] = a[:, :DH].astype(BF16)
        q_sc[rows, :] = a[:, DH : 2 * DH].astype(BF16)
        k_sc[rows, :] = a[:, 2 * DH :].astype(BF16)
        kt_sc[:, rows] = a[:, 2 * DH :].T.astype(BF16)
    scale = DH ** (-0.5)
    d = d_ref[...].reshape(S, DH)
    for bj in range(S // TI):
        j0 = bj * TI
        rows = slice(j0, j0 + TI)
        dw = nt(v_sc[rows, :], d[j0:, :])
        ds_sc[rows, j0:] = (dw * g_ref[rows, j0:].astype(F32)).astype(BF16)
        dk = mm(ds_sc[rows, j0:], q_sc[j0:, :]) * scale
        dv = mm(w_ref[rows, j0:], d[j0:, :])
        for t in range(TI // T):
            at = slice(j0 + t * T, j0 + (t + 1) * T)
            dest = bj * (TI // T) + t
            for n, grad in ((0, dv), (2, dk)):
                p = proj_ref[at, n * DH : (n + 1) * DH]
                sg = sigmoid(p)
                slope = sg * (1.0 + p * (1.0 - sg))
                out_ref[dest, :, n * DH : (n + 1) * DH] = (
                    grad[t * T : (t + 1) * T] * slope
                ).astype(BF16)
    for bi in range(S // TI):
        i0 = bi * TI
        dqt_sc[:, i0 : i0 + TI] = (
            mm(kt_sc[:, : i0 + TI], ds_sc[: i0 + TI, i0 : i0 + TI]) * scale
        )
    for t in range(8):
        at = slice(t * T, (t + 1) * T)
        p = proj_ref[at, DH : 2 * DH]
        sg = sigmoid(p)
        slope = sg * (1.0 + p * (1.0 - sg))
        out_ref[t, :, DH : 2 * DH] = (dqt_sc[:, at].T * slope).astype(BF16)
    for k in range(H):
        outs[k][...] = out_ref[lax.rem(me + k, H)]


def final_kernel(*refs):
    blocks = refs[:8]
    back_ref, w_ref, x_ref, cot_ref, gain_ref, out_ref, msg_ref, lhs, acc = refs[8:]
    me = lax.axis_index("seq")
    b = pl.program_id(0)

    @pl.when(b == 0)
    def _():
        for k in range(H):
            msg_ref[lax.rem(me - k + H, H)] = blocks[k][...]
        for n in range(3):
            for h in range(H):
                lhs[n, :, h * DH : (h + 1) * DH] = msg_ref[h, :, n * DH : (n + 1) * DH]
        acc[...] = back_ref[...]

    def columns(n, carry):
        at = pl.ds(pl.multiple_of(n * 256, 256), 256)
        acc[:, at] += nt(lhs[b], w_ref[at, :])
        return carry

    lax.fori_loop(0, D // 256, columns, 0)

    @pl.when(b == 2)
    def _():
        x = x_ref[...].astype(F32)
        c = x - jnp.mean(x, axis=-1, keepdims=True)
        var = jnp.mean(c * c, axis=-1, keepdims=True)
        r = lax.rsqrt(var + EPS)
        xhat = c * r
        u = acc[...] * gain_ref[...]
        dx = r * (
            u
            - jnp.mean(u, axis=-1, keepdims=True)
            - xhat * jnp.mean(u * xhat, axis=-1, keepdims=True)
        )
        out_ref[...] = (cot_ref[...].astype(F32) + dx).astype(BF16)


def params(kib=LIMIT, **more):
    return pltpu.CompilerParams(vmem_limit_bytes=kib * 1024, **more)


def cost(us):
    flops = int(us * 3.0e8)
    return pl.CostEstimate(flops=flops, bytes_accessed=1 << 20, transcendentals=0)


def paired(value, axis, mask):
    count = lax.axis_size(axis)
    return lax.ppermute(value, axis, [(i, i ^ mask) for i in range(count)])


def shifted(value, by):
    return lax.ppermute(value, "seq", [(i, (i + by) % H) for i in range(H)])


def layer(tokens, cotangent, stamps, lengths, w_qkvu, w_out, gain_in, gain_out, bias_table):
    x = tokens[0]
    cot = cotangent[0]
    gain_in = gain_in.reshape(1, D)
    gain_out = gain_out.reshape(1, D)

    na, nb, early, late, copies = pl.pallas_call(
        prep_kernel,
        out_shape=[
            jax.ShapeDtypeStruct((64, D), BF16),
            jax.ShapeDtypeStruct((64, D), BF16),
            jax.ShapeDtypeStruct((32, 2 * D), BF16),
            jax.ShapeDtypeStruct((32, 3 * D), BF16),
            jax.ShapeDtypeStruct((32, 32, 3 * DH), BF16),
        ],
        in_specs=[VMEM] * 4,
        out_specs=[VMEM] * 5,
        compiler_params=params(61500),
        cost_estimate=cost(2),
        name="prep",
    )(x, gain_in, w_qkvu, w_out)
    w_early = lax.all_gather(early, DP, axis=0, tiled=True)
    w_late = lax.all_gather(late, DP, axis=0, tiled=True)
    ws = lax.all_to_all(copies, DP, 0, 0, tiled=True)
    ws = ws.reshape(D, 3 * DH)

    arrived = {(0, 0): na, (0, 1): nb}
    for k in range(1, 5):
        arrived[(-k, 0)] = shifted(arrived[(1 - k, 0)], 1)
        arrived[(k, 1)] = shifted(arrived[(k - 1, 1)], -1)
        if k < 4:
            arrived[(-k, 1)] = shifted(arrived[(1 - k, 1)], 1)
            arrived[(k, 0)] = shifted(arrived[(k - 1, 0)], -1)

    msg, proj, weight, slope = pl.pallas_call(
        forward_kernel,
        out_shape=[
            jax.ShapeDtypeStruct((H, MSG, T), BF16),
            jax.ShapeDtypeStruct((S, 3 * DH), F32),
            jax.ShapeDtypeStruct((S, S), BF16),
            jax.ShapeDtypeStruct((S, S), BF16),
        ],
        in_specs=[SMEM, SMEM] + [VMEM] * 18,
        out_specs=[VMEM] * 4,
        scratch_shapes=[
            pltpu.VMEM((S, D), BF16),
            pltpu.VMEM((S, T), F32),
            pltpu.VMEM((S, DH), BF16),
            pltpu.VMEM((S, DH), BF16),
            pltpu.VMEM((DH, S), BF16),
            pltpu.VMEM((TI, TI), F32),
        ],
        compiler_params=params(),
        cost_estimate=cost(10),
        name="attend",
    )(lengths, bias_table, *[arrived[a] for a in ARRIVALS], ws, stamps)

    att_msg = lax.all_to_all(msg, "seq", 0, 0, tiled=True)

    mixed, d_pg, w_own, w_send, *d_att = pl.pallas_call(
        tail_kernel,
        grid=(1,),
        out_shape=[
            jax.ShapeDtypeStruct((T, D), BF16),
            jax.ShapeDtypeStruct((T, D), BF16),
            jax.ShapeDtypeStruct((D // 2, D), BF16),
            jax.ShapeDtypeStruct((D // 2, D), BF16),
        ]
        + [jax.ShapeDtypeStruct((T, DH), BF16)] * H,
        in_specs=[SMEM]
        + [VMEM] * 5
        + [
            pl.BlockSpec((D, D), lambda i: (0, 0)),
            pl.BlockSpec((D, D), lambda i: (0, 1)),
            VMEM,
        ],
        out_specs=[VMEM] * (4 + H),
        scratch_shapes=[
            pltpu.VMEM((T, D), F32),
            pltpu.VMEM((H, T, DH), BF16),
            pltpu.VMEM((T, D), BF16),
            pltpu.VMEM((T, D), F32),
            pltpu.VMEM((T, D), F32),
        ],
        compiler_params=params(),
        cost_estimate=cost(5),
        name="tail",
    )(lengths, att_msg, na, nb, x, cot, w_early, w_early, gain_out)

    d_all = {0: d_att[0]}
    for k in ORDER:
        d_all[k] = shifted(d_att[k], k)

    gate_call = pl.pallas_call(
        gate_kernel,
        grid=(1,),
        out_shape=jax.ShapeDtypeStruct((T, D), F32),
        in_specs=[VMEM, pl.BlockSpec((D, D), lambda i: (0, 0))],
        out_specs=VMEM,
        compiler_params=params(),
        cost_estimate=cost(2),
        name="gate",
    )
    gate_back = gate_call(d_pg, w_early)

    other = paired(w_send, "dp_2", 1)
    pair = (w_own.astype(F32) + other.astype(F32)).astype(BF16)

    attend_back = pl.pallas_call(
        backward_kernel,
        out_shape=[jax.ShapeDtypeStruct((T, 3 * DH), BF16)] * H,
        in_specs=[VMEM] * (3 + H),
        out_specs=[VMEM] * H,
        scratch_shapes=[
            pltpu.VMEM((S, DH), BF16),
            pltpu.VMEM((S, DH), BF16),
            pltpu.VMEM((DH, S), BF16),
            pltpu.VMEM((S, DH), BF16),
            pltpu.VMEM((S, S), BF16),
            pltpu.VMEM((DH, S), F32),
            pltpu.VMEM((H, T, 3 * DH), BF16),
            pltpu.VMEM((H, T, DH), BF16),
        ],
        compiler_params=params(24000),
        cost_estimate=cost(6),
        name="attend_back",
    )
    d_proj = attend_back(*[d_all[k] for k in range(H)], proj, weight, slope)

    pair, first = lax.optimization_barrier((pair, d_proj[0]))
    d_proj = [first, *d_proj[1:]]
    planes = lax.all_to_all(pair.reshape(16, 32, D), ("dp_0", "dp_1"), 0, 0, tiled=True)

    total = jnp.sum(planes.astype(F32), axis=0)
    for mask in (1, 3, 7):
        own = total.astype(BF16)
        far = paired(own, "seq", mask)
        total = own.astype(F32) + far.astype(F32)
    w_grad = total

    d_rows = {0: d_proj[0]}
    for k in ORDER:
        d_rows[k] = shifted(d_proj[k], k)

    final = pl.pallas_call(
        final_kernel,
        grid=(3,),
        out_shape=jax.ShapeDtypeStruct((T, D), BF16),
        in_specs=[VMEM] * (H + 1)
        + [pl.BlockSpec((D, D), lambda b: (0, b)), VMEM, VMEM, VMEM],
        out_specs=VMEM,
        scratch_shapes=[
            pltpu.VMEM((H, T, 3 * DH), BF16),
            pltpu.VMEM((3, T, D), BF16),
            pltpu.VMEM((T, D), F32),
        ],
        compiler_params=params(dimension_semantics=("arbitrary",)),
        cost_estimate=cost(5),
        name="final",
    )
    input_grad = final(
        *[d_rows[k] for k in range(H)], gate_back, w_late, x, cot, gain_in
    )

    return (mixed[None], input_grad[None], w_grad)


def solution(mesh):
    finer = Mesh(mesh.devices.reshape(4, 4, 2, mesh.shape["seq"]), (*DP, "seq"))
    placed = (
        P(DP, "seq", None),
        P(DP, "seq", None),
        P(DP, None),
        P(DP),
        P(DP, None),
        P(DP, None),
        P(),
        P(),
        P(),
    )
    return jax.shard_map(
        layer,
        mesh=finer,
        in_specs=placed,
        out_specs=(P(DP, "seq", None), P(DP, "seq", None), P(DP, None)),
        check_vma=False,
    )
```

```python
import jax
import jax.numpy as jnp
from jax import lax
from jax.experimental import pallas as pl
from jax.experimental.pallas import tpu as pltpu
from jax.sharding import Mesh
from jax.sharding import PartitionSpec as P


H = 8
DH = 128
D = 1024
T = 128
S = 1024
NB = 16
TI = 256
CH = 32
DP = ("dp_0", "dp_1", "dp_2")
EPS = 1e-05
MSG = 144
LIMIT = 52000
UNROLL = 8
F32 = jnp.float32
BF16 = jnp.bfloat16

ORDER = (4, 5, 3, 6, 2, 7, 1)

VMEM = pl.BlockSpec(memory_space=pltpu.VMEM)
SMEM = pl.BlockSpec(memory_space=pltpu.SMEM)


def sigmoid(v):
    return 0.5 * jnp.tanh(0.5 * v) + 0.5


def nt(a, b):
    return lax.dot_general(a, b, (((1,), (1,)), ((), ())), preferred_element_type=F32)


def tn(a, b):
    return lax.dot_general(a, b, (((0,), (0,)), ((), ())), preferred_element_type=F32)


def mm(a, b):
    return jnp.dot(a, b, preferred_element_type=F32)


def prep_kernel(
    x_ref, gain_ref, w_ref, wout_ref, a_ref, b_ref, all_ref, copies_ref
):
    me = lax.axis_index("seq")
    x = x_ref[...].astype(F32)
    c = x - jnp.mean(x, axis=-1, keepdims=True)
    var = jnp.mean(c * c, axis=-1, keepdims=True)
    n = (c * lax.rsqrt(var + EPS) * gain_ref[...]).astype(BF16)
    a_ref[...] = n[:64]
    b_ref[...] = n[64:]
    all_ref[:, : 4 * D] = w_ref[...]
    all_ref[:, 4 * D :] = wout_ref[...]
    for part in range(3):
        at = pl.multiple_of((part + 1) * D + me * DH, DH)
        own = w_ref[:, pl.ds(at, DH)]
        for n in range(32):
            copies_ref[n, :, part * DH : (part + 1) * DH] = own


ARRIVALS = (
    [(0, 0), (0, 1)]
    + [(-k, 0) for k in (1, 2, 3, 4)]
    + [(-k, 1) for k in (1, 2, 3)]
    + [(k, 0) for k in (1, 2, 3)]
    + [(k, 1) for k in (1, 2, 3, 4)]
)


def forward_kernel(*refs):
    length_ref, bias_ref = refs[0], refs[1]
    blocks = refs[2:18]
    ws_ref, row_ref = refs[18:20]
    msg_ref, proj_ref, w_ref, g_ref = refs[20:24]
    x_all, col_sc, q_sc, k_sc, vt_sc, s_sc = refs[24:]
    me, length = lax.axis_index("seq"), length_ref[0]
    for (far, half), blk in zip(ARRIVALS, blocks):
        at = lax.rem(me + far + H, H) * T + half * 64
        x_all[pl.ds(pl.multiple_of(at, 64), 64), :] = blk[...]

    proj_ref[...] = mm(x_all[...], ws_ref[...])
    for c in range(8):
        cols = slice(c * T, (c + 1) * T)
        col_sc[cols, :] = jnp.broadcast_to(row_ref[:, cols].astype(F32), (T, T)).T
    for c in range(8):
        rows = slice(c * T, (c + 1) * T)
        p = proj_ref[rows, :]
        a = p * sigmoid(p)
        vt_sc[:, rows] = a[:, :DH].T.astype(BF16)
        q_sc[rows, :] = a[:, DH : 2 * DH].astype(BF16)
        k_sc[rows, :] = a[:, 2 * DH :].astype(BF16)
    scale = DH ** (-0.5)
    levels = [bias_ref[me, b] for b in range(NB)]

    def tile(i0, j0, diagonal):
        s_sc[...] = nt(k_sc[pl.ds(j0, TI), :], q_sc[i0 : i0 + TI, :])

        def chunk(c, carry):
            at = pl.multiple_of(c * CH, CH)
            rows = pl.ds(pl.multiple_of(j0 + at, CH), CH)
            col = col_sc[rows, :]
            e = row_ref[:, i0 : i0 + TI].astype(F32) - jnp.concatenate([col, col], axis=1)
            bias = jnp.full((CH, TI), levels[0], F32)
            for b in range(1, NB):
                bias = jnp.where(e >= float(2**b - 1), levels[b], bias)
            s = s_sc[pl.ds(at, CH), :] * scale + bias
            sg = sigmoid(s)
            w = s * sg
            g = sg + w * (1.0 - sg)
            if diagonal:
                jj = lax.broadcasted_iota(jnp.int32, (CH, TI), 0) + at
                ii = lax.broadcasted_iota(jnp.int32, (CH, TI), 1)
                keep = jj <= ii
                w = jnp.where(keep, w, 0.0)
                g = jnp.where(keep, g, 0.0)
            w_ref[rows, i0 : i0 + TI] = w.astype(BF16)
            g_ref[rows, i0 : i0 + TI] = g.astype(BF16)
            return carry

        lax.fori_loop(0, TI // CH, chunk, 0, unroll=UNROLL)

    for bi in range(S // TI):
        i0 = bi * TI
        if bi:

            def below(bj, carry, i0=i0):
                tile(i0, pl.multiple_of(bj * TI, TI), False)
                return carry

            lax.fori_loop(0, bi, below, 0)
        tile(i0, i0, True)
        att = mm(vt_sc[:, : i0 + TI], w_ref[: i0 + TI, i0 : i0 + TI])
        pos = lax.broadcasted_iota(jnp.int32, (DH, TI), 1) + i0
        att = jnp.where(pos < length, att, 0.0)
        mean = jnp.mean(att, axis=0, keepdims=True)
        high = mean.astype(BF16)
        left = mean - high.astype(F32)
        mid = left.astype(BF16)
        low = (left - mid.astype(F32)).astype(BF16)
        kept = high.astype(F32) + mid.astype(F32) + low.astype(F32)
        centred = (att - kept).astype(BF16)
        which = lax.broadcasted_iota(jnp.int32, (16, TI), 0)
        tail = jnp.where(
            which == 0,
            high.astype(F32),
            jnp.where(which == 1, mid.astype(F32), jnp.where(which == 2, low.astype(F32), 0.0)),
        ).astype(BF16)
        for t in range(TI // T):
            dest = bi * (TI // T) + t
            msg_ref[dest, :DH, :] = centred[:, t * T : (t + 1) * T]
            msg_ref[dest, DH:, :] = tail[:, t * T : (t + 1) * T]


def tail_kernel(
    length_ref,
    msg_ref,
    na_ref,
    nb_ref,
    x_ref,
    cot_ref,
    wg_ref,
    wo_ref,
    gain_ref,
    mixed_ref,
    dpg_ref,
    own_ref,
    send_ref,
    *more,
):
    datt_out, (att_sc, datt_ref, rows_sc, pg_sc, dmix_sc) = more[:H], more[H:]
    me, core, length = lax.axis_index("seq"), lax.axis_index("dp_2"), length_ref[0]
    for h in range(H):
        blk = msg_ref[h].astype(F32)
        att_t = blk[:DH] + (blk[DH : DH + 1] + blk[DH + 1 : DH + 2] + blk[DH + 2 : DH + 3])
        att_sc[:, h * DH : (h + 1) * DH] = att_t.T
    rows_sc[:64, :] = na_ref[...]
    rows_sc[64:, :] = nb_ref[...]
    cot = cot_ref[...]

    def columns(n, carry):
        at = pl.ds(pl.multiple_of(n * 512, 512), 512)
        pg_sc[:, at] = mm(rows_sc[...], wg_ref[:, at])
        dmix_sc[:, at] = nt(cot, wo_ref[at, :])
        return carry

    lax.fori_loop(0, D // 512, columns, 0)
    pg = pg_sc[...]
    d_mix = dmix_sc[...]
    att = att_sc[...]
    gain = gain_ref[...]
    c = att - jnp.mean(att, axis=-1, keepdims=True)
    var = jnp.mean(c * c, axis=-1, keepdims=True)
    r = lax.rsqrt(var + EPS)
    xhat = c * r
    normed_att = xhat * gain
    sg = sigmoid(pg)
    gate = pg * sg
    mixed_rows = (normed_att * gate).astype(BF16)
    rows_sc[...] = mixed_rows
    dpg_ref[...] = (d_mix * normed_att * (sg + gate * (1.0 - sg))).astype(BF16)
    u = d_mix * gate * gain
    d_att = r * (
        u
        - jnp.mean(u, axis=-1, keepdims=True)
        - xhat * jnp.mean(u * xhat, axis=-1, keepdims=True)
    )
    pos = lax.broadcasted_iota(jnp.int32, (T, D), 0) + me * T
    d_att = jnp.where(pos < length, d_att, 0.0).astype(BF16)
    for h in range(H):
        datt_ref[h] = d_att[:, h * DH : (h + 1) * DH]

    for h in range(H):
        part = tn(rows_sc[:, h * DH : (h + 1) * DH], cot).astype(BF16)
        for t in range(2):
            at = slice((2 * h + t) * 32, (2 * h + t + 1) * 32)
            even, odd = part[t * 64 : t * 64 + 32], part[t * 64 + 32 : t * 64 + 64]
            own_ref[at, :] = jnp.where(core == 0, even, odd)
            send_ref[at, :] = jnp.where(core == 0, odd, even)
    mixed_ref[...] = (x_ref[...].astype(F32) + mm(rows_sc[...], wo_ref[...])).astype(BF16)
    for k in range(H):
        datt_out[k][...] = datt_ref[lax.rem(me + k, H)]


def gate_kernel(dpg_ref, wg_ref, out_ref):
    def columns(n, carry):
        at = pl.ds(pl.multiple_of(n * 256, 256), 256)
        out_ref[:, at] = nt(dpg_ref[...], wg_ref[at, :])
        return carry

    lax.fori_loop(0, D // 256, columns, 0)


def backward_kernel(*refs):
    blocks = refs[:8]
    proj_ref, w_ref, g_ref = refs[8:11]
    outs = refs[11:19]
    me = lax.axis_index("seq")
    q_sc, k_sc, kt_sc, v_sc, ds_sc, dqt_sc, out_ref, d_ref = refs[19:]
    for k in range(H):
        d_ref[lax.rem(me - k + H, H)] = blocks[k][...]
    for c in range(8):
        rows = slice(c * T, (c + 1) * T)
        p = proj_ref[rows, :]
        a = p * sigmoid(p)
        v_sc[rows, :] = a[:, :DH].astype(BF16)
        q_sc[rows, :] = a[:, DH : 2 * DH].astype(BF16)
        k_sc[rows, :] = a[:, 2 * DH :].astype(BF16)
        kt_sc[:, rows] = a[:, 2 * DH :].T.astype(BF16)
    scale = DH ** (-0.5)
    d = d_ref[...].reshape(S, DH)
    for bj in range(S // TI):
        j0 = bj * TI
        rows = slice(j0, j0 + TI)
        dw = nt(v_sc[rows, :], d[j0:, :])
        ds_sc[rows, j0:] = (dw * g_ref[rows, j0:].astype(F32)).astype(BF16)
        dk = mm(ds_sc[rows, j0:], q_sc[j0:, :]) * scale
        dv = mm(w_ref[rows, j0:], d[j0:, :])
        for t in range(TI // T):
            at = slice(j0 + t * T, j0 + (t + 1) * T)
            dest = bj * (TI // T) + t
            for n, grad in ((0, dv), (2, dk)):
                p = proj_ref[at, n * DH : (n + 1) * DH]
                sg = sigmoid(p)
                slope = sg * (1.0 + p * (1.0 - sg))
                out_ref[dest, :, n * DH : (n + 1) * DH] = (
                    grad[t * T : (t + 1) * T] * slope
                ).astype(BF16)
    for bi in range(S // TI):
        i0 = bi * TI
        dqt_sc[:, i0 : i0 + TI] = (
            mm(kt_sc[:, : i0 + TI], ds_sc[: i0 + TI, i0 : i0 + TI]) * scale
        )
    for t in range(8):
        at = slice(t * T, (t + 1) * T)
        p = proj_ref[at, DH : 2 * DH]
        sg = sigmoid(p)
        slope = sg * (1.0 + p * (1.0 - sg))
        out_ref[t, :, DH : 2 * DH] = (dqt_sc[:, at].T * slope).astype(BF16)
    for k in range(H):
        outs[k][...] = out_ref[lax.rem(me + k, H)]


def final_kernel(*refs):
    blocks = refs[:8]
    back_ref, w_ref, x_ref, cot_ref, gain_ref, out_ref, msg_ref, lhs, acc = refs[8:]
    me = lax.axis_index("seq")
    b = pl.program_id(0)

    @pl.when(b == 0)
    def _():
        for k in range(H):
            msg_ref[lax.rem(me - k + H, H)] = blocks[k][...]
        for n in range(3):
            for h in range(H):
                lhs[n, :, h * DH : (h + 1) * DH] = msg_ref[h, :, n * DH : (n + 1) * DH]
        acc[...] = back_ref[...]

    def columns(n, carry):
        at = pl.ds(pl.multiple_of(n * 512, 512), 512)
        acc[:, at] += nt(lhs[b], w_ref[at, :])
        return carry

    lax.fori_loop(0, D // 512, columns, 0)

    @pl.when(b == 2)
    def _():
        x = x_ref[...].astype(F32)
        c = x - jnp.mean(x, axis=-1, keepdims=True)
        var = jnp.mean(c * c, axis=-1, keepdims=True)
        r = lax.rsqrt(var + EPS)
        xhat = c * r
        u = acc[...] * gain_ref[...]
        dx = r * (
            u
            - jnp.mean(u, axis=-1, keepdims=True)
            - xhat * jnp.mean(u * xhat, axis=-1, keepdims=True)
        )
        out_ref[...] = (cot_ref[...].astype(F32) + dx).astype(BF16)


def params(kib=LIMIT, **more):
    return pltpu.CompilerParams(vmem_limit_bytes=kib * 1024, **more)


def cost(us):
    flops = int(us * 3.0e8)
    return pl.CostEstimate(flops=flops, bytes_accessed=1 << 20, transcendentals=0)


def paired(value, axis, mask):
    count = lax.axis_size(axis)
    return lax.ppermute(value, axis, [(i, i ^ mask) for i in range(count)])


def shifted(value, by):
    return lax.ppermute(value, "seq", [(i, (i + by) % H) for i in range(H)])


def layer(tokens, cotangent, stamps, lengths, w_qkvu, w_out, gain_in, gain_out, bias_table):
    x = tokens[0]
    cot = cotangent[0]
    gain_in = gain_in.reshape(1, D)
    gain_out = gain_out.reshape(1, D)

    na, nb, w_rows, copies = pl.pallas_call(
        prep_kernel,
        out_shape=[
            jax.ShapeDtypeStruct((64, D), BF16),
            jax.ShapeDtypeStruct((64, D), BF16),
            jax.ShapeDtypeStruct((32, 5 * D), BF16),
            jax.ShapeDtypeStruct((32, 32, 3 * DH), BF16),
        ],
        in_specs=[VMEM] * 4,
        out_specs=[VMEM] * 4,
        compiler_params=params(61500),
        cost_estimate=cost(2),
        name="prep",
    )(x, gain_in, w_qkvu, w_out)
    w_full = lax.all_gather(w_rows, DP, axis=0, tiled=True)
    ws = lax.all_to_all(copies, DP, 0, 0, tiled=True)
    ws = ws.reshape(D, 3 * DH)

    arrived = {(0, 0): na, (0, 1): nb}
    for k in range(1, 5):
        arrived[(-k, 0)] = shifted(arrived[(1 - k, 0)], 1)
        arrived[(k, 1)] = shifted(arrived[(k - 1, 1)], -1)
        if k < 4:
            arrived[(-k, 1)] = shifted(arrived[(1 - k, 1)], 1)
            arrived[(k, 0)] = shifted(arrived[(k - 1, 0)], -1)

    msg, proj, weight, slope = pl.pallas_call(
        forward_kernel,
        out_shape=[
            jax.ShapeDtypeStruct((H, MSG, T), BF16),
            jax.ShapeDtypeStruct((S, 3 * DH), F32),
            jax.ShapeDtypeStruct((S, S), BF16),
            jax.ShapeDtypeStruct((S, S), BF16),
        ],
        in_specs=[SMEM, SMEM] + [VMEM] * 18,
        out_specs=[VMEM] * 4,
        scratch_shapes=[
            pltpu.VMEM((S, D), BF16),
            pltpu.VMEM((S, T), F32),
            pltpu.VMEM((S, DH), BF16),
            pltpu.VMEM((S, DH), BF16),
            pltpu.VMEM((DH, S), BF16),
            pltpu.VMEM((TI, TI), F32),
        ],
        compiler_params=params(),
        cost_estimate=cost(10),
        name="attend",
    )(lengths, bias_table, *[arrived[a] for a in ARRIVALS], ws, stamps)

    att_msg = lax.all_to_all(msg, "seq", 0, 0, tiled=True)

    mixed, d_pg, w_own, w_send, *d_att = pl.pallas_call(
        tail_kernel,
        grid=(1,),
        out_shape=[
            jax.ShapeDtypeStruct((T, D), BF16),
            jax.ShapeDtypeStruct((T, D), BF16),
            jax.ShapeDtypeStruct((D // 2, D), BF16),
            jax.ShapeDtypeStruct((D // 2, D), BF16),
        ]
        + [jax.ShapeDtypeStruct((T, DH), BF16)] * H,
        in_specs=[SMEM]
        + [VMEM] * 5
        + [
            pl.BlockSpec((D, D), lambda i: (0, 0)),
            pl.BlockSpec((D, D), lambda i: (0, 4)),
            VMEM,
        ],
        out_specs=[VMEM] * (4 + H),
        scratch_shapes=[
            pltpu.VMEM((T, D), F32),
            pltpu.VMEM((H, T, DH), BF16),
            pltpu.VMEM((T, D), BF16),
            pltpu.VMEM((T, D), F32),
            pltpu.VMEM((T, D), F32),
        ],
        compiler_params=params(61500),
        cost_estimate=cost(5),
        name="tail",
    )(lengths, att_msg, na, nb, x, cot, w_full, w_full, gain_out)

    d_all = {0: d_att[0]}
    for k in ORDER:
        d_all[k] = shifted(d_att[k], k)

    gate_call = pl.pallas_call(
        gate_kernel,
        grid=(1,),
        out_shape=jax.ShapeDtypeStruct((T, D), F32),
        in_specs=[VMEM, pl.BlockSpec((D, D), lambda i: (0, 0))],
        out_specs=VMEM,
        compiler_params=params(),
        cost_estimate=cost(2),
        name="gate",
    )
    gate_back = gate_call(d_pg, w_full)

    other = paired(w_send, "dp_2", 1)
    pair = (w_own.astype(F32) + other.astype(F32)).astype(BF16)

    attend_back = pl.pallas_call(
        backward_kernel,
        out_shape=[jax.ShapeDtypeStruct((T, 3 * DH), BF16)] * H,
        in_specs=[VMEM] * (3 + H),
        out_specs=[VMEM] * H,
        scratch_shapes=[
            pltpu.VMEM((S, DH), BF16),
            pltpu.VMEM((S, DH), BF16),
            pltpu.VMEM((DH, S), BF16),
            pltpu.VMEM((S, DH), BF16),
            pltpu.VMEM((S, S), BF16),
            pltpu.VMEM((DH, S), F32),
            pltpu.VMEM((H, T, 3 * DH), BF16),
            pltpu.VMEM((H, T, DH), BF16),
        ],
        compiler_params=params(24000),
        cost_estimate=cost(6),
        name="attend_back",
    )
    d_proj = attend_back(*[d_all[k] for k in range(H)], proj, weight, slope)

    pair, first = lax.optimization_barrier((pair, d_proj[0]))
    d_proj = [first, *d_proj[1:]]
    planes = lax.all_to_all(pair.reshape(16, 32, D), ("dp_0", "dp_1"), 0, 0, tiled=True)

    total = jnp.sum(planes.astype(F32), axis=0)
    for mask in (1, 3, 7):
        own = total.astype(BF16)
        far = paired(own, "seq", mask)
        total = own.astype(F32) + far.astype(F32)
    w_grad = total

    d_rows = {0: d_proj[0]}
    for k in ORDER:
        d_rows[k] = shifted(d_proj[k], k)

    final = pl.pallas_call(
        final_kernel,
        grid=(3,),
        out_shape=jax.ShapeDtypeStruct((T, D), BF16),
        in_specs=[VMEM] * (H + 1)
        + [pl.BlockSpec((D, D), lambda b: (0, b + 1)), VMEM, VMEM, VMEM],
        out_specs=VMEM,
        scratch_shapes=[
            pltpu.VMEM((H, T, 3 * DH), BF16),
            pltpu.VMEM((3, T, D), BF16),
            pltpu.VMEM((T, D), F32),
        ],
        compiler_params=params(dimension_semantics=("arbitrary",)),
        cost_estimate=cost(5),
        name="final",
    )
    input_grad = final(
        *[d_rows[k] for k in range(H)], gate_back, w_full, x, cot, gain_in
    )

    return (mixed[None], input_grad[None], w_grad)


def solution(mesh):
    finer = Mesh(mesh.devices.reshape(4, 4, 2, mesh.shape["seq"]), (*DP, "seq"))
    placed = (
        P(DP, "seq", None),
        P(DP, "seq", None),
        P(DP, None),
        P(DP),
        P(DP, None),
        P(DP, None),
        P(),
        P(),
        P(),
    )
    return jax.shard_map(
        layer,
        mesh=finer,
        in_specs=placed,
        out_specs=(P(DP, "seq", None), P(DP, "seq", None), P(DP, None)),
        check_vma=False,
    )
```

```python
import jax
import jax.numpy as jnp
from jax import lax
from jax.experimental import pallas as pl
from jax.experimental.pallas import tpu as pltpu
from jax.sharding import Mesh
from jax.sharding import PartitionSpec as P


H = 8
DH = 128
D = 1024
T = 128
S = 1024
NB = 16
TI = 256
CH = 32
DP = ("dp_0", "dp_1", "dp_2")
EPS = 1e-05
MSG = 144
LIMIT = 52000
UNROLL = 8
F32 = jnp.float32
BF16 = jnp.bfloat16

ORDER = (4, 5, 3, 6, 2, 7, 1)

VMEM = pl.BlockSpec(memory_space=pltpu.VMEM)
SMEM = pl.BlockSpec(memory_space=pltpu.SMEM)


def sigmoid(v):
    return 0.5 * jnp.tanh(0.5 * v) + 0.5


def nt(a, b):
    return lax.dot_general(a, b, (((1,), (1,)), ((), ())), preferred_element_type=F32)


def tn(a, b):
    return lax.dot_general(a, b, (((0,), (0,)), ((), ())), preferred_element_type=F32)


def mm(a, b):
    return jnp.dot(a, b, preferred_element_type=F32)


def prep_kernel(
    x_ref, gain_ref, w_ref, wout_ref, a_ref, b_ref, all_ref, copies_ref
):
    me = lax.axis_index("seq")
    x = x_ref[...].astype(F32)
    c = x - jnp.mean(x, axis=-1, keepdims=True)
    var = jnp.mean(c * c, axis=-1, keepdims=True)
    n = (c * lax.rsqrt(var + EPS) * gain_ref[...]).astype(BF16)
    a_ref[...] = n[:64]
    b_ref[...] = n[64:]
    all_ref[:, : 4 * D] = w_ref[...]
    all_ref[:, 4 * D :] = wout_ref[...]
    for part in range(3):
        at = pl.multiple_of((part + 1) * D + me * DH, DH)
        own = w_ref[:, pl.ds(at, DH)]
        for n in range(32):
            copies_ref[n, :, part * DH : (part + 1) * DH] = own


ARRIVALS = (
    [(0, 0), (0, 1)]
    + [(-k, 0) for k in (1, 2, 3, 4)]
    + [(-k, 1) for k in (1, 2, 3)]
    + [(k, 0) for k in (1, 2, 3)]
    + [(k, 1) for k in (1, 2, 3, 4)]
)


def forward_kernel(*refs):
    length_ref, bias_ref = refs[0], refs[1]
    blocks = refs[2:18]
    ws_ref, row_ref = refs[18:20]
    msg_ref, proj_ref, w_ref, g_ref = refs[20:24]
    x_all, col_sc, q_sc, k_sc, vt_sc, s_sc = refs[24:]
    me, length = lax.axis_index("seq"), length_ref[0]
    for (far, half), blk in zip(ARRIVALS, blocks):
        at = lax.rem(me + far + H, H) * T + half * 64
        x_all[pl.ds(pl.multiple_of(at, 64), 64), :] = blk[...]

    proj_ref[...] = mm(x_all[...], ws_ref[...])
    for c in range(8):
        cols = slice(c * T, (c + 1) * T)
        col_sc[cols, :] = jnp.broadcast_to(row_ref[:, cols].astype(F32), (T, T)).T
    for c in range(8):
        rows = slice(c * T, (c + 1) * T)
        p = proj_ref[rows, :]
        a = p * sigmoid(p)
        vt_sc[:, rows] = a[:, :DH].T.astype(BF16)
        q_sc[rows, :] = a[:, DH : 2 * DH].astype(BF16)
        k_sc[rows, :] = a[:, 2 * DH :].astype(BF16)
    scale = DH ** (-0.5)
    levels = [bias_ref[me, b] for b in range(NB)]

    def tile(i0, j0, diagonal):
        s_sc[...] = nt(k_sc[pl.ds(j0, TI), :], q_sc[i0 : i0 + TI, :])

        def chunk(c, carry):
            at = pl.multiple_of(c * CH, CH)
            rows = pl.ds(pl.multiple_of(j0 + at, CH), CH)
            col = col_sc[rows, :]
            e = row_ref[:, i0 : i0 + TI].astype(F32) - jnp.concatenate([col, col], axis=1)
            bias = jnp.full((CH, TI), levels[0], F32)
            for b in range(1, NB):
                bias = jnp.where(e >= float(2**b - 1), levels[b], bias)
            s = s_sc[pl.ds(at, CH), :] * scale + bias
            sg = sigmoid(s)
            w = s * sg
            g = sg + w * (1.0 - sg)
            if diagonal:
                jj = lax.broadcasted_iota(jnp.int32, (CH, TI), 0) + at
                ii = lax.broadcasted_iota(jnp.int32, (CH, TI), 1)
                keep = jj <= ii
                w = jnp.where(keep, w, 0.0)
                g = jnp.where(keep, g, 0.0)
            w_ref[rows, i0 : i0 + TI] = w.astype(BF16)
            g_ref[rows, i0 : i0 + TI] = g.astype(BF16)
            return carry

        lax.fori_loop(0, TI // CH, chunk, 0, unroll=UNROLL)

    for bi in range(S // TI):
        i0 = bi * TI
        if bi:

            def below(bj, carry, i0=i0):
                tile(i0, pl.multiple_of(bj * TI, TI), False)
                return carry

            lax.fori_loop(0, bi, below, 0)
        tile(i0, i0, True)
        att = mm(vt_sc[:, : i0 + TI], w_ref[: i0 + TI, i0 : i0 + TI])
        pos = lax.broadcasted_iota(jnp.int32, (DH, TI), 1) + i0
        att = jnp.where(pos < length, att, 0.0)
        mean = jnp.mean(att, axis=0, keepdims=True)
        high = mean.astype(BF16)
        left = mean - high.astype(F32)
        mid = left.astype(BF16)
        low = (left - mid.astype(F32)).astype(BF16)
        kept = high.astype(F32) + mid.astype(F32) + low.astype(F32)
        centred = (att - kept).astype(BF16)
        which = lax.broadcasted_iota(jnp.int32, (16, TI), 0)
        tail = jnp.where(
            which == 0,
            high.astype(F32),
            jnp.where(which == 1, mid.astype(F32), jnp.where(which == 2, low.astype(F32), 0.0)),
        ).astype(BF16)
        for t in range(TI // T):
            dest = bi * (TI // T) + t
            msg_ref[dest, :DH, :] = centred[:, t * T : (t + 1) * T]
            msg_ref[dest, DH:, :] = tail[:, t * T : (t + 1) * T]


def tail_kernel(
    length_ref,
    msg_ref,
    na_ref,
    nb_ref,
    x_ref,
    cot_ref,
    wg_ref,
    wo_ref,
    gain_ref,
    mixed_ref,
    dpg_ref,
    own_ref,
    send_ref,
    *more,
):
    datt_out, (att_sc, datt_ref, rows_sc, pg_sc, dmix_sc) = more[:H], more[H:]
    me, core, length = lax.axis_index("seq"), lax.axis_index("dp_2"), length_ref[0]
    for h in range(H):
        blk = msg_ref[h].astype(F32)
        att_t = blk[:DH] + (blk[DH : DH + 1] + blk[DH + 1 : DH + 2] + blk[DH + 2 : DH + 3])
        att_sc[:, h * DH : (h + 1) * DH] = att_t.T
    rows_sc[:64, :] = na_ref[...]
    rows_sc[64:, :] = nb_ref[...]
    cot = cot_ref[...]

    def columns(n, carry):
        at = pl.ds(pl.multiple_of(n * 512, 512), 512)
        pg_sc[:, at] = mm(rows_sc[...], wg_ref[:, at])
        dmix_sc[:, at] = nt(cot, wo_ref[at, :])
        return carry

    lax.fori_loop(0, D // 512, columns, 0)
    pg = pg_sc[...]
    d_mix = dmix_sc[...]
    att = att_sc[...]
    gain = gain_ref[...]
    c = att - jnp.mean(att, axis=-1, keepdims=True)
    var = jnp.mean(c * c, axis=-1, keepdims=True)
    r = lax.rsqrt(var + EPS)
    xhat = c * r
    normed_att = xhat * gain
    sg = sigmoid(pg)
    gate = pg * sg
    mixed_rows = (normed_att * gate).astype(BF16)
    rows_sc[...] = mixed_rows
    dpg_ref[...] = (d_mix * normed_att * (sg + gate * (1.0 - sg))).astype(BF16)
    u = d_mix * gate * gain
    d_att = r * (
        u
        - jnp.mean(u, axis=-1, keepdims=True)
        - xhat * jnp.mean(u * xhat, axis=-1, keepdims=True)
    )
    pos = lax.broadcasted_iota(jnp.int32, (T, D), 0) + me * T
    d_att = jnp.where(pos < length, d_att, 0.0).astype(BF16)
    for h in range(H):
        datt_ref[h] = d_att[:, h * DH : (h + 1) * DH]

    for h in range(H):
        part = tn(rows_sc[:, h * DH : (h + 1) * DH], cot).astype(BF16)
        for t in range(2):
            at = slice((2 * h + t) * 32, (2 * h + t + 1) * 32)
            even, odd = part[t * 64 : t * 64 + 32], part[t * 64 + 32 : t * 64 + 64]
            own_ref[at, :] = jnp.where(core == 0, even, odd)
            send_ref[at, :] = jnp.where(core == 0, odd, even)
    mixed_ref[...] = (x_ref[...].astype(F32) + mm(rows_sc[...], wo_ref[...])).astype(BF16)
    for k in range(H):
        datt_out[k][...] = datt_ref[lax.rem(me + k, H)]


def backward_kernel(*refs):
    blocks = refs[:8]
    proj_ref, w_ref, g_ref = refs[8:11]
    outs = refs[11:19]
    me = lax.axis_index("seq")
    q_sc, k_sc, kt_sc, v_sc, ds_sc, dqt_sc, out_ref, d_ref = refs[19:]
    for k in range(H):
        d_ref[lax.rem(me - k + H, H)] = blocks[k][...]
    for c in range(8):
        rows = slice(c * T, (c + 1) * T)
        p = proj_ref[rows, :]
        a = p * sigmoid(p)
        v_sc[rows, :] = a[:, :DH].astype(BF16)
        q_sc[rows, :] = a[:, DH : 2 * DH].astype(BF16)
        k_sc[rows, :] = a[:, 2 * DH :].astype(BF16)
        kt_sc[:, rows] = a[:, 2 * DH :].T.astype(BF16)
    scale = DH ** (-0.5)
    d = d_ref[...].reshape(S, DH)
    for bj in range(S // TI):
        j0 = bj * TI
        rows = slice(j0, j0 + TI)
        dw = nt(v_sc[rows, :], d[j0:, :])
        ds_sc[rows, j0:] = (dw * g_ref[rows, j0:].astype(F32)).astype(BF16)
        dk = mm(ds_sc[rows, j0:], q_sc[j0:, :]) * scale
        dv = mm(w_ref[rows, j0:], d[j0:, :])
        for t in range(TI // T):
            at = slice(j0 + t * T, j0 + (t + 1) * T)
            dest = bj * (TI // T) + t
            for n, grad in ((0, dv), (2, dk)):
                p = proj_ref[at, n * DH : (n + 1) * DH]
                sg = sigmoid(p)
                slope = sg * (1.0 + p * (1.0 - sg))
                out_ref[dest, :, n * DH : (n + 1) * DH] = (
                    grad[t * T : (t + 1) * T] * slope
                ).astype(BF16)
    for bi in range(S // TI):
        i0 = bi * TI
        dqt_sc[:, i0 : i0 + TI] = (
            mm(kt_sc[:, : i0 + TI], ds_sc[: i0 + TI, i0 : i0 + TI]) * scale
        )
    for t in range(8):
        at = slice(t * T, (t + 1) * T)
        p = proj_ref[at, DH : 2 * DH]
        sg = sigmoid(p)
        slope = sg * (1.0 + p * (1.0 - sg))
        out_ref[t, :, DH : 2 * DH] = (dqt_sc[:, at].T * slope).astype(BF16)
    for k in range(H):
        outs[k][...] = out_ref[lax.rem(me + k, H)]


def final_kernel(*refs):
    blocks = refs[:8]
    dpg_ref, w_ref, x_ref, cot_ref, gain_ref, out_ref, msg_ref, lhs, acc = refs[8:]
    me = lax.axis_index("seq")
    b = pl.program_id(0)

    @pl.when(b == 0)
    def _():
        for k in range(H):
            msg_ref[lax.rem(me - k + H, H)] = blocks[k][...]
        for n in range(3):
            for h in range(H):
                lhs[n + 1, :, h * DH : (h + 1) * DH] = msg_ref[h, :, n * DH : (n + 1) * DH]
        lhs[0] = dpg_ref[...]
        acc[...] = jnp.zeros_like(acc)

    def columns(n, carry):
        at = pl.ds(pl.multiple_of(n * 512, 512), 512)
        acc[:, at] += nt(lhs[b], w_ref[at, :])
        return carry

    lax.fori_loop(0, D // 512, columns, 0)

    @pl.when(b == 3)
    def _():
        x = x_ref[...].astype(F32)
        c = x - jnp.mean(x, axis=-1, keepdims=True)
        var = jnp.mean(c * c, axis=-1, keepdims=True)
        r = lax.rsqrt(var + EPS)
        xhat = c * r
        u = acc[...] * gain_ref[...]
        dx = r * (
            u
            - jnp.mean(u, axis=-1, keepdims=True)
            - xhat * jnp.mean(u * xhat, axis=-1, keepdims=True)
        )
        out_ref[...] = (cot_ref[...].astype(F32) + dx).astype(BF16)


def params(kib=LIMIT, **more):
    return pltpu.CompilerParams(vmem_limit_bytes=kib * 1024, **more)


def cost(us):
    flops = int(us * 3.0e8)
    return pl.CostEstimate(flops=flops, bytes_accessed=1 << 20, transcendentals=0)


def paired(value, axis, mask):
    count = lax.axis_size(axis)
    return lax.ppermute(value, axis, [(i, i ^ mask) for i in range(count)])


def shifted(value, by):
    return lax.ppermute(value, "seq", [(i, (i + by) % H) for i in range(H)])


def layer(tokens, cotangent, stamps, lengths, w_qkvu, w_out, gain_in, gain_out, bias_table):
    x = tokens[0]
    cot = cotangent[0]
    gain_in = gain_in.reshape(1, D)
    gain_out = gain_out.reshape(1, D)

    na, nb, w_rows, copies = pl.pallas_call(
        prep_kernel,
        out_shape=[
            jax.ShapeDtypeStruct((64, D), BF16),
            jax.ShapeDtypeStruct((64, D), BF16),
            jax.ShapeDtypeStruct((32, 5 * D), BF16),
            jax.ShapeDtypeStruct((32, 32, 3 * DH), BF16),
        ],
        in_specs=[VMEM] * 4,
        out_specs=[VMEM] * 4,
        compiler_params=params(61500),
        cost_estimate=cost(2),
        name="prep",
    )(x, gain_in, w_qkvu, w_out)
    w_full = lax.all_gather(w_rows, DP, axis=0, tiled=True)
    ws = lax.all_to_all(copies, DP, 0, 0, tiled=True)
    ws = ws.reshape(D, 3 * DH)

    arrived = {(0, 0): na, (0, 1): nb}
    for k in range(1, 5):
        arrived[(-k, 0)] = shifted(arrived[(1 - k, 0)], 1)
        arrived[(k, 1)] = shifted(arrived[(k - 1, 1)], -1)
        if k < 4:
            arrived[(-k, 1)] = shifted(arrived[(1 - k, 1)], 1)
            arrived[(k, 0)] = shifted(arrived[(k - 1, 0)], -1)

    msg, proj, weight, slope = pl.pallas_call(
        forward_kernel,
        out_shape=[
            jax.ShapeDtypeStruct((H, MSG, T), BF16),
            jax.ShapeDtypeStruct((S, 3 * DH), F32),
            jax.ShapeDtypeStruct((S, S), BF16),
            jax.ShapeDtypeStruct((S, S), BF16),
        ],
        in_specs=[SMEM, SMEM] + [VMEM] * 18,
        out_specs=[VMEM] * 4,
        scratch_shapes=[
            pltpu.VMEM((S, D), BF16),
            pltpu.VMEM((S, T), F32),
            pltpu.VMEM((S, DH), BF16),
            pltpu.VMEM((S, DH), BF16),
            pltpu.VMEM((DH, S), BF16),
            pltpu.VMEM((TI, TI), F32),
        ],
        compiler_params=params(),
        cost_estimate=cost(10),
        name="attend",
    )(lengths, bias_table, *[arrived[a] for a in ARRIVALS], ws, stamps)

    att_msg = lax.all_to_all(msg, "seq", 0, 0, tiled=True)

    mixed, d_pg, w_own, w_send, *d_att = pl.pallas_call(
        tail_kernel,
        grid=(1,),
        out_shape=[
            jax.ShapeDtypeStruct((T, D), BF16),
            jax.ShapeDtypeStruct((T, D), BF16),
            jax.ShapeDtypeStruct((D // 2, D), BF16),
            jax.ShapeDtypeStruct((D // 2, D), BF16),
        ]
        + [jax.ShapeDtypeStruct((T, DH), BF16)] * H,
        in_specs=[SMEM]
        + [VMEM] * 5
        + [
            pl.BlockSpec((D, D), lambda i: (0, 0)),
            pl.BlockSpec((D, D), lambda i: (0, 4)),
            VMEM,
        ],
        out_specs=[VMEM] * (4 + H),
        scratch_shapes=[
            pltpu.VMEM((T, D), F32),
            pltpu.VMEM((H, T, DH), BF16),
            pltpu.VMEM((T, D), BF16),
            pltpu.VMEM((T, D), F32),
            pltpu.VMEM((T, D), F32),
        ],
        compiler_params=params(),
        cost_estimate=cost(5),
        name="tail",
    )(lengths, att_msg, na, nb, x, cot, w_full, w_full, gain_out)

    d_all = {0: d_att[0]}
    for k in ORDER:
        d_all[k] = shifted(d_att[k], k)

    other = paired(w_send, "dp_2", 1)
    pair = (w_own.astype(F32) + other.astype(F32)).astype(BF16)
    planes = lax.all_to_all(pair.reshape(16, 32, D), ("dp_0", "dp_1"), 0, 0, tiled=True)

    attend_back = pl.pallas_call(
        backward_kernel,
        out_shape=[jax.ShapeDtypeStruct((T, 3 * DH), BF16)] * H,
        in_specs=[VMEM] * (3 + H),
        out_specs=[VMEM] * H,
        scratch_shapes=[
            pltpu.VMEM((S, DH), BF16),
            pltpu.VMEM((S, DH), BF16),
            pltpu.VMEM((DH, S), BF16),
            pltpu.VMEM((S, DH), BF16),
            pltpu.VMEM((S, S), BF16),
            pltpu.VMEM((DH, S), F32),
            pltpu.VMEM((H, T, 3 * DH), BF16),
            pltpu.VMEM((H, T, DH), BF16),
        ],
        compiler_params=params(63400),
        cost_estimate=cost(6),
        name="attend_back",
    )
    d_proj = attend_back(*[d_all[k] for k in range(H)], proj, weight, slope)

    total = jnp.sum(planes.astype(F32), axis=0)
    for mask in (1, 3, 7):
        own = total.astype(BF16)
        far = paired(own, "seq", mask)
        total = own.astype(F32) + far.astype(F32)
    w_grad = total

    d_rows = {0: d_proj[0]}
    for k in ORDER:
        d_rows[k] = shifted(d_proj[k], k)

    final = pl.pallas_call(
        final_kernel,
        grid=(4,),
        out_shape=jax.ShapeDtypeStruct((T, D), BF16),
        in_specs=[VMEM] * (H + 1)
        + [pl.BlockSpec((D, D), lambda b: (0, b)), VMEM, VMEM, VMEM],
        out_specs=VMEM,
        scratch_shapes=[
            pltpu.VMEM((H, T, 3 * DH), BF16),
            pltpu.VMEM((4, T, D), BF16),
            pltpu.VMEM((T, D), F32),
        ],
        compiler_params=params(dimension_semantics=("arbitrary",)),
        cost_estimate=cost(5),
        name="final",
    )
    input_grad = final(*[d_rows[k] for k in range(H)], d_pg, w_full, x, cot, gain_in)

    return (mixed[None], input_grad[None], w_grad)


def solution(mesh):
    finer = Mesh(mesh.devices.reshape(4, 4, 2, mesh.shape["seq"]), (*DP, "seq"))
    placed = (
        P(DP, "seq", None),
        P(DP, "seq", None),
        P(DP, None),
        P(DP),
        P(DP, None),
        P(DP, None),
        P(),
        P(),
        P(),
    )
    return jax.shard_map(
        layer,
        mesh=finer,
        in_specs=placed,
        out_specs=(P(DP, "seq", None), P(DP, "seq", None), P(DP, None)),
        check_vma=False,
    )
```

```python
import jax
import jax.numpy as jnp
from jax import lax
from jax.experimental import pallas as pl
from jax.experimental.pallas import tpu as pltpu
from jax.sharding import Mesh
from jax.sharding import PartitionSpec as P


H = 8
DH = 128
D = 1024
T = 128
S = 1024
NB = 16
TI = 256
CH = 32
DP = ("dp_0", "dp_1", "dp_2")
EPS = 1e-05
MSG = 144
LIMIT = 52000
UNROLL = 8
F32 = jnp.float32
BF16 = jnp.bfloat16

ORDER = (4, 5, 3, 6, 2, 7, 1)

VMEM = pl.BlockSpec(memory_space=pltpu.VMEM)
SMEM = pl.BlockSpec(memory_space=pltpu.SMEM)


def sigmoid(v):
    return 0.5 * jnp.tanh(0.5 * v) + 0.5


def nt(a, b):
    return lax.dot_general(a, b, (((1,), (1,)), ((), ())), preferred_element_type=F32)


def tn(a, b):
    return lax.dot_general(a, b, (((0,), (0,)), ((), ())), preferred_element_type=F32)


def mm(a, b):
    return jnp.dot(a, b, preferred_element_type=F32)


def prep_kernel(
    x_ref, gain_ref, w_ref, wout_ref, a_ref, b_ref, early_ref, late_ref, copies_ref
):
    me = lax.axis_index("seq")
    x = x_ref[...].astype(F32)
    c = x - jnp.mean(x, axis=-1, keepdims=True)
    var = jnp.mean(c * c, axis=-1, keepdims=True)
    n = (c * lax.rsqrt(var + EPS) * gain_ref[...]).astype(BF16)
    a_ref[...] = n[:64]
    b_ref[...] = n[64:]
    early_ref[:, :D] = w_ref[:, :D]
    early_ref[:, D:] = wout_ref[...]
    late_ref[...] = w_ref[:, D:]
    for part in range(3):
        at = pl.multiple_of((part + 1) * D + me * DH, DH)
        own = w_ref[:, pl.ds(at, DH)]
        for n in range(32):
            copies_ref[n, :, part * DH : (part + 1) * DH] = own


ARRIVALS = (
    [(0, 0), (0, 1)]
    + [(-k, 0) for k in (1, 2, 3, 4)]
    + [(-k, 1) for k in (1, 2, 3)]
    + [(k, 0) for k in (1, 2, 3)]
    + [(k, 1) for k in (1, 2, 3, 4)]
)


def forward_kernel(*refs):
    length_ref, bias_ref = refs[0], refs[1]
    blocks = refs[2:18]
    ws_ref, row_ref = refs[18:20]
    msg_ref, proj_ref, w_ref, g_ref = refs[20:24]
    x_all, col_sc, q_sc, k_sc, vt_sc, s_sc = refs[24:]
    me, length = lax.axis_index("seq"), length_ref[0]
    for (far, half), blk in zip(ARRIVALS, blocks):
        at = lax.rem(me + far + H, H) * T + half * 64
        x_all[pl.ds(pl.multiple_of(at, 64), 64), :] = blk[...]

    proj_ref[...] = mm(x_all[...], ws_ref[...])
    for c in range(8):
        cols = slice(c * T, (c + 1) * T)
        col_sc[cols, :] = jnp.broadcast_to(row_ref[:, cols].astype(F32), (T, T)).T
    for c in range(8):
        rows = slice(c * T, (c + 1) * T)
        p = proj_ref[rows, :]
        a = p * sigmoid(p)
        vt_sc[:, rows] = a[:, :DH].T.astype(BF16)
        q_sc[rows, :] = a[:, DH : 2 * DH].astype(BF16)
        k_sc[rows, :] = a[:, 2 * DH :].astype(BF16)
    scale = DH ** (-0.5)
    levels = [bias_ref[me, b] for b in range(NB)]

    def tile(i0, j0, diagonal):
        s_sc[...] = nt(k_sc[pl.ds(j0, TI), :], q_sc[i0 : i0 + TI, :])

        def chunk(c, carry):
            at = pl.multiple_of(c * CH, CH)
            rows = pl.ds(pl.multiple_of(j0 + at, CH), CH)
            col = col_sc[rows, :]
            e = row_ref[:, i0 : i0 + TI].astype(F32) - jnp.concatenate([col, col], axis=1)
            bias = jnp.full((CH, TI), levels[0], F32)
            for b in range(1, NB):
                bias = jnp.where(e >= float(2**b - 1), levels[b], bias)
            s = s_sc[pl.ds(at, CH), :] * scale + bias
            sg = sigmoid(s)
            w = s * sg
            g = sg + w * (1.0 - sg)
            if diagonal:
                jj = lax.broadcasted_iota(jnp.int32, (CH, TI), 0) + at
                ii = lax.broadcasted_iota(jnp.int32, (CH, TI), 1)
                keep = jj <= ii
                w = jnp.where(keep, w, 0.0)
                g = jnp.where(keep, g, 0.0)
            w_ref[rows, i0 : i0 + TI] = w.astype(BF16)
            g_ref[rows, i0 : i0 + TI] = g.astype(BF16)
            return carry

        lax.fori_loop(0, TI // CH, chunk, 0, unroll=UNROLL)

    for bi in range(S // TI):
        i0 = bi * TI
        if bi:

            def below(bj, carry, i0=i0):
                tile(i0, pl.multiple_of(bj * TI, TI), False)
                return carry

            lax.fori_loop(0, bi, below, 0)
        tile(i0, i0, True)
        att = mm(vt_sc[:, : i0 + TI], w_ref[: i0 + TI, i0 : i0 + TI])
        pos = lax.broadcasted_iota(jnp.int32, (DH, TI), 1) + i0
        att = jnp.where(pos < length, att, 0.0)
        mean = jnp.mean(att, axis=0, keepdims=True)
        high = mean.astype(BF16)
        left = mean - high.astype(F32)
        mid = left.astype(BF16)
        low = (left - mid.astype(F32)).astype(BF16)
        kept = high.astype(F32) + mid.astype(F32) + low.astype(F32)
        centred = (att - kept).astype(BF16)
        which = lax.broadcasted_iota(jnp.int32, (16, TI), 0)
        tail = jnp.where(
            which == 0,
            high.astype(F32),
            jnp.where(which == 1, mid.astype(F32), jnp.where(which == 2, low.astype(F32), 0.0)),
        ).astype(BF16)
        for t in range(TI // T):
            dest = bi * (TI // T) + t
            msg_ref[dest, :DH, :] = centred[:, t * T : (t + 1) * T]
            msg_ref[dest, DH:, :] = tail[:, t * T : (t + 1) * T]


def tail_kernel(
    length_ref,
    msg_ref,
    na_ref,
    nb_ref,
    x_ref,
    cot_ref,
    wg_ref,
    wo_ref,
    gain_ref,
    mixed_ref,
    dpg_ref,
    own_ref,
    send_ref,
    *more,
):
    datt_out, (att_sc, datt_ref, rows_sc, pg_sc, dmix_sc) = more[:H], more[H:]
    me, core, length = lax.axis_index("seq"), lax.axis_index("dp_2"), length_ref[0]
    for h in range(H):
        blk = msg_ref[h].astype(F32)
        att_t = blk[:DH] + (blk[DH : DH + 1] + blk[DH + 1 : DH + 2] + blk[DH + 2 : DH + 3])
        att_sc[:, h * DH : (h + 1) * DH] = att_t.T
    rows_sc[:64, :] = na_ref[...]
    rows_sc[64:, :] = nb_ref[...]
    cot = cot_ref[...]

    def columns(n, carry):
        at = pl.ds(pl.multiple_of(n * 512, 512), 512)
        pg_sc[:, at] = mm(rows_sc[...], wg_ref[:, at])
        dmix_sc[:, at] = nt(cot, wo_ref[at, :])
        return carry

    lax.fori_loop(0, D // 512, columns, 0)
    pg = pg_sc[...]
    d_mix = dmix_sc[...]
    att = att_sc[...]
    gain = gain_ref[...]
    c = att - jnp.mean(att, axis=-1, keepdims=True)
    var = jnp.mean(c * c, axis=-1, keepdims=True)
    r = lax.rsqrt(var + EPS)
    xhat = c * r
    normed_att = xhat * gain
    sg = sigmoid(pg)
    gate = pg * sg
    mixed_rows = (normed_att * gate).astype(BF16)
    rows_sc[...] = mixed_rows
    dpg_ref[...] = (d_mix * normed_att * (sg + gate * (1.0 - sg))).astype(BF16)
    u = d_mix * gate * gain
    d_att = r * (
        u
        - jnp.mean(u, axis=-1, keepdims=True)
        - xhat * jnp.mean(u * xhat, axis=-1, keepdims=True)
    )
    pos = lax.broadcasted_iota(jnp.int32, (T, D), 0) + me * T
    d_att = jnp.where(pos < length, d_att, 0.0).astype(BF16)
    for h in range(H):
        datt_ref[h] = d_att[:, h * DH : (h + 1) * DH]

    for h in range(H):
        part = tn(rows_sc[:, h * DH : (h + 1) * DH], cot).astype(BF16)
        for t in range(2):
            at = slice((2 * h + t) * 32, (2 * h + t + 1) * 32)
            even, odd = part[t * 64 : t * 64 + 32], part[t * 64 + 32 : t * 64 + 64]
            own_ref[at, :] = jnp.where(core == 0, even, odd)
            send_ref[at, :] = jnp.where(core == 0, odd, even)
    mixed_ref[...] = (x_ref[...].astype(F32) + mm(rows_sc[...], wo_ref[...])).astype(BF16)
    for k in range(H):
        datt_out[k][...] = datt_ref[lax.rem(me + k, H)]


def backward_kernel(*refs):
    blocks = refs[:8]
    proj_ref, w_ref, g_ref = refs[8:11]
    outs = refs[11:19]
    me = lax.axis_index("seq")
    q_sc, k_sc, kt_sc, v_sc, ds_sc, dqt_sc, out_ref, d_ref = refs[19:]
    for k in range(H):
        d_ref[lax.rem(me - k + H, H)] = blocks[k][...]
    for c in range(8):
        rows = slice(c * T, (c + 1) * T)
        p = proj_ref[rows, :]
        a = p * sigmoid(p)
        v_sc[rows, :] = a[:, :DH].astype(BF16)
        q_sc[rows, :] = a[:, DH : 2 * DH].astype(BF16)
        k_sc[rows, :] = a[:, 2 * DH :].astype(BF16)
        kt_sc[:, rows] = a[:, 2 * DH :].T.astype(BF16)
    scale = DH ** (-0.5)
    d = d_ref[...].reshape(S, DH)
    for bj in range(S // TI):
        j0 = bj * TI
        rows = slice(j0, j0 + TI)
        dw = nt(v_sc[rows, :], d[j0:, :])
        ds_sc[rows, j0:] = (dw * g_ref[rows, j0:].astype(F32)).astype(BF16)
        dk = mm(ds_sc[rows, j0:], q_sc[j0:, :]) * scale
        dv = mm(w_ref[rows, j0:], d[j0:, :])
        for t in range(TI // T):
            at = slice(j0 + t * T, j0 + (t + 1) * T)
            dest = bj * (TI // T) + t
            for n, grad in ((0, dv), (2, dk)):
                p = proj_ref[at, n * DH : (n + 1) * DH]
                sg = sigmoid(p)
                slope = sg * (1.0 + p * (1.0 - sg))
                out_ref[dest, :, n * DH : (n + 1) * DH] = (
                    grad[t * T : (t + 1) * T] * slope
                ).astype(BF16)
    for bi in range(S // TI):
        i0 = bi * TI
        dqt_sc[:, i0 : i0 + TI] = (
            mm(kt_sc[:, : i0 + TI], ds_sc[: i0 + TI, i0 : i0 + TI]) * scale
        )
    for t in range(8):
        at = slice(t * T, (t + 1) * T)
        p = proj_ref[at, DH : 2 * DH]
        sg = sigmoid(p)
        slope = sg * (1.0 + p * (1.0 - sg))
        out_ref[t, :, DH : 2 * DH] = (dqt_sc[:, at].T * slope).astype(BF16)
    for k in range(H):
        outs[k][...] = out_ref[lax.rem(me + k, H)]


def final_kernel(*refs):
    blocks = refs[:8]
    dpg_ref, early_ref, w_ref, x_ref, cot_ref, gain_ref, out_ref, msg_ref, lhs, acc = refs[8:]
    me = lax.axis_index("seq")
    b = pl.program_id(0)

    @pl.when(b == 0)
    def _():
        for k in range(H):
            msg_ref[lax.rem(me - k + H, H)] = blocks[k][...]
        for n in range(3):
            for h in range(H):
                lhs[n + 1, :, h * DH : (h + 1) * DH] = msg_ref[h, :, n * DH : (n + 1) * DH]
        lhs[0] = dpg_ref[...]
        acc[...] = jnp.zeros_like(acc)

        def gate(n, carry):
            at = pl.ds(pl.multiple_of(n * 512, 512), 512)
            acc[:, at] += nt(lhs[0], early_ref[at, :])
            return carry

        lax.fori_loop(0, D // 512, gate, 0)

    def columns(n, carry):
        at = pl.ds(pl.multiple_of(n * 512, 512), 512)
        acc[:, at] += nt(lhs[b + 1], w_ref[at, :])
        return carry

    lax.fori_loop(0, D // 512, columns, 0)

    @pl.when(b == 2)
    def _():
        x = x_ref[...].astype(F32)
        c = x - jnp.mean(x, axis=-1, keepdims=True)
        var = jnp.mean(c * c, axis=-1, keepdims=True)
        r = lax.rsqrt(var + EPS)
        xhat = c * r
        u = acc[...] * gain_ref[...]
        dx = r * (
            u
            - jnp.mean(u, axis=-1, keepdims=True)
            - xhat * jnp.mean(u * xhat, axis=-1, keepdims=True)
        )
        out_ref[...] = (cot_ref[...].astype(F32) + dx).astype(BF16)


def params(kib=LIMIT, **more):
    return pltpu.CompilerParams(vmem_limit_bytes=kib * 1024, **more)


def cost(us):
    flops = int(us * 3.0e8)
    return pl.CostEstimate(flops=flops, bytes_accessed=1 << 20, transcendentals=0)


def paired(value, axis, mask):
    count = lax.axis_size(axis)
    return lax.ppermute(value, axis, [(i, i ^ mask) for i in range(count)])


def shifted(value, by):
    return lax.ppermute(value, "seq", [(i, (i + by) % H) for i in range(H)])


def layer(tokens, cotangent, stamps, lengths, w_qkvu, w_out, gain_in, gain_out, bias_table):
    x = tokens[0]
    cot = cotangent[0]
    gain_in = gain_in.reshape(1, D)
    gain_out = gain_out.reshape(1, D)

    na, nb, early, late, copies = pl.pallas_call(
        prep_kernel,
        out_shape=[
            jax.ShapeDtypeStruct((64, D), BF16),
            jax.ShapeDtypeStruct((64, D), BF16),
            jax.ShapeDtypeStruct((32, 2 * D), BF16),
            jax.ShapeDtypeStruct((32, 3 * D), BF16),
            jax.ShapeDtypeStruct((32, 32, 3 * DH), BF16),
        ],
        in_specs=[VMEM] * 4,
        out_specs=[VMEM] * 5,
        compiler_params=params(61500),
        cost_estimate=cost(2),
        name="prep",
    )(x, gain_in, w_qkvu, w_out)
    w_early = lax.all_gather(early, DP, axis=0, tiled=True)
    w_late = lax.all_gather(late, DP, axis=0, tiled=True)
    ws = lax.all_to_all(copies, DP, 0, 0, tiled=True)
    ws = ws.reshape(D, 3 * DH)

    arrived = {(0, 0): na, (0, 1): nb}
    for k in range(1, 5):
        arrived[(-k, 0)] = shifted(arrived[(1 - k, 0)], 1)
        arrived[(k, 1)] = shifted(arrived[(k - 1, 1)], -1)
        if k < 4:
            arrived[(-k, 1)] = shifted(arrived[(1 - k, 1)], 1)
            arrived[(k, 0)] = shifted(arrived[(k - 1, 0)], -1)

    msg, proj, weight, slope = pl.pallas_call(
        forward_kernel,
        out_shape=[
            jax.ShapeDtypeStruct((H, MSG, T), BF16),
            jax.ShapeDtypeStruct((S, 3 * DH), F32),
            jax.ShapeDtypeStruct((S, S), BF16),
            jax.ShapeDtypeStruct((S, S), BF16),
        ],
        in_specs=[SMEM, SMEM] + [VMEM] * 18,
        out_specs=[VMEM] * 4,
        scratch_shapes=[
            pltpu.VMEM((S, D), BF16),
            pltpu.VMEM((S, T), F32),
            pltpu.VMEM((S, DH), BF16),
            pltpu.VMEM((S, DH), BF16),
            pltpu.VMEM((DH, S), BF16),
            pltpu.VMEM((TI, TI), F32),
        ],
        compiler_params=params(),
        cost_estimate=cost(10),
        name="attend",
    )(lengths, bias_table, *[arrived[a] for a in ARRIVALS], ws, stamps)

    att_msg = lax.all_to_all(msg, "seq", 0, 0, tiled=True)

    mixed, d_pg, w_own, w_send, *d_att = pl.pallas_call(
        tail_kernel,
        grid=(1,),
        out_shape=[
            jax.ShapeDtypeStruct((T, D), BF16),
            jax.ShapeDtypeStruct((T, D), BF16),
            jax.ShapeDtypeStruct((D // 2, D), BF16),
            jax.ShapeDtypeStruct((D // 2, D), BF16),
        ]
        + [jax.ShapeDtypeStruct((T, DH), BF16)] * H,
        in_specs=[SMEM]
        + [VMEM] * 5
        + [
            pl.BlockSpec((D, D), lambda i: (0, 0)),
            pl.BlockSpec((D, D), lambda i: (0, 1)),
            VMEM,
        ],
        out_specs=[VMEM] * (4 + H),
        scratch_shapes=[
            pltpu.VMEM((T, D), F32),
            pltpu.VMEM((H, T, DH), BF16),
            pltpu.VMEM((T, D), BF16),
            pltpu.VMEM((T, D), F32),
            pltpu.VMEM((T, D), F32),
        ],
        compiler_params=params(),
        cost_estimate=cost(5),
        name="tail",
    )(lengths, att_msg, na, nb, x, cot, w_early, w_early, gain_out)

    d_all = {0: d_att[0]}
    for k in ORDER:
        d_all[k] = shifted(d_att[k], k)

    other = paired(w_send, "dp_2", 1)
    pair = (w_own.astype(F32) + other.astype(F32)).astype(BF16)
    planes = lax.all_to_all(pair.reshape(16, 32, D), ("dp_0", "dp_1"), 0, 0, tiled=True)

    attend_back = pl.pallas_call(
        backward_kernel,
        out_shape=[jax.ShapeDtypeStruct((T, 3 * DH), BF16)] * H,
        in_specs=[VMEM] * (3 + H),
        out_specs=[VMEM] * H,
        scratch_shapes=[
            pltpu.VMEM((S, DH), BF16),
            pltpu.VMEM((S, DH), BF16),
            pltpu.VMEM((DH, S), BF16),
            pltpu.VMEM((S, DH), BF16),
            pltpu.VMEM((S, S), BF16),
            pltpu.VMEM((DH, S), F32),
            pltpu.VMEM((H, T, 3 * DH), BF16),
            pltpu.VMEM((H, T, DH), BF16),
        ],
        compiler_params=params(52000),
        cost_estimate=cost(6),
        name="attend_back",
    )
    d_proj = attend_back(*[d_all[k] for k in range(H)], proj, weight, slope)

    total = jnp.sum(planes.astype(F32), axis=0)
    for mask in (1, 3, 7):
        own = total.astype(BF16)
        far = paired(own, "seq", mask)
        total = own.astype(F32) + far.astype(F32)
    w_grad = total

    d_rows = {0: d_proj[0]}
    for k in ORDER:
        d_rows[k] = shifted(d_proj[k], k)

    final = pl.pallas_call(
        final_kernel,
        grid=(3,),
        out_shape=jax.ShapeDtypeStruct((T, D), BF16),
        in_specs=[VMEM] * (H + 1)
        + [
            pl.BlockSpec((D, D), lambda b: (0, 0)),
            pl.BlockSpec((D, D), lambda b: (0, b)),
            VMEM,
            VMEM,
            VMEM,
        ],
        out_specs=VMEM,
        scratch_shapes=[
            pltpu.VMEM((H, T, 3 * DH), BF16),
            pltpu.VMEM((4, T, D), BF16),
            pltpu.VMEM((T, D), F32),
        ],
        compiler_params=params(dimension_semantics=("arbitrary",)),
        cost_estimate=cost(5),
        name="final",
    )
    input_grad = final(
        *[d_rows[k] for k in range(H)], d_pg, w_early, w_late, x, cot, gain_in
    )

    return (mixed[None], input_grad[None], w_grad)


def solution(mesh):
    finer = Mesh(mesh.devices.reshape(4, 4, 2, mesh.shape["seq"]), (*DP, "seq"))
    placed = (
        P(DP, "seq", None),
        P(DP, "seq", None),
        P(DP, None),
        P(DP),
        P(DP, None),
        P(DP, None),
        P(),
        P(),
        P(),
    )
    return jax.shard_map(
        layer,
        mesh=finer,
        in_specs=placed,
        out_specs=(P(DP, "seq", None), P(DP, "seq", None), P(DP, None)),
        check_vma=False,
    )
```

```python
import jax
import jax.numpy as jnp
from jax import lax
from jax.experimental import pallas as pl
from jax.experimental.pallas import tpu as pltpu
from jax.sharding import Mesh
from jax.sharding import PartitionSpec as P


H = 8
DH = 128
D = 1024
T = 128
S = 1024
NB = 16
TI = 256
CH = 32
DP = ("dp_0", "dp_1", "dp_2")
EPS = 1e-05
MSG = 144
LIMIT = 52000
UNROLL = 8
FINAL = 52000
F32 = jnp.float32
BF16 = jnp.bfloat16

ORDER = (4, 5, 3, 6, 2, 7, 1)

VMEM = pl.BlockSpec(memory_space=pltpu.VMEM)
SMEM = pl.BlockSpec(memory_space=pltpu.SMEM)


def sigmoid(v):
    return 0.5 * jnp.tanh(0.5 * v) + 0.5


def nt(a, b):
    return lax.dot_general(a, b, (((1,), (1,)), ((), ())), preferred_element_type=F32)


def tn(a, b):
    return lax.dot_general(a, b, (((0,), (0,)), ((), ())), preferred_element_type=F32)


def mm(a, b):
    return jnp.dot(a, b, preferred_element_type=F32)


def prep_kernel(
    x_ref, gain_ref, w_ref, wout_ref, a_ref, b_ref, early_ref, late_ref, copies_ref
):
    me = lax.axis_index("seq")
    x = x_ref[...].astype(F32)
    c = x - jnp.mean(x, axis=-1, keepdims=True)
    var = jnp.mean(c * c, axis=-1, keepdims=True)
    n = (c * lax.rsqrt(var + EPS) * gain_ref[...]).astype(BF16)
    a_ref[...] = n[:64]
    b_ref[...] = n[64:]
    early_ref[:, :D] = w_ref[:, :D]
    early_ref[:, D:] = wout_ref[...]
    late_ref[...] = w_ref[:, D:]
    for part in range(3):
        at = pl.multiple_of((part + 1) * D + me * DH, DH)
        own = w_ref[:, pl.ds(at, DH)]
        for n in range(32):
            copies_ref[n, :, part * DH : (part + 1) * DH] = own


ARRIVALS = (
    [(0, 0), (0, 1)]
    + [(-k, 0) for k in (1, 2, 3, 4)]
    + [(-k, 1) for k in (1, 2, 3)]
    + [(k, 0) for k in (1, 2, 3)]
    + [(k, 1) for k in (1, 2, 3, 4)]
)


def forward_kernel(*refs):
    length_ref, bias_ref = refs[0], refs[1]
    blocks = refs[2:18]
    ws_ref, row_ref = refs[18:20]
    msg_ref, proj_ref, w_ref, g_ref = refs[20:24]
    x_all, col_sc, q_sc, k_sc, vt_sc, s_sc = refs[24:]
    me, length = lax.axis_index("seq"), length_ref[0]
    for (far, half), blk in zip(ARRIVALS, blocks):
        at = lax.rem(me + far + H, H) * T + half * 64
        x_all[pl.ds(pl.multiple_of(at, 64), 64), :] = blk[...]

    proj_ref[...] = mm(x_all[...], ws_ref[...])
    for c in range(8):
        cols = slice(c * T, (c + 1) * T)
        col_sc[cols, :] = jnp.broadcast_to(row_ref[:, cols].astype(F32), (T, T)).T
    for c in range(8):
        rows = slice(c * T, (c + 1) * T)
        p = proj_ref[rows, :]
        a = p * sigmoid(p)
        vt_sc[:, rows] = a[:, :DH].T.astype(BF16)
        q_sc[rows, :] = a[:, DH : 2 * DH].astype(BF16)
        k_sc[rows, :] = a[:, 2 * DH :].astype(BF16)
    scale = DH ** (-0.5)
    levels = [bias_ref[me, b] for b in range(NB)]

    def tile(i0, j0, diagonal):
        s_sc[...] = nt(k_sc[pl.ds(j0, TI), :], q_sc[i0 : i0 + TI, :])

        def chunk(c, carry):
            at = pl.multiple_of(c * CH, CH)
            rows = pl.ds(pl.multiple_of(j0 + at, CH), CH)
            col = col_sc[rows, :]
            e = row_ref[:, i0 : i0 + TI].astype(F32) - jnp.concatenate([col, col], axis=1)
            bias = jnp.full((CH, TI), levels[0], F32)
            for b in range(1, NB):
                bias = jnp.where(e >= float(2**b - 1), levels[b], bias)
            s = s_sc[pl.ds(at, CH), :] * scale + bias
            sg = sigmoid(s)
            w = s * sg
            g = sg + w * (1.0 - sg)
            if diagonal:
                jj = lax.broadcasted_iota(jnp.int32, (CH, TI), 0) + at
                ii = lax.broadcasted_iota(jnp.int32, (CH, TI), 1)
                keep = jj <= ii
                w = jnp.where(keep, w, 0.0)
                g = jnp.where(keep, g, 0.0)
            w_ref[rows, i0 : i0 + TI] = w.astype(BF16)
            g_ref[rows, i0 : i0 + TI] = g.astype(BF16)
            return carry

        lax.fori_loop(0, TI // CH, chunk, 0, unroll=UNROLL)

    for bi in range(S // TI):
        i0 = bi * TI
        if bi:

            def below(bj, carry, i0=i0):
                tile(i0, pl.multiple_of(bj * TI, TI), False)
                return carry

            lax.fori_loop(0, bi, below, 0)
        tile(i0, i0, True)
        att = mm(vt_sc[:, : i0 + TI], w_ref[: i0 + TI, i0 : i0 + TI])
        pos = lax.broadcasted_iota(jnp.int32, (DH, TI), 1) + i0
        att = jnp.where(pos < length, att, 0.0)
        mean = jnp.mean(att, axis=0, keepdims=True)
        high = mean.astype(BF16)
        left = mean - high.astype(F32)
        mid = left.astype(BF16)
        low = (left - mid.astype(F32)).astype(BF16)
        kept = high.astype(F32) + mid.astype(F32) + low.astype(F32)
        centred = (att - kept).astype(BF16)
        which = lax.broadcasted_iota(jnp.int32, (16, TI), 0)
        tail = jnp.where(
            which == 0,
            high.astype(F32),
            jnp.where(which == 1, mid.astype(F32), jnp.where(which == 2, low.astype(F32), 0.0)),
        ).astype(BF16)
        for t in range(TI // T):
            dest = bi * (TI // T) + t
            msg_ref[dest, :DH, :] = centred[:, t * T : (t + 1) * T]
            msg_ref[dest, DH:, :] = tail[:, t * T : (t + 1) * T]


def tail_kernel(
    length_ref,
    msg_ref,
    na_ref,
    nb_ref,
    x_ref,
    cot_ref,
    wg_ref,
    wo_ref,
    gain_ref,
    mixed_ref,
    dpg_ref,
    own_ref,
    send_ref,
    *more,
):
    datt_out, (att_sc, datt_ref, rows_sc, pg_sc, dmix_sc) = more[:H], more[H:]
    me, core, length = lax.axis_index("seq"), lax.axis_index("dp_2"), length_ref[0]
    for h in range(H):
        blk = msg_ref[h].astype(F32)
        att_t = blk[:DH] + (blk[DH : DH + 1] + blk[DH + 1 : DH + 2] + blk[DH + 2 : DH + 3])
        att_sc[:, h * DH : (h + 1) * DH] = att_t.T
    rows_sc[:64, :] = na_ref[...]
    rows_sc[64:, :] = nb_ref[...]
    cot = cot_ref[...]

    def columns(n, carry):
        at = pl.ds(pl.multiple_of(n * 512, 512), 512)
        pg_sc[:, at] = mm(rows_sc[...], wg_ref[:, at])
        dmix_sc[:, at] = nt(cot, wo_ref[at, :])
        return carry

    lax.fori_loop(0, D // 512, columns, 0)
    pg = pg_sc[...]
    d_mix = dmix_sc[...]
    att = att_sc[...]
    gain = gain_ref[...]
    c = att - jnp.mean(att, axis=-1, keepdims=True)
    var = jnp.mean(c * c, axis=-1, keepdims=True)
    r = lax.rsqrt(var + EPS)
    xhat = c * r
    normed_att = xhat * gain
    sg = sigmoid(pg)
    gate = pg * sg
    mixed_rows = (normed_att * gate).astype(BF16)
    rows_sc[...] = mixed_rows
    dpg_ref[...] = (d_mix * normed_att * (sg + gate * (1.0 - sg))).astype(BF16)
    u = d_mix * gate * gain
    d_att = r * (
        u
        - jnp.mean(u, axis=-1, keepdims=True)
        - xhat * jnp.mean(u * xhat, axis=-1, keepdims=True)
    )
    pos = lax.broadcasted_iota(jnp.int32, (T, D), 0) + me * T
    d_att = jnp.where(pos < length, d_att, 0.0).astype(BF16)
    for h in range(H):
        datt_ref[h] = d_att[:, h * DH : (h + 1) * DH]

    for h in range(H):
        part = tn(rows_sc[:, h * DH : (h + 1) * DH], cot).astype(BF16)
        for t in range(2):
            at = slice((2 * h + t) * 32, (2 * h + t + 1) * 32)
            even, odd = part[t * 64 : t * 64 + 32], part[t * 64 + 32 : t * 64 + 64]
            own_ref[at, :] = jnp.where(core == 0, even, odd)
            send_ref[at, :] = jnp.where(core == 0, odd, even)
    mixed_ref[...] = (x_ref[...].astype(F32) + mm(rows_sc[...], wo_ref[...])).astype(BF16)
    for k in range(H):
        datt_out[k][...] = datt_ref[lax.rem(me + k, H)]


def backward_kernel(*refs):
    blocks = refs[:8]
    proj_ref, w_ref, g_ref = refs[8:11]
    outs = refs[11:19]
    me = lax.axis_index("seq")
    q_sc, k_sc, kt_sc, v_sc, ds_sc, dqt_sc, out_ref, d_ref = refs[19:]
    for k in range(H):
        d_ref[lax.rem(me - k + H, H)] = blocks[k][...]
    for c in range(8):
        rows = slice(c * T, (c + 1) * T)
        p = proj_ref[rows, :]
        a = p * sigmoid(p)
        v_sc[rows, :] = a[:, :DH].astype(BF16)
        q_sc[rows, :] = a[:, DH : 2 * DH].astype(BF16)
        k_sc[rows, :] = a[:, 2 * DH :].astype(BF16)
        kt_sc[:, rows] = a[:, 2 * DH :].T.astype(BF16)
    scale = DH ** (-0.5)
    d = d_ref[...].reshape(S, DH)
    for bj in range(S // TI):
        j0 = bj * TI
        rows = slice(j0, j0 + TI)
        dw = nt(v_sc[rows, :], d[j0:, :])
        ds_sc[rows, j0:] = (dw * g_ref[rows, j0:].astype(F32)).astype(BF16)
        dk = mm(ds_sc[rows, j0:], q_sc[j0:, :]) * scale
        dv = mm(w_ref[rows, j0:], d[j0:, :])
        for t in range(TI // T):
            at = slice(j0 + t * T, j0 + (t + 1) * T)
            dest = bj * (TI // T) + t
            for n, grad in ((0, dv), (2, dk)):
                p = proj_ref[at, n * DH : (n + 1) * DH]
                sg = sigmoid(p)
                slope = sg * (1.0 + p * (1.0 - sg))
                out_ref[dest, :, n * DH : (n + 1) * DH] = (
                    grad[t * T : (t + 1) * T] * slope
                ).astype(BF16)
    for bi in range(S // TI):
        i0 = bi * TI
        dqt_sc[:, i0 : i0 + TI] = (
            mm(kt_sc[:, : i0 + TI], ds_sc[: i0 + TI, i0 : i0 + TI]) * scale
        )
    for t in range(8):
        at = slice(t * T, (t + 1) * T)
        p = proj_ref[at, DH : 2 * DH]
        sg = sigmoid(p)
        slope = sg * (1.0 + p * (1.0 - sg))
        out_ref[t, :, DH : 2 * DH] = (dqt_sc[:, at].T * slope).astype(BF16)
    for k in range(H):
        outs[k][...] = out_ref[lax.rem(me + k, H)]


def gate_kernel(dpg_ref, wg_ref, out_ref):
    def columns(n, carry):
        at = pl.ds(pl.multiple_of(n * 512, 512), 512)
        out_ref[:, at] = nt(dpg_ref[...], wg_ref[at, :])
        return carry

    lax.fori_loop(0, D // 512, columns, 0)


def final_kernel(*refs):
    blocks = refs[:8]
    back_ref, w_ref, x_ref, cot_ref, gain_ref, out_ref, lhs, acc = refs[8:]
    b = pl.program_id(0)

    @pl.when(b == 0)
    def _():
        me = lax.axis_index("seq")
        for k in range(H):
            h = lax.rem(me - k + H, H)
            at = pl.ds(pl.multiple_of(h * DH, DH), DH)
            for n in range(3):
                lhs[n, :, at] = blocks[k][:, n * DH : (n + 1) * DH]
        acc[...] = back_ref[...]

    def columns(n, carry):
        at = pl.ds(pl.multiple_of(n * 512, 512), 512)
        acc[:, at] += nt(lhs[b], w_ref[at, :])
        return carry

    lax.fori_loop(0, D // 512, columns, 0)

    @pl.when(b == 2)
    def _():
        x = x_ref[...].astype(F32)
        c = x - jnp.mean(x, axis=-1, keepdims=True)
        var = jnp.mean(c * c, axis=-1, keepdims=True)
        r = lax.rsqrt(var + EPS)
        xhat = c * r
        u = acc[...] * gain_ref[...]
        dx = r * (
            u
            - jnp.mean(u, axis=-1, keepdims=True)
            - xhat * jnp.mean(u * xhat, axis=-1, keepdims=True)
        )
        out_ref[...] = (cot_ref[...].astype(F32) + dx).astype(BF16)


def params(kib=LIMIT, **more):
    return pltpu.CompilerParams(vmem_limit_bytes=kib * 1024, **more)


def cost(us):
    flops = int(us * 3.0e8)
    return pl.CostEstimate(flops=flops, bytes_accessed=1 << 20, transcendentals=0)


def paired(value, axis, mask):
    count = lax.axis_size(axis)
    return lax.ppermute(value, axis, [(i, i ^ mask) for i in range(count)])


def shifted(value, by):
    return lax.ppermute(value, "seq", [(i, (i + by) % H) for i in range(H)])


def layer(tokens, cotangent, stamps, lengths, w_qkvu, w_out, gain_in, gain_out, bias_table):
    x = tokens[0]
    cot = cotangent[0]
    gain_in = gain_in.reshape(1, D)
    gain_out = gain_out.reshape(1, D)

    na, nb, early, late, copies = pl.pallas_call(
        prep_kernel,
        out_shape=[
            jax.ShapeDtypeStruct((64, D), BF16),
            jax.ShapeDtypeStruct((64, D), BF16),
            jax.ShapeDtypeStruct((32, 2 * D), BF16),
            jax.ShapeDtypeStruct((32, 3 * D), BF16),
            jax.ShapeDtypeStruct((32, 32, 3 * DH), BF16),
        ],
        in_specs=[VMEM] * 4,
        out_specs=[VMEM] * 5,
        compiler_params=params(61500),
        cost_estimate=cost(2),
        name="prep",
    )(x, gain_in, w_qkvu, w_out)
    w_early = lax.all_gather(early, DP, axis=0, tiled=True)
    w_late = lax.all_gather(late, DP, axis=0, tiled=True)
    ws = lax.all_to_all(copies, DP, 0, 0, tiled=True)
    ws = ws.reshape(D, 3 * DH)

    arrived = {(0, 0): na, (0, 1): nb}
    for k in range(1, 5):
        arrived[(-k, 0)] = shifted(arrived[(1 - k, 0)], 1)
        arrived[(k, 1)] = shifted(arrived[(k - 1, 1)], -1)
        if k < 4:
            arrived[(-k, 1)] = shifted(arrived[(1 - k, 1)], 1)
            arrived[(k, 0)] = shifted(arrived[(k - 1, 0)], -1)

    msg, proj, weight, slope = pl.pallas_call(
        forward_kernel,
        out_shape=[
            jax.ShapeDtypeStruct((H, MSG, T), BF16),
            jax.ShapeDtypeStruct((S, 3 * DH), F32),
            jax.ShapeDtypeStruct((S, S), BF16),
            jax.ShapeDtypeStruct((S, S), BF16),
        ],
        in_specs=[SMEM, SMEM] + [VMEM] * 18,
        out_specs=[VMEM] * 4,
        scratch_shapes=[
            pltpu.VMEM((S, D), BF16),
            pltpu.VMEM((S, T), F32),
            pltpu.VMEM((S, DH), BF16),
            pltpu.VMEM((S, DH), BF16),
            pltpu.VMEM((DH, S), BF16),
            pltpu.VMEM((TI, TI), F32),
        ],
        compiler_params=params(),
        cost_estimate=cost(10),
        name="attend",
    )(lengths, bias_table, *[arrived[a] for a in ARRIVALS], ws, stamps)

    att_msg = lax.all_to_all(msg, "seq", 0, 0, tiled=True)

    mixed, d_pg, w_own, w_send, *d_att = pl.pallas_call(
        tail_kernel,
        grid=(1,),
        out_shape=[
            jax.ShapeDtypeStruct((T, D), BF16),
            jax.ShapeDtypeStruct((T, D), BF16),
            jax.ShapeDtypeStruct((D // 2, D), BF16),
            jax.ShapeDtypeStruct((D // 2, D), BF16),
        ]
        + [jax.ShapeDtypeStruct((T, DH), BF16)] * H,
        in_specs=[SMEM]
        + [VMEM] * 5
        + [
            pl.BlockSpec((D, D), lambda i: (0, 0)),
            pl.BlockSpec((D, D), lambda i: (0, 1)),
            VMEM,
        ],
        out_specs=[VMEM] * (4 + H),
        scratch_shapes=[
            pltpu.VMEM((T, D), F32),
            pltpu.VMEM((H, T, DH), BF16),
            pltpu.VMEM((T, D), BF16),
            pltpu.VMEM((T, D), F32),
            pltpu.VMEM((T, D), F32),
        ],
        compiler_params=params(),
        cost_estimate=cost(5),
        name="tail",
    )(lengths, att_msg, na, nb, x, cot, w_early, w_early, gain_out)

    d_all = {0: d_att[0]}
    for k in ORDER:
        d_all[k] = shifted(d_att[k], k)

    other = paired(w_send, "dp_2", 1)
    pair = (w_own.astype(F32) + other.astype(F32)).astype(BF16)
    planes = lax.all_to_all(pair.reshape(16, 32, D), ("dp_0", "dp_1"), 0, 0, tiled=True)

    attend_back = pl.pallas_call(
        backward_kernel,
        out_shape=[jax.ShapeDtypeStruct((T, 3 * DH), BF16)] * H,
        in_specs=[VMEM] * (3 + H),
        out_specs=[VMEM] * H,
        scratch_shapes=[
            pltpu.VMEM((S, DH), BF16),
            pltpu.VMEM((S, DH), BF16),
            pltpu.VMEM((DH, S), BF16),
            pltpu.VMEM((S, DH), BF16),
            pltpu.VMEM((S, S), BF16),
            pltpu.VMEM((DH, S), F32),
            pltpu.VMEM((H, T, 3 * DH), BF16),
            pltpu.VMEM((H, T, DH), BF16),
        ],
        compiler_params=params(52000),
        cost_estimate=cost(6),
        name="attend_back",
    )
    d_proj = attend_back(*[d_all[k] for k in range(H)], proj, weight, slope)

    total = jnp.sum(planes.astype(F32), axis=0)
    for mask in (1, 3, 7):
        own = total.astype(BF16)
        far = paired(own, "seq", mask)
        total = own.astype(F32) + far.astype(F32)
    w_grad = total

    d_rows = {0: d_proj[0]}
    for k in ORDER:
        d_rows[k] = shifted(d_proj[k], k)

    gate_call = pl.pallas_call(
        gate_kernel,
        grid=(1,),
        out_shape=jax.ShapeDtypeStruct((T, D), F32),
        in_specs=[VMEM, pl.BlockSpec((D, D), lambda i: (0, 0))],
        out_specs=VMEM,
        compiler_params=params(),
        cost_estimate=cost(2),
        name="gate",
    )
    gate_back = gate_call(d_pg, w_early)

    final = pl.pallas_call(
        final_kernel,
        grid=(3,),
        out_shape=jax.ShapeDtypeStruct((T, D), BF16),
        in_specs=[VMEM] * (H + 1)
        + [pl.BlockSpec((D, D), lambda b: (0, b)), VMEM, VMEM, VMEM],
        out_specs=VMEM,
        scratch_shapes=[pltpu.VMEM((3, T, D), BF16), pltpu.VMEM((T, D), F32)],
        compiler_params=params(FINAL, dimension_semantics=("arbitrary",)),
        cost_estimate=cost(5),
        name="final",
    )
    input_grad = final(
        *[d_rows[k] for k in range(H)], gate_back, w_late, x, cot, gain_in
    )

    return (mixed[None], input_grad[None], w_grad)


def solution(mesh):
    finer = Mesh(mesh.devices.reshape(4, 4, 2, mesh.shape["seq"]), (*DP, "seq"))
    placed = (
        P(DP, "seq", None),
        P(DP, "seq", None),
        P(DP, None),
        P(DP),
        P(DP, None),
        P(DP, None),
        P(),
        P(),
        P(),
    )
    return jax.shard_map(
        layer,
        mesh=finer,
        in_specs=placed,
        out_specs=(P(DP, "seq", None), P(DP, "seq", None), P(DP, None)),
        check_vma=False,
    )
```

```python
import jax
import jax.numpy as jnp
from jax import lax
from jax.experimental import pallas as pl
from jax.experimental.pallas import tpu as pltpu
from jax.sharding import Mesh
from jax.sharding import PartitionSpec as P


H = 8
DH = 128
D = 1024
T = 128
S = 1024
NB = 16
TI = 256
CH = 32
DP = ("dp_0", "dp_1", "dp_2")
EPS = 1e-05
MSG = 144
LIMIT = 52000
UNROLL = 8
FINAL = 52000
F32 = jnp.float32
BF16 = jnp.bfloat16

ORDER = (4, 5, 3, 6, 2, 7, 1)

VMEM = pl.BlockSpec(memory_space=pltpu.VMEM)
SMEM = pl.BlockSpec(memory_space=pltpu.SMEM)


def sigmoid(v):
    return 0.5 * jnp.tanh(0.5 * v) + 0.5


def nt(a, b):
    return lax.dot_general(a, b, (((1,), (1,)), ((), ())), preferred_element_type=F32)


def tn(a, b):
    return lax.dot_general(a, b, (((0,), (0,)), ((), ())), preferred_element_type=F32)


def mm(a, b):
    return jnp.dot(a, b, preferred_element_type=F32)


def prep_kernel(
    x_ref, gain_ref, w_ref, wout_ref, a_ref, b_ref, own_ref, early_ref, late_ref, copies_ref
):
    me = lax.axis_index("seq")
    x = x_ref[...].astype(F32)
    c = x - jnp.mean(x, axis=-1, keepdims=True)
    var = jnp.mean(c * c, axis=-1, keepdims=True)
    n = (c * lax.rsqrt(var + EPS) * gain_ref[...]).astype(BF16)
    own_ref[...] = n
    a_ref[...] = n[:64]
    b_ref[...] = n[64:]
    early_ref[:, :D] = w_ref[:, :D]
    early_ref[:, D:] = wout_ref[...]
    late_ref[...] = w_ref[:, D:]
    for part in range(3):
        at = pl.multiple_of((part + 1) * D + me * DH, DH)
        own = w_ref[:, pl.ds(at, DH)]
        for n in range(32):
            copies_ref[n, :, part * DH : (part + 1) * DH] = own


ARRIVALS = (
    [(-k, 0) for k in (1, 2, 3, 4)]
    + [(-k, 1) for k in (1, 2, 3)]
    + [(k, 0) for k in (1, 2, 3)]
    + [(k, 1) for k in (1, 2, 3, 4)]
)


def forward_kernel(*refs):
    length_ref, bias_ref = refs[0], refs[1]
    own_ref, blocks = refs[2], refs[3:17]
    ws_ref, row_ref = refs[17:19]
    msg_ref, proj_ref, w_ref, g_ref = refs[19:23]
    x_all, col_sc, q_sc, k_sc, vt_sc, s_sc = refs[23:]
    me, length = lax.axis_index("seq"), length_ref[0]
    x_all[pl.ds(pl.multiple_of(me * T, T), T), :] = own_ref[...]
    for (far, half), blk in zip(ARRIVALS, blocks):
        at = lax.rem(me + far + H, H) * T + half * 64
        x_all[pl.ds(pl.multiple_of(at, 64), 64), :] = blk[...]

    proj_ref[...] = mm(x_all[...], ws_ref[...])
    for c in range(8):
        cols = slice(c * T, (c + 1) * T)
        col_sc[cols, :] = jnp.broadcast_to(row_ref[:, cols].astype(F32), (T, T)).T
    for c in range(8):
        rows = slice(c * T, (c + 1) * T)
        p = proj_ref[rows, :]
        a = p * sigmoid(p)
        vt_sc[:, rows] = a[:, :DH].T.astype(BF16)
        q_sc[rows, :] = a[:, DH : 2 * DH].astype(BF16)
        k_sc[rows, :] = a[:, 2 * DH :].astype(BF16)
    scale = DH ** (-0.5)
    levels = [bias_ref[me, b] for b in range(NB)]

    def tile(i0, j0, diagonal):
        s_sc[...] = nt(k_sc[pl.ds(j0, TI), :], q_sc[i0 : i0 + TI, :])

        def chunk(c, carry):
            at = pl.multiple_of(c * CH, CH)
            rows = pl.ds(pl.multiple_of(j0 + at, CH), CH)
            col = col_sc[rows, :]
            e = row_ref[:, i0 : i0 + TI].astype(F32) - jnp.concatenate([col, col], axis=1)
            bias = jnp.full((CH, TI), levels[0], F32)
            for b in range(1, NB):
                bias = jnp.where(e >= float(2**b - 1), levels[b], bias)
            s = s_sc[pl.ds(at, CH), :] * scale + bias
            sg = sigmoid(s)
            w = s * sg
            g = sg + w * (1.0 - sg)
            if diagonal:
                jj = lax.broadcasted_iota(jnp.int32, (CH, TI), 0) + at
                ii = lax.broadcasted_iota(jnp.int32, (CH, TI), 1)
                keep = jj <= ii
                w = jnp.where(keep, w, 0.0)
                g = jnp.where(keep, g, 0.0)
            w_ref[rows, i0 : i0 + TI] = w.astype(BF16)
            g_ref[rows, i0 : i0 + TI] = g.astype(BF16)
            return carry

        lax.fori_loop(0, TI // CH, chunk, 0, unroll=UNROLL)

    for bi in range(S // TI):
        i0 = bi * TI
        if bi:

            def below(bj, carry, i0=i0):
                tile(i0, pl.multiple_of(bj * TI, TI), False)
                return carry

            lax.fori_loop(0, bi, below, 0)
        tile(i0, i0, True)
        att = mm(vt_sc[:, : i0 + TI], w_ref[: i0 + TI, i0 : i0 + TI])
        pos = lax.broadcasted_iota(jnp.int32, (DH, TI), 1) + i0
        att = jnp.where(pos < length, att, 0.0)
        mean = jnp.mean(att, axis=0, keepdims=True)
        high = mean.astype(BF16)
        left = mean - high.astype(F32)
        mid = left.astype(BF16)
        low = (left - mid.astype(F32)).astype(BF16)
        kept = high.astype(F32) + mid.astype(F32) + low.astype(F32)
        centred = (att - kept).astype(BF16)
        which = lax.broadcasted_iota(jnp.int32, (16, TI), 0)
        tail = jnp.where(
            which == 0,
            high.astype(F32),
            jnp.where(which == 1, mid.astype(F32), jnp.where(which == 2, low.astype(F32), 0.0)),
        ).astype(BF16)
        for t in range(TI // T):
            dest = bi * (TI // T) + t
            msg_ref[dest, :DH, :] = centred[:, t * T : (t + 1) * T]
            msg_ref[dest, DH:, :] = tail[:, t * T : (t + 1) * T]


def tail_kernel(
    length_ref,
    msg_ref,
    own_rows_ref,
    x_ref,
    cot_ref,
    wg_ref,
    wo_ref,
    gain_ref,
    mixed_ref,
    dpg_ref,
    own_ref,
    send_ref,
    *more,
):
    datt_out, (att_sc, datt_ref, rows_sc, pg_sc, dmix_sc) = more[:H], more[H:]
    me, core, length = lax.axis_index("seq"), lax.axis_index("dp_2"), length_ref[0]
    for h in range(H):
        blk = msg_ref[h].astype(F32)
        att_t = blk[:DH] + (blk[DH : DH + 1] + blk[DH + 1 : DH + 2] + blk[DH + 2 : DH + 3])
        att_sc[:, h * DH : (h + 1) * DH] = att_t.T
    rows_sc[...] = own_rows_ref[...]
    cot = cot_ref[...]

    def columns(n, carry):
        at = pl.ds(pl.multiple_of(n * 512, 512), 512)
        pg_sc[:, at] = mm(rows_sc[...], wg_ref[:, at])
        dmix_sc[:, at] = nt(cot, wo_ref[at, :])
        return carry

    lax.fori_loop(0, D // 512, columns, 0)
    pg = pg_sc[...]
    d_mix = dmix_sc[...]
    att = att_sc[...]
    gain = gain_ref[...]
    c = att - jnp.mean(att, axis=-1, keepdims=True)
    var = jnp.mean(c * c, axis=-1, keepdims=True)
    r = lax.rsqrt(var + EPS)
    xhat = c * r
    normed_att = xhat * gain
    sg = sigmoid(pg)
    gate = pg * sg
    mixed_rows = (normed_att * gate).astype(BF16)
    rows_sc[...] = mixed_rows
    dpg_ref[...] = (d_mix * normed_att * (sg + gate * (1.0 - sg))).astype(BF16)
    u = d_mix * gate * gain
    d_att = r * (
        u
        - jnp.mean(u, axis=-1, keepdims=True)
        - xhat * jnp.mean(u * xhat, axis=-1, keepdims=True)
    )
    pos = lax.broadcasted_iota(jnp.int32, (T, D), 0) + me * T
    d_att = jnp.where(pos < length, d_att, 0.0).astype(BF16)
    for h in range(H):
        datt_ref[h] = d_att[:, h * DH : (h + 1) * DH]

    for h in range(H):
        part = tn(rows_sc[:, h * DH : (h + 1) * DH], cot).astype(BF16)
        for t in range(2):
            at = slice((2 * h + t) * 32, (2 * h + t + 1) * 32)
            even, odd = part[t * 64 : t * 64 + 32], part[t * 64 + 32 : t * 64 + 64]
            own_ref[at, :] = jnp.where(core == 0, even, odd)
            send_ref[at, :] = jnp.where(core == 0, odd, even)
    mixed_ref[...] = (x_ref[...].astype(F32) + mm(rows_sc[...], wo_ref[...])).astype(BF16)
    for k in range(H):
        datt_out[k][...] = datt_ref[lax.rem(me + k, H)]


def backward_kernel(*refs):
    blocks = refs[:8]
    proj_ref, w_ref, g_ref = refs[8:11]
    outs = refs[11:19]
    me = lax.axis_index("seq")
    q_sc, k_sc, kt_sc, v_sc, ds_sc, dqt_sc, out_ref, d_ref = refs[19:]
    for k in range(H):
        d_ref[lax.rem(me - k + H, H)] = blocks[k][...]
    for c in range(8):
        rows = slice(c * T, (c + 1) * T)
        p = proj_ref[rows, :]
        a = p * sigmoid(p)
        v_sc[rows, :] = a[:, :DH].astype(BF16)
        q_sc[rows, :] = a[:, DH : 2 * DH].astype(BF16)
        k_sc[rows, :] = a[:, 2 * DH :].astype(BF16)
        kt_sc[:, rows] = a[:, 2 * DH :].T.astype(BF16)
    scale = DH ** (-0.5)
    d = d_ref[...].reshape(S, DH)
    for bj in range(S // TI):
        j0 = bj * TI
        rows = slice(j0, j0 + TI)
        dw = nt(v_sc[rows, :], d[j0:, :])
        ds_sc[rows, j0:] = (dw * g_ref[rows, j0:].astype(F32)).astype(BF16)
        dk = mm(ds_sc[rows, j0:], q_sc[j0:, :]) * scale
        dv = mm(w_ref[rows, j0:], d[j0:, :])
        for t in range(TI // T):
            at = slice(j0 + t * T, j0 + (t + 1) * T)
            dest = bj * (TI // T) + t
            for n, grad in ((0, dv), (2, dk)):
                p = proj_ref[at, n * DH : (n + 1) * DH]
                sg = sigmoid(p)
                slope = sg * (1.0 + p * (1.0 - sg))
                out_ref[dest, :, n * DH : (n + 1) * DH] = (
                    grad[t * T : (t + 1) * T] * slope
                ).astype(BF16)
    for bi in range(S // TI):
        i0 = bi * TI
        dqt_sc[:, i0 : i0 + TI] = (
            mm(kt_sc[:, : i0 + TI], ds_sc[: i0 + TI, i0 : i0 + TI]) * scale
        )
    for t in range(8):
        at = slice(t * T, (t + 1) * T)
        p = proj_ref[at, DH : 2 * DH]
        sg = sigmoid(p)
        slope = sg * (1.0 + p * (1.0 - sg))
        out_ref[t, :, DH : 2 * DH] = (dqt_sc[:, at].T * slope).astype(BF16)
    for k in range(H):
        outs[k][...] = out_ref[lax.rem(me + k, H)]


def gate_kernel(dpg_ref, wg_ref, out_ref):
    def columns(n, carry):
        at = pl.ds(pl.multiple_of(n * 512, 512), 512)
        out_ref[:, at] = nt(dpg_ref[...], wg_ref[at, :])
        return carry

    lax.fori_loop(0, D // 512, columns, 0)


def final_kernel(*refs):
    blocks = refs[:8]
    back_ref, w_ref, x_ref, cot_ref, gain_ref, out_ref, lhs, acc = refs[8:]
    b = pl.program_id(0)

    @pl.when(b == 0)
    def _():
        me = lax.axis_index("seq")
        for k in range(H):
            h = lax.rem(me - k + H, H)
            at = pl.ds(pl.multiple_of(h * DH, DH), DH)
            for n in range(3):
                lhs[n, :, at] = blocks[k][:, n * DH : (n + 1) * DH]
        acc[...] = back_ref[...]

    def columns(n, carry):
        at = pl.ds(pl.multiple_of(n * 512, 512), 512)
        acc[:, at] += nt(lhs[b], w_ref[at, :])
        return carry

    lax.fori_loop(0, D // 512, columns, 0)

    @pl.when(b == 2)
    def _():
        x = x_ref[...].astype(F32)
        c = x - jnp.mean(x, axis=-1, keepdims=True)
        var = jnp.mean(c * c, axis=-1, keepdims=True)
        r = lax.rsqrt(var + EPS)
        xhat = c * r
        u = acc[...] * gain_ref[...]
        dx = r * (
            u
            - jnp.mean(u, axis=-1, keepdims=True)
            - xhat * jnp.mean(u * xhat, axis=-1, keepdims=True)
        )
        out_ref[...] = (cot_ref[...].astype(F32) + dx).astype(BF16)


def params(kib=LIMIT, **more):
    return pltpu.CompilerParams(vmem_limit_bytes=kib * 1024, **more)


def cost(us):
    flops = int(us * 3.0e8)
    return pl.CostEstimate(flops=flops, bytes_accessed=1 << 20, transcendentals=0)


def paired(value, axis, mask):
    count = lax.axis_size(axis)
    return lax.ppermute(value, axis, [(i, i ^ mask) for i in range(count)])


def shifted(value, by):
    return lax.ppermute(value, "seq", [(i, (i + by) % H) for i in range(H)])


def layer(tokens, cotangent, stamps, lengths, w_qkvu, w_out, gain_in, gain_out, bias_table):
    x = tokens[0]
    cot = cotangent[0]
    gain_in = gain_in.reshape(1, D)
    gain_out = gain_out.reshape(1, D)

    na, nb, own_rows, early, late, copies = pl.pallas_call(
        prep_kernel,
        out_shape=[
            jax.ShapeDtypeStruct((64, D), BF16),
            jax.ShapeDtypeStruct((64, D), BF16),
            jax.ShapeDtypeStruct((T, D), BF16),
            jax.ShapeDtypeStruct((32, 2 * D), BF16),
            jax.ShapeDtypeStruct((32, 3 * D), BF16),
            jax.ShapeDtypeStruct((32, 32, 3 * DH), BF16),
        ],
        in_specs=[VMEM] * 4,
        out_specs=[VMEM] * 6,
        compiler_params=params(61500),
        cost_estimate=cost(2),
        name="prep",
    )(x, gain_in, w_qkvu, w_out)
    w_early = lax.all_gather(early, DP, axis=0, tiled=True)
    w_late = lax.all_gather(late, DP, axis=0, tiled=True)
    ws = lax.all_to_all(copies, DP, 0, 0, tiled=True)
    ws = ws.reshape(D, 3 * DH)

    arrived = {(0, 0): na, (0, 1): nb}
    for k in range(1, 5):
        arrived[(-k, 0)] = shifted(arrived[(1 - k, 0)], 1)
        arrived[(k, 1)] = shifted(arrived[(k - 1, 1)], -1)
        if k < 4:
            arrived[(-k, 1)] = shifted(arrived[(1 - k, 1)], 1)
            arrived[(k, 0)] = shifted(arrived[(k - 1, 0)], -1)

    msg, proj, weight, slope = pl.pallas_call(
        forward_kernel,
        out_shape=[
            jax.ShapeDtypeStruct((H, MSG, T), BF16),
            jax.ShapeDtypeStruct((S, 3 * DH), F32),
            jax.ShapeDtypeStruct((S, S), BF16),
            jax.ShapeDtypeStruct((S, S), BF16),
        ],
        in_specs=[SMEM, SMEM] + [VMEM] * 17,
        out_specs=[VMEM] * 4,
        scratch_shapes=[
            pltpu.VMEM((S, D), BF16),
            pltpu.VMEM((S, T), F32),
            pltpu.VMEM((S, DH), BF16),
            pltpu.VMEM((S, DH), BF16),
            pltpu.VMEM((DH, S), BF16),
            pltpu.VMEM((TI, TI), F32),
        ],
        compiler_params=params(),
        cost_estimate=cost(10),
        name="attend",
    )(lengths, bias_table, own_rows, *[arrived[a] for a in ARRIVALS], ws, stamps)

    att_msg = lax.all_to_all(msg, "seq", 0, 0, tiled=True)

    mixed, d_pg, w_own, w_send, *d_att = pl.pallas_call(
        tail_kernel,
        grid=(1,),
        out_shape=[
            jax.ShapeDtypeStruct((T, D), BF16),
            jax.ShapeDtypeStruct((T, D), BF16),
            jax.ShapeDtypeStruct((D // 2, D), BF16),
            jax.ShapeDtypeStruct((D // 2, D), BF16),
        ]
        + [jax.ShapeDtypeStruct((T, DH), BF16)] * H,
        in_specs=[SMEM]
        + [VMEM] * 4
        + [
            pl.BlockSpec((D, D), lambda i: (0, 0)),
            pl.BlockSpec((D, D), lambda i: (0, 1)),
            VMEM,
        ],
        out_specs=[VMEM] * (4 + H),
        scratch_shapes=[
            pltpu.VMEM((T, D), F32),
            pltpu.VMEM((H, T, DH), BF16),
            pltpu.VMEM((T, D), BF16),
            pltpu.VMEM((T, D), F32),
            pltpu.VMEM((T, D), F32),
        ],
        compiler_params=params(),
        cost_estimate=cost(5),
        name="tail",
    )(lengths, att_msg, own_rows, x, cot, w_early, w_early, gain_out)

    d_all = {0: d_att[0]}
    for k in ORDER:
        d_all[k] = shifted(d_att[k], k)

    other = paired(w_send, "dp_2", 1)
    pair = (w_own.astype(F32) + other.astype(F32)).astype(BF16)
    planes = lax.all_to_all(pair.reshape(16, 32, D), ("dp_0", "dp_1"), 0, 0, tiled=True)

    attend_back = pl.pallas_call(
        backward_kernel,
        out_shape=[jax.ShapeDtypeStruct((T, 3 * DH), BF16)] * H,
        in_specs=[VMEM] * (3 + H),
        out_specs=[VMEM] * H,
        scratch_shapes=[
            pltpu.VMEM((S, DH), BF16),
            pltpu.VMEM((S, DH), BF16),
            pltpu.VMEM((DH, S), BF16),
            pltpu.VMEM((S, DH), BF16),
            pltpu.VMEM((S, S), BF16),
            pltpu.VMEM((DH, S), F32),
            pltpu.VMEM((H, T, 3 * DH), BF16),
            pltpu.VMEM((H, T, DH), BF16),
        ],
        compiler_params=params(52000),
        cost_estimate=cost(6),
        name="attend_back",
    )
    d_proj = attend_back(*[d_all[k] for k in range(H)], proj, weight, slope)

    total = jnp.sum(planes.astype(F32), axis=0)
    for mask in (1, 3, 7):
        own = total.astype(BF16)
        far = paired(own, "seq", mask)
        total = own.astype(F32) + far.astype(F32)
    w_grad = total

    d_rows = {0: d_proj[0]}
    for k in ORDER:
        d_rows[k] = shifted(d_proj[k], k)

    gate_call = pl.pallas_call(
        gate_kernel,
        grid=(1,),
        out_shape=jax.ShapeDtypeStruct((T, D), F32),
        in_specs=[VMEM, pl.BlockSpec((D, D), lambda i: (0, 0))],
        out_specs=VMEM,
        compiler_params=params(),
        cost_estimate=cost(2),
        name="gate",
    )
    gate_back = gate_call(d_pg, w_early)

    final = pl.pallas_call(
        final_kernel,
        grid=(3,),
        out_shape=jax.ShapeDtypeStruct((T, D), BF16),
        in_specs=[VMEM] * (H + 1)
        + [pl.BlockSpec((D, D), lambda b: (0, b)), VMEM, VMEM, VMEM],
        out_specs=VMEM,
        scratch_shapes=[pltpu.VMEM((3, T, D), BF16), pltpu.VMEM((T, D), F32)],
        compiler_params=params(FINAL, dimension_semantics=("arbitrary",)),
        cost_estimate=cost(5),
        name="final",
    )
    input_grad = final(
        *[d_rows[k] for k in range(H)], gate_back, w_late, x, cot, gain_in
    )

    return (mixed[None], input_grad[None], w_grad)


def solution(mesh):
    finer = Mesh(mesh.devices.reshape(4, 4, 2, mesh.shape["seq"]), (*DP, "seq"))
    placed = (
        P(DP, "seq", None),
        P(DP, "seq", None),
        P(DP, None),
        P(DP),
        P(DP, None),
        P(DP, None),
        P(),
        P(),
        P(),
    )
    return jax.shard_map(
        layer,
        mesh=finer,
        in_specs=placed,
        out_specs=(P(DP, "seq", None), P(DP, "seq", None), P(DP, None)),
        check_vma=False,
    )
```

```python
import jax
import jax.numpy as jnp
from jax import lax
from jax.experimental import pallas as pl
from jax.experimental.pallas import tpu as pltpu
from jax.sharding import Mesh
from jax.sharding import PartitionSpec as P


H = 8
DH = 128
D = 1024
T = 128
S = 1024
NB = 16
TI = 256
CH = 32
DP = ("dp_0", "dp_1", "dp_2")
EPS = 1e-05
MSG = 144
LIMIT = 52000
UNROLL = 8
FINAL = 52000
F32 = jnp.float32
BF16 = jnp.bfloat16

ORDER = (4, 5, 3, 6, 2, 7, 1)

VMEM = pl.BlockSpec(memory_space=pltpu.VMEM)
SMEM = pl.BlockSpec(memory_space=pltpu.SMEM)


def sigmoid(v):
    return 0.5 * jnp.tanh(0.5 * v) + 0.5


def nt(a, b):
    return lax.dot_general(a, b, (((1,), (1,)), ((), ())), preferred_element_type=F32)


def tn(a, b):
    return lax.dot_general(a, b, (((0,), (0,)), ((), ())), preferred_element_type=F32)


def mm(a, b):
    return jnp.dot(a, b, preferred_element_type=F32)


def prep_kernel(
    x_ref, gain_ref, w_ref, wout_ref, a_ref, b_ref, own_ref, early_ref, late_ref, copies_ref
):
    me = lax.axis_index("seq")
    x = x_ref[...].astype(F32)
    c = x - jnp.mean(x, axis=-1, keepdims=True)
    var = jnp.mean(c * c, axis=-1, keepdims=True)
    n = (c * lax.rsqrt(var + EPS) * gain_ref[...]).astype(BF16)
    own_ref[...] = n
    a_ref[...] = n[:64]
    b_ref[...] = n[64:]
    early_ref[:, :D] = w_ref[:, :D]
    early_ref[:, D:] = wout_ref[...]
    late_ref[...] = w_ref[:, D:]
    for part in range(3):
        at = pl.multiple_of((part + 1) * D + me * DH, DH)
        own = w_ref[:, pl.ds(at, DH)]
        for n in range(32):
            copies_ref[n, :, part * DH : (part + 1) * DH] = own


ARRIVALS = (
    [(-k, 0) for k in (1, 2, 3, 4)]
    + [(-k, 1) for k in (1, 2, 3)]
    + [(k, 0) for k in (1, 2, 3)]
    + [(k, 1) for k in (1, 2, 3, 4)]
)


def forward_kernel(*refs):
    length_ref, bias_ref = refs[0], refs[1]
    own_ref, blocks = refs[2], refs[3:17]
    ws_ref, row_ref = refs[17:19]
    msg_ref, proj_ref, w_ref, g_ref = refs[19:23]
    x_all, col_sc, q_sc, k_sc, vt_sc, s_sc, own_sem = refs[23:]
    me, length = lax.axis_index("seq"), length_ref[0]
    fetch = pltpu.make_async_copy(
        own_ref, x_all.at[pl.ds(pl.multiple_of(me * T, T), T), :], own_sem
    )
    fetch.start()
    for (far, half), blk in zip(ARRIVALS, blocks):
        at = lax.rem(me + far + H, H) * T + half * 64
        x_all[pl.ds(pl.multiple_of(at, 64), 64), :] = blk[...]

    fetch.wait()
    proj_ref[...] = mm(x_all[...], ws_ref[...])
    for c in range(8):
        cols = slice(c * T, (c + 1) * T)
        col_sc[cols, :] = jnp.broadcast_to(row_ref[:, cols].astype(F32), (T, T)).T
    for c in range(8):
        rows = slice(c * T, (c + 1) * T)
        p = proj_ref[rows, :]
        a = p * sigmoid(p)
        vt_sc[:, rows] = a[:, :DH].T.astype(BF16)
        q_sc[rows, :] = a[:, DH : 2 * DH].astype(BF16)
        k_sc[rows, :] = a[:, 2 * DH :].astype(BF16)
    scale = DH ** (-0.5)
    levels = [bias_ref[me, b] for b in range(NB)]

    def tile(i0, j0, diagonal):
        s_sc[...] = nt(k_sc[pl.ds(j0, TI), :], q_sc[i0 : i0 + TI, :])

        def chunk(c, carry):
            at = pl.multiple_of(c * CH, CH)
            rows = pl.ds(pl.multiple_of(j0 + at, CH), CH)
            col = col_sc[rows, :]
            e = row_ref[:, i0 : i0 + TI].astype(F32) - jnp.concatenate([col, col], axis=1)
            bias = jnp.full((CH, TI), levels[0], F32)
            for b in range(1, NB):
                bias = jnp.where(e >= float(2**b - 1), levels[b], bias)
            s = s_sc[pl.ds(at, CH), :] * scale + bias
            sg = sigmoid(s)
            w = s * sg
            g = sg + w * (1.0 - sg)
            if diagonal:
                jj = lax.broadcasted_iota(jnp.int32, (CH, TI), 0) + at
                ii = lax.broadcasted_iota(jnp.int32, (CH, TI), 1)
                keep = jj <= ii
                w = jnp.where(keep, w, 0.0)
                g = jnp.where(keep, g, 0.0)
            w_ref[rows, i0 : i0 + TI] = w.astype(BF16)
            g_ref[rows, i0 : i0 + TI] = g.astype(BF16)
            return carry

        lax.fori_loop(0, TI // CH, chunk, 0, unroll=UNROLL)

    for bi in range(S // TI):
        i0 = bi * TI
        if bi:

            def below(bj, carry, i0=i0):
                tile(i0, pl.multiple_of(bj * TI, TI), False)
                return carry

            lax.fori_loop(0, bi, below, 0)
        tile(i0, i0, True)
        att = mm(vt_sc[:, : i0 + TI], w_ref[: i0 + TI, i0 : i0 + TI])
        pos = lax.broadcasted_iota(jnp.int32, (DH, TI), 1) + i0
        att = jnp.where(pos < length, att, 0.0)
        mean = jnp.mean(att, axis=0, keepdims=True)
        high = mean.astype(BF16)
        left = mean - high.astype(F32)
        mid = left.astype(BF16)
        low = (left - mid.astype(F32)).astype(BF16)
        kept = high.astype(F32) + mid.astype(F32) + low.astype(F32)
        centred = (att - kept).astype(BF16)
        which = lax.broadcasted_iota(jnp.int32, (16, TI), 0)
        tail = jnp.where(
            which == 0,
            high.astype(F32),
            jnp.where(which == 1, mid.astype(F32), jnp.where(which == 2, low.astype(F32), 0.0)),
        ).astype(BF16)
        for t in range(TI // T):
            dest = bi * (TI // T) + t
            msg_ref[dest, :DH, :] = centred[:, t * T : (t + 1) * T]
            msg_ref[dest, DH:, :] = tail[:, t * T : (t + 1) * T]


def tail_kernel(
    length_ref,
    msg_ref,
    own_rows_ref,
    x_ref,
    cot_ref,
    wg_ref,
    wo_ref,
    gain_ref,
    mixed_ref,
    dpg_ref,
    own_ref,
    send_ref,
    *more,
):
    datt_out, (att_sc, datt_ref, rows_sc, pg_sc, dmix_sc) = more[:H], more[H:]
    me, core, length = lax.axis_index("seq"), lax.axis_index("dp_2"), length_ref[0]
    for h in range(H):
        blk = msg_ref[h].astype(F32)
        att_t = blk[:DH] + (blk[DH : DH + 1] + blk[DH + 1 : DH + 2] + blk[DH + 2 : DH + 3])
        att_sc[:, h * DH : (h + 1) * DH] = att_t.T
    rows_sc[...] = own_rows_ref[...]
    cot = cot_ref[...]

    def columns(n, carry):
        at = pl.ds(pl.multiple_of(n * 512, 512), 512)
        pg_sc[:, at] = mm(rows_sc[...], wg_ref[:, at])
        dmix_sc[:, at] = nt(cot, wo_ref[at, :])
        return carry

    lax.fori_loop(0, D // 512, columns, 0)
    pg = pg_sc[...]
    d_mix = dmix_sc[...]
    att = att_sc[...]
    gain = gain_ref[...]
    c = att - jnp.mean(att, axis=-1, keepdims=True)
    var = jnp.mean(c * c, axis=-1, keepdims=True)
    r = lax.rsqrt(var + EPS)
    xhat = c * r
    normed_att = xhat * gain
    sg = sigmoid(pg)
    gate = pg * sg
    mixed_rows = (normed_att * gate).astype(BF16)
    rows_sc[...] = mixed_rows
    dpg_ref[...] = (d_mix * normed_att * (sg + gate * (1.0 - sg))).astype(BF16)
    u = d_mix * gate * gain
    d_att = r * (
        u
        - jnp.mean(u, axis=-1, keepdims=True)
        - xhat * jnp.mean(u * xhat, axis=-1, keepdims=True)
    )
    pos = lax.broadcasted_iota(jnp.int32, (T, D), 0) + me * T
    d_att = jnp.where(pos < length, d_att, 0.0).astype(BF16)
    for h in range(H):
        datt_ref[h] = d_att[:, h * DH : (h + 1) * DH]

    for h in range(H):
        part = tn(rows_sc[:, h * DH : (h + 1) * DH], cot).astype(BF16)
        for t in range(2):
            at = slice((2 * h + t) * 32, (2 * h + t + 1) * 32)
            even, odd = part[t * 64 : t * 64 + 32], part[t * 64 + 32 : t * 64 + 64]
            own_ref[at, :] = jnp.where(core == 0, even, odd)
            send_ref[at, :] = jnp.where(core == 0, odd, even)
    mixed_ref[...] = (x_ref[...].astype(F32) + mm(rows_sc[...], wo_ref[...])).astype(BF16)
    for k in range(H):
        datt_out[k][...] = datt_ref[lax.rem(me + k, H)]


def backward_kernel(*refs):
    blocks = refs[:8]
    proj_ref, w_ref, g_ref = refs[8:11]
    outs = refs[11:19]
    me = lax.axis_index("seq")
    q_sc, k_sc, kt_sc, v_sc, ds_sc, dqt_sc, out_ref, d_ref = refs[19:]
    for k in range(H):
        d_ref[lax.rem(me - k + H, H)] = blocks[k][...]
    for c in range(8):
        rows = slice(c * T, (c + 1) * T)
        p = proj_ref[rows, :]
        a = p * sigmoid(p)
        v_sc[rows, :] = a[:, :DH].astype(BF16)
        q_sc[rows, :] = a[:, DH : 2 * DH].astype(BF16)
        k_sc[rows, :] = a[:, 2 * DH :].astype(BF16)
        kt_sc[:, rows] = a[:, 2 * DH :].T.astype(BF16)
    scale = DH ** (-0.5)
    d = d_ref[...].reshape(S, DH)
    for bj in range(S // TI):
        j0 = bj * TI
        rows = slice(j0, j0 + TI)
        dw = nt(v_sc[rows, :], d[j0:, :])
        ds_sc[rows, j0:] = (dw * g_ref[rows, j0:].astype(F32)).astype(BF16)
        dk = mm(ds_sc[rows, j0:], q_sc[j0:, :]) * scale
        dv = mm(w_ref[rows, j0:], d[j0:, :])
        for t in range(TI // T):
            at = slice(j0 + t * T, j0 + (t + 1) * T)
            dest = bj * (TI // T) + t
            for n, grad in ((0, dv), (2, dk)):
                p = proj_ref[at, n * DH : (n + 1) * DH]
                sg = sigmoid(p)
                slope = sg * (1.0 + p * (1.0 - sg))
                out_ref[dest, :, n * DH : (n + 1) * DH] = (
                    grad[t * T : (t + 1) * T] * slope
                ).astype(BF16)
    for bi in range(S // TI):
        i0 = bi * TI
        dqt_sc[:, i0 : i0 + TI] = (
            mm(kt_sc[:, : i0 + TI], ds_sc[: i0 + TI, i0 : i0 + TI]) * scale
        )
    for t in range(8):
        at = slice(t * T, (t + 1) * T)
        p = proj_ref[at, DH : 2 * DH]
        sg = sigmoid(p)
        slope = sg * (1.0 + p * (1.0 - sg))
        out_ref[t, :, DH : 2 * DH] = (dqt_sc[:, at].T * slope).astype(BF16)
    for k in range(H):
        outs[k][...] = out_ref[lax.rem(me + k, H)]


def gate_kernel(dpg_ref, wg_ref, out_ref):
    def columns(n, carry):
        at = pl.ds(pl.multiple_of(n * 512, 512), 512)
        out_ref[:, at] = nt(dpg_ref[...], wg_ref[at, :])
        return carry

    lax.fori_loop(0, D // 512, columns, 0)


def final_kernel(*refs):
    blocks = refs[:8]
    back_ref, w_ref, x_ref, cot_ref, gain_ref, out_ref, lhs, acc = refs[8:]
    b = pl.program_id(0)

    @pl.when(b == 0)
    def _():
        me = lax.axis_index("seq")
        for k in range(H):
            h = lax.rem(me - k + H, H)
            at = pl.ds(pl.multiple_of(h * DH, DH), DH)
            for n in range(3):
                lhs[n, :, at] = blocks[k][:, n * DH : (n + 1) * DH]
        acc[...] = back_ref[...]

    def columns(n, carry):
        at = pl.ds(pl.multiple_of(n * 512, 512), 512)
        acc[:, at] += nt(lhs[b], w_ref[at, :])
        return carry

    lax.fori_loop(0, D // 512, columns, 0)

    @pl.when(b == 2)
    def _():
        x = x_ref[...].astype(F32)
        c = x - jnp.mean(x, axis=-1, keepdims=True)
        var = jnp.mean(c * c, axis=-1, keepdims=True)
        r = lax.rsqrt(var + EPS)
        xhat = c * r
        u = acc[...] * gain_ref[...]
        dx = r * (
            u
            - jnp.mean(u, axis=-1, keepdims=True)
            - xhat * jnp.mean(u * xhat, axis=-1, keepdims=True)
        )
        out_ref[...] = (cot_ref[...].astype(F32) + dx).astype(BF16)


def params(kib=LIMIT, **more):
    return pltpu.CompilerParams(vmem_limit_bytes=kib * 1024, **more)


def cost(us):
    flops = int(us * 3.0e8)
    return pl.CostEstimate(flops=flops, bytes_accessed=1 << 20, transcendentals=0)


def paired(value, axis, mask):
    count = lax.axis_size(axis)
    return lax.ppermute(value, axis, [(i, i ^ mask) for i in range(count)])


def shifted(value, by):
    return lax.ppermute(value, "seq", [(i, (i + by) % H) for i in range(H)])


def layer(tokens, cotangent, stamps, lengths, w_qkvu, w_out, gain_in, gain_out, bias_table):
    x = tokens[0]
    cot = cotangent[0]
    gain_in = gain_in.reshape(1, D)
    gain_out = gain_out.reshape(1, D)

    na, nb, own_rows, early, late, copies = pl.pallas_call(
        prep_kernel,
        out_shape=[
            jax.ShapeDtypeStruct((64, D), BF16),
            jax.ShapeDtypeStruct((64, D), BF16),
            jax.ShapeDtypeStruct((T, D), BF16),
            jax.ShapeDtypeStruct((32, 2 * D), BF16),
            jax.ShapeDtypeStruct((32, 3 * D), BF16),
            jax.ShapeDtypeStruct((32, 32, 3 * DH), BF16),
        ],
        in_specs=[VMEM] * 4,
        out_specs=[VMEM] * 6,
        compiler_params=params(61500),
        cost_estimate=cost(2),
        name="prep",
    )(x, gain_in, w_qkvu, w_out)
    w_early = lax.all_gather(early, DP, axis=0, tiled=True)
    w_late = lax.all_gather(late, DP, axis=0, tiled=True)
    ws = lax.all_to_all(copies, DP, 0, 0, tiled=True)
    ws = ws.reshape(D, 3 * DH)

    arrived = {(0, 0): na, (0, 1): nb}
    for k in range(1, 5):
        arrived[(-k, 0)] = shifted(arrived[(1 - k, 0)], 1)
        arrived[(k, 1)] = shifted(arrived[(k - 1, 1)], -1)
        if k < 4:
            arrived[(-k, 1)] = shifted(arrived[(1 - k, 1)], 1)
            arrived[(k, 0)] = shifted(arrived[(k - 1, 0)], -1)

    msg, proj, weight, slope = pl.pallas_call(
        forward_kernel,
        out_shape=[
            jax.ShapeDtypeStruct((H, MSG, T), BF16),
            jax.ShapeDtypeStruct((S, 3 * DH), F32),
            jax.ShapeDtypeStruct((S, S), BF16),
            jax.ShapeDtypeStruct((S, S), BF16),
        ],
        in_specs=[SMEM, SMEM, pl.BlockSpec(memory_space=pl.ANY)] + [VMEM] * 16,
        out_specs=[VMEM] * 4,
        scratch_shapes=[
            pltpu.VMEM((S, D), BF16),
            pltpu.VMEM((S, T), F32),
            pltpu.VMEM((S, DH), BF16),
            pltpu.VMEM((S, DH), BF16),
            pltpu.VMEM((DH, S), BF16),
            pltpu.VMEM((TI, TI), F32),
            pltpu.SemaphoreType.DMA,
        ],
        compiler_params=params(),
        cost_estimate=cost(10),
        name="attend",
    )(lengths, bias_table, own_rows, *[arrived[a] for a in ARRIVALS], ws, stamps)

    att_msg = lax.all_to_all(msg, "seq", 0, 0, tiled=True)

    mixed, d_pg, w_own, w_send, *d_att = pl.pallas_call(
        tail_kernel,
        grid=(1,),
        out_shape=[
            jax.ShapeDtypeStruct((T, D), BF16),
            jax.ShapeDtypeStruct((T, D), BF16),
            jax.ShapeDtypeStruct((D // 2, D), BF16),
            jax.ShapeDtypeStruct((D // 2, D), BF16),
        ]
        + [jax.ShapeDtypeStruct((T, DH), BF16)] * H,
        in_specs=[SMEM]
        + [VMEM] * 4
        + [
            pl.BlockSpec((D, D), lambda i: (0, 0)),
            pl.BlockSpec((D, D), lambda i: (0, 1)),
            VMEM,
        ],
        out_specs=[VMEM] * (4 + H),
        scratch_shapes=[
            pltpu.VMEM((T, D), F32),
            pltpu.VMEM((H, T, DH), BF16),
            pltpu.VMEM((T, D), BF16),
            pltpu.VMEM((T, D), F32),
            pltpu.VMEM((T, D), F32),
        ],
        compiler_params=params(),
        cost_estimate=cost(5),
        name="tail",
    )(lengths, att_msg, own_rows, x, cot, w_early, w_early, gain_out)

    d_all = {0: d_att[0]}
    for k in ORDER:
        d_all[k] = shifted(d_att[k], k)

    other = paired(w_send, "dp_2", 1)
    pair = (w_own.astype(F32) + other.astype(F32)).astype(BF16)
    planes = lax.all_to_all(pair.reshape(16, 32, D), ("dp_0", "dp_1"), 0, 0, tiled=True)

    attend_back = pl.pallas_call(
        backward_kernel,
        out_shape=[jax.ShapeDtypeStruct((T, 3 * DH), BF16)] * H,
        in_specs=[VMEM] * (3 + H),
        out_specs=[VMEM] * H,
        scratch_shapes=[
            pltpu.VMEM((S, DH), BF16),
            pltpu.VMEM((S, DH), BF16),
            pltpu.VMEM((DH, S), BF16),
            pltpu.VMEM((S, DH), BF16),
            pltpu.VMEM((S, S), BF16),
            pltpu.VMEM((DH, S), F32),
            pltpu.VMEM((H, T, 3 * DH), BF16),
            pltpu.VMEM((H, T, DH), BF16),
        ],
        compiler_params=params(52000),
        cost_estimate=cost(6),
        name="attend_back",
    )
    d_proj = attend_back(*[d_all[k] for k in range(H)], proj, weight, slope)

    total = jnp.sum(planes.astype(F32), axis=0)
    for mask in (1, 3, 7):
        own = total.astype(BF16)
        far = paired(own, "seq", mask)
        total = own.astype(F32) + far.astype(F32)
    w_grad = total

    d_rows = {0: d_proj[0]}
    for k in ORDER:
        d_rows[k] = shifted(d_proj[k], k)

    gate_call = pl.pallas_call(
        gate_kernel,
        grid=(1,),
        out_shape=jax.ShapeDtypeStruct((T, D), F32),
        in_specs=[VMEM, pl.BlockSpec((D, D), lambda i: (0, 0))],
        out_specs=VMEM,
        compiler_params=params(),
        cost_estimate=cost(2),
        name="gate",
    )
    gate_back = gate_call(d_pg, w_early)

    final = pl.pallas_call(
        final_kernel,
        grid=(3,),
        out_shape=jax.ShapeDtypeStruct((T, D), BF16),
        in_specs=[VMEM] * (H + 1)
        + [pl.BlockSpec((D, D), lambda b: (0, b)), VMEM, VMEM, VMEM],
        out_specs=VMEM,
        scratch_shapes=[pltpu.VMEM((3, T, D), BF16), pltpu.VMEM((T, D), F32)],
        compiler_params=params(FINAL, dimension_semantics=("arbitrary",)),
        cost_estimate=cost(5),
        name="final",
    )
    input_grad = final(
        *[d_rows[k] for k in range(H)], gate_back, w_late, x, cot, gain_in
    )

    return (mixed[None], input_grad[None], w_grad)


def solution(mesh):
    finer = Mesh(mesh.devices.reshape(4, 4, 2, mesh.shape["seq"]), (*DP, "seq"))
    placed = (
        P(DP, "seq", None),
        P(DP, "seq", None),
        P(DP, None),
        P(DP),
        P(DP, None),
        P(DP, None),
        P(),
        P(),
        P(),
    )
    return jax.shard_map(
        layer,
        mesh=finer,
        in_specs=placed,
        out_specs=(P(DP, "seq", None), P(DP, "seq", None), P(DP, None)),
        check_vma=False,
    )
```
